8 devices in a mesh: dp: 1 (over z), tp: 2 (over y), pp: 4 (over x, core).
Axes of the slice: x: 2, y: 2, z: 1, core: 2. Of those that a mesh axis runs over, the one named last changes fastest.
Arguments:
- x_in: bfloat16 [4, 2, 1024, 2816], P(None, 'dp', 'tp')
- ln1_gain: float32 [4, 2816], P('pp')
- ln1_bias: float32 [4, 2816], P('pp')
- w_q: bfloat16 [4, 2816, 2816], P('pp', None, 'tp')
- b_q: float32 [4, 2816], P('pp', 'tp')
- w_kv: bfloat16 [4, 2816, 256], P('pp')
- b_kv: float32 [4, 256], P('pp')
- w_o: bfloat16 [4, 2816, 2816], P('pp', 'tp')
- b_o: float32 [4, 2816], P('pp')
- ln2_gain: float32 [4, 2816], P('pp')
- ln2_bias: float32 [4, 2816], P('pp')
- w_up: bfloat16 [4, 2816, 11264], P('pp', None, 'tp')
- b_up: float32 [4, 11264], P('pp', 'tp')
- w_down: bfloat16 [4, 11264, 2816], P('pp', 'tp')
- b_down: float32 [4, 2816], P('pp')
Outputs:
- output: bfloat16 [4, 4, 2, 1024, 2816], P('pp', None, 'dp', 'tp')
All inputs are finite; a program needn't handle non-finite values.
Results may differ from the reference program's by a relative error of at most 0.0192473.
Values are sent between devices in bfloat16 or wider.
A program may use at most 1 GiB of HBM per device.

```python
import jax
import jax.numpy as jnp
from jax import lax

N_MICRO = 4
MICRO_BATCH = 2
SEQ_LEN = 1024
HIDDEN = 2816
N_HEADS = 22
FFN_DIM = 11264
HEAD_DIM = 128
N_STAGES = 4


def setup_inputs(seed: int = 0, part: int = 0) -> dict:
    keys = jax.random.split(jax.random.key(seed), 15)
    hidden_scale = HIDDEN ** -0.5

    def normal_draw(key_index, arr_shape, std_scale, offset):
        return jax.random.normal(keys[key_index], arr_shape, jnp.float32) * std_scale + offset

    x_key = jax.random.fold_in(keys[0], part)
    x_in = jax.random.normal(x_key, (N_MICRO, MICRO_BATCH, SEQ_LEN, HIDDEN), jnp.float32).astype(jnp.bfloat16)
    stage_vec = (N_STAGES, HIDDEN)
    return {
        'x_in': x_in,
        'ln1_gain': normal_draw(1, stage_vec, 0.2, 1.0),
        'ln1_bias': normal_draw(2, stage_vec, 0.3, 0.0),
        'w_q': normal_draw(3, (N_STAGES, HIDDEN, HIDDEN), 2.0 * hidden_scale, 0.0).astype(jnp.bfloat16),
        'b_q': normal_draw(4, stage_vec, 0.3, 0.0),
        'w_kv': normal_draw(5, (N_STAGES, HIDDEN, 2 * HEAD_DIM), hidden_scale, 0.0).astype(jnp.bfloat16),
        'b_kv': normal_draw(6, (N_STAGES, 2 * HEAD_DIM), 0.3, 0.0),
        'w_o': normal_draw(7, (N_STAGES, HIDDEN, HIDDEN), hidden_scale, 0.0).astype(jnp.bfloat16),
        'b_o': normal_draw(8, stage_vec, 0.3, 0.0),
        'ln2_gain': normal_draw(9, stage_vec, 0.2, 1.0),
        'ln2_bias': normal_draw(10, stage_vec, 0.3, 0.0),
        'w_up': normal_draw(11, (N_STAGES, HIDDEN, FFN_DIM), hidden_scale, 0.0).astype(jnp.bfloat16),
        'b_up': normal_draw(12, (N_STAGES, FFN_DIM), 0.3, 0.0),
        'w_down': normal_draw(13, (N_STAGES, FFN_DIM, HIDDEN), FFN_DIM ** -0.5, 0.0).astype(jnp.bfloat16),
        'b_down': normal_draw(14, stage_vec, 0.3, 0.0),
    }


def layer_norm(values, ln_gain, ln_shift):
    average = jnp.mean(values, axis=-1, keepdims=True)
    centered = values - average
    variance = jnp.mean(jnp.square(centered), axis=-1, keepdims=True)
    return centered * lax.rsqrt(variance + 1e-5) * ln_gain + ln_shift


def block(x_tok, params):
    (ln1_gain, ln1_bias, w_q, b_q, w_kv, b_kv, w_o, b_o, ln2_gain, ln2_bias, w_up, b_up, w_down, b_down) = params
    residual = x_tok.reshape(MICRO_BATCH * SEQ_LEN, HIDDEN).astype(jnp.float32)
    normed = layer_norm(residual, ln1_gain, ln1_bias).astype(jnp.bfloat16)
    queries = (jnp.dot(normed, w_q, preferred_element_type=jnp.float32) + b_q).astype(jnp.bfloat16)
    key_val = (jnp.dot(normed, w_kv, preferred_element_type=jnp.float32) + b_kv).astype(jnp.bfloat16)
    queries = queries.reshape(MICRO_BATCH, SEQ_LEN, N_HEADS, HEAD_DIM).astype(jnp.float32)
    key_val = key_val.reshape(MICRO_BATCH, SEQ_LEN, 2 * HEAD_DIM).astype(jnp.float32)
    keys_part = key_val[:, :, :HEAD_DIM]
    vals_part = key_val[:, :, HEAD_DIM:]
    scores = jnp.einsum('bqhd,bkd->bqhk', queries, keys_part) * (HEAD_DIM ** -0.5)
    positions = jnp.arange(SEQ_LEN)
    causal = positions[:, None, None] >= positions[None, None, :]
    attn_probs = jax.nn.softmax(jnp.where(causal, scores, -1e30), axis=-1).astype(jnp.bfloat16).astype(jnp.float32)
    context = jnp.einsum('bqhk,bkd->bqhd', attn_probs, vals_part).astype(jnp.bfloat16)
    context = context.reshape(MICRO_BATCH * SEQ_LEN, HIDDEN)
    attn_out = jnp.dot(context, w_o, preferred_element_type=jnp.float32) + b_o
    mid_f32 = (residual + attn_out).astype(jnp.bfloat16).astype(jnp.float32)
    normed2 = layer_norm(mid_f32, ln2_gain, ln2_bias).astype(jnp.bfloat16)
    up_act = jax.nn.gelu(jnp.dot(normed2, w_up, preferred_element_type=jnp.float32) + b_up, approximate=True).astype(jnp.bfloat16)
    mlp_out = jnp.dot(up_act, w_down, preferred_element_type=jnp.float32) + b_down
    return (mid_f32 + mlp_out).astype(jnp.bfloat16).reshape(MICRO_BATCH, SEQ_LEN, HIDDEN)


def reference(x_in, ln1_gain, ln1_bias, w_q, b_q, w_kv, b_kv, w_o, b_o, ln2_gain, ln2_bias, w_up, b_up, w_down, b_down):
    params = (ln1_gain, ln1_bias, w_q, b_q, w_kv, b_kv, w_o, b_o, ln2_gain, ln2_bias, w_up, b_up, w_down, b_down)

    def run_micro(micro_in):
        def stage_step(carried, stage_params):
            return block(carried, stage_params), None
        micro_out, _unused = lax.scan(stage_step, micro_in, params)
        return micro_out

    results = lax.map(run_micro, x_in)
    zero_lead = jnp.zeros((N_STAGES - 1,) + results.shape, jnp.bfloat16)
    return jnp.concatenate([zero_lead, results[None]], axis=0)
```

```python
import functools

import jax
import jax.numpy as jnp
from jax import lax
from jax.experimental import pallas as pl
from jax.experimental.pallas import tpu as pltpu
from jax.sharding import PartitionSpec as P

F32 = jnp.float32
BF16 = jnp.bfloat16
MESH = pl.DeviceIdType.MESH

PARAM_SPECS = (P('pp', None), P('pp', None), P('pp', None, 'tp'), P('pp', 'tp'), P('pp', None, None), P('pp', None), P('pp', 'tp', None), P('pp', None), P('pp', None), P('pp', None), P('pp', None, 'tp'), P('pp', 'tp'), P('pp', 'tp', None), P('pp', None))

CW = 256
HEAD = 128
UNIT_ROWS = 256
SLOTS = 8


def stage_kernel(cfg, x_in, g1, s1, wq, bq, wkv, bkv, wo, bo, g2, s2, wup, bup, wdn, bdn,
                 out, x_recv, wq_peer, wo_peer,
                 ring, xbuf, hbuf, qbuf, cbuf, x1own, x1recv, ubuf, zbuf, psend, precv, ybuf, kt, vbuf, bq_all,
                 ring_sem, xload_sem, xrecv_sem, xin_send_sem, w_send_sem, w_recv_sem, x1_send_sem, x1_recv_sem,
                 p_send_sem, p_recv_sem, y_send_sem, out_recv_sem, go_sem):
    (n_stages, n_units, quarters, rows, hidden, ffn_loc) = cfg
    half_q = quarters // 2
    nq = hidden // CW
    nu = ffn_loc // CW
    heads_half = hidden // 2 // HEAD
    n_heads = 2 * heads_half
    scale = HEAD ** -0.5
    stage = lax.axis_index('pp')
    rank = lax.axis_index('tp')
    peer = {'tp': 1 - rank}
    nxt = {'pp': jnp.minimum(stage + 1, n_stages - 1)}
    prv = {'pp': jnp.maximum(stage - 1, 0)}
    first = stage == 0
    last = stage == n_stages - 1
    even = lax.rem(stage, 2) == 0

    counts = (1 + nq, nq, nu, nu, 2 * nq)
    bases = tuple(sum(counts[:i]) for i in range(len(counts)))
    total = sum(counts)

    def slot_of(u, phase, idx):
        return lax.rem(u * total + bases[phase] + idx, SLOTS)

    def start_chunk(u, phase, idx):
        slot = slot_of(u, phase, idx)
        dst = ring.at[slot]
        sem = ring_sem.at[slot]

        def cols(c, width):
            return pl.ds(pl.multiple_of(c * width, width), width)

        if phase == 0:
            @pl.when(idx == 0)
            def _():
                pltpu.make_async_copy(wkv.at[0], dst, sem).start()

            for b in range(2):
                block = (idx - 1) * 2 + b
                piece = dst.at[:, pl.ds(b * HEAD, HEAD)]

                @pl.when((idx > 0) & (block < heads_half))
                def _():
                    pltpu.make_async_copy(wq.at[0, :, cols(block, HEAD)], piece, sem).start()

                @pl.when((idx > 0) & (block >= heads_half))
                def _():
                    pltpu.make_async_copy(wq_peer.at[:, cols(block - heads_half, HEAD)], piece, sem).start()
        elif phase == 1:
            half = hidden // 2
            pltpu.make_async_copy(wo.at[0, :, cols(idx, CW)], dst.at[pl.ds(0, half), :], sem).start()
            pltpu.make_async_copy(wo_peer.at[:, cols(idx, CW)], dst.at[pl.ds(half, half), :], sem).start()
        elif phase in (2, 3):
            pltpu.make_async_copy(wup.at[0, :, cols(idx, CW)], dst, sem).start()
        else:
            part = lax.rem(idx, 2)
            pltpu.make_async_copy(
                wdn.at[0, pl.ds(pl.multiple_of(part * hidden, hidden), hidden), cols(idx // 2, CW)], dst, sem).start()

    def prefetch(u, phase, idx):
        ahead = idx + SLOTS
        n = counts[phase]

        @pl.when(ahead < n)
        def _():
            start_chunk(u, phase, ahead)

        if phase + 1 < len(counts):
            @pl.when(ahead >= n)
            def _():
                start_chunk(u, phase + 1, ahead - n)
        else:
            @pl.when((ahead >= n) & (u + 1 < n_units))
            def _():
                start_chunk(u + 1, 0, ahead - n)

    def wait_chunk(u, phase, idx):
        slot = slot_of(u, phase, idx)
        pltpu.make_async_copy(wkv.at[0], ring.at[slot], ring_sem.at[slot]).wait()
        return slot

    def layer_norm(src, dst, gain, shift):
        block = 32

        def body(i, carry):
            r = pl.ds(pl.multiple_of(i * block, block), block)
            v = src[r, :].astype(F32)
            mean = jnp.mean(v, axis=-1, keepdims=True)
            cen = v - mean
            var = jnp.mean(cen * cen, axis=-1, keepdims=True)
            dst[r, :] = (cen * lax.rsqrt(var + 1e-5) * gain[...] + shift[...]).astype(BF16)
            return carry

        lax.fori_loop(0, rows // block, body, 0)

    def send_x_in(t):
        mb = t // quarters
        j = lax.rem(t, quarters)

        @pl.when(first & (t < n_units) & (j // half_q == rank))
        def _():
            src = x_in.at[mb, 1 - rank, pl.ds(pl.multiple_of(lax.rem(j, half_q) * rows, rows), rows), :]
            pltpu.make_async_remote_copy(src, x_recv.at[t], xin_send_sem.at[t], xrecv_sem.at[t],
                                         device_id=peer, device_id_type=MESH).start()

    def weight_copy(i):
        src, dst = ((bq, bq_all.at[pl.ds(heads_half, heads_half)]), (wq.at[0], wq_peer), (wo.at[0], wo_peer))[i]
        return pltpu.make_async_remote_copy(src, dst, w_send_sem.at[i], w_recv_sem.at[i], device_id=peer, device_id_type=MESH)

    barrier = pltpu.get_barrier_semaphore()
    pl.semaphore_signal(barrier, inc=1, device_id=peer, device_id_type=MESH)

    @pl.when(stage > 0)
    def _():
        pl.semaphore_signal(barrier, inc=1, device_id=prv, device_id_type=MESH)

    @pl.when(jnp.logical_not(last))
    def _():
        pl.semaphore_signal(barrier, inc=1, device_id=nxt, device_id_type=MESH)

    pl.semaphore_wait(barrier, 1 + (stage > 0).astype(jnp.int32) + (stage < n_stages - 1).astype(jnp.int32))

    for t in range(half_q):
        send_x_in(jnp.int32(t))

    @pl.when(jnp.logical_not(even))
    def _():
        pl.semaphore_wait(go_sem, 1)

    for i in range(3):
        weight_copy(i).start()
    bq_all[pl.ds(0, heads_half)] = bq[...]

    own_chunks = 1 + heads_half // 2
    for i in range(min(SLOTS, own_chunks)):
        start_chunk(0, 0, jnp.int32(i))
    weight_copy(0).wait_recv()
    weight_copy(1).wait_recv()
    for i in range(min(SLOTS, own_chunks), SLOTS):
        start_chunk(0, 0, jnp.int32(i))

    def attention(j):
        rh = 128

        def one_head(jj, h):
            q = qbuf[h]
            for b in range(rows // rh):
                nk = rows * jj + rh * (b + 1)
                s = jnp.dot(q[b * rh:(b + 1) * rh], kt[:, :nk], preferred_element_type=F32) * scale
                row = lax.broadcasted_iota(jnp.int32, (rh, nk), 0) + (nk - rh)
                col = lax.broadcasted_iota(jnp.int32, (rh, nk), 1)
                s = jnp.where(col <= row, s, -1e30)
                p = jnp.exp(s - jnp.max(s, axis=-1, keepdims=True))
                p = (p * (1.0 / jnp.sum(p, axis=-1, keepdims=True))).astype(BF16)
                c = jnp.dot(p, vbuf[:nk, :], preferred_element_type=F32)
                cbuf[pl.ds(b * rh, rh), pl.ds(pl.multiple_of(h * HEAD, HEAD), HEAD)] = c.astype(BF16)

        for jj in range(quarters):
            @pl.when(j == jj)
            def _():
                def body(i, carry):
                    one_head(jj, 2 * i)
                    one_head(jj, 2 * i + 1)
                    return carry

                lax.fori_loop(0, n_heads // 2, body, 0)

    def x1_copy(slot, c):
        cols = pl.ds(pl.multiple_of(c * CW, CW), CW)
        return pltpu.make_async_remote_copy(x1own.at[:, cols], x1recv.at[slot, :, cols], x1_send_sem, x1_recv_sem.at[slot],
                                            device_id=peer, device_id_type=MESH)

    def p_copy(slot, c):
        cols = pl.ds(pl.multiple_of(c * CW, CW), CW)
        return pltpu.make_async_remote_copy(psend.at[:, cols], precv.at[slot, :, cols], p_send_sem, p_recv_sem.at[slot],
                                            device_id=peer, device_id_type=MESH)

    def whole(src, dst, send_sem, recv_sem):
        return pltpu.make_async_remote_copy(src, dst, send_sem, recv_sem, device_id=peer, device_id_type=MESH)

    def finish(u):
        slot = lax.rem(u, 2)
        mb = u // quarters
        j = lax.rem(u, quarters)
        whole(psend, precv.at[slot], p_send_sem, p_recv_sem.at[slot]).wait_recv()

        @pl.when(u > 0)
        def _():
            pltpu.make_async_copy(ybuf, x_recv.at[0], y_send_sem).wait()

        block = 32

        def body(i, carry):
            r = pl.ds(pl.multiple_of(i * block, block), block)
            ybuf[r, :] = (zbuf[r, :] + precv[slot, r, :].astype(F32)).astype(BF16)
            return carry

        lax.fori_loop(0, rows // block, body, 0)

        @pl.when(jnp.logical_not(last))
        def _():
            pltpu.make_async_remote_copy(ybuf, x_recv.at[u], y_send_sem, xrecv_sem.at[u], device_id=nxt, device_id_type=MESH).start()

        place = out.at[mb, rank, pl.ds(pl.multiple_of(lax.rem(j, half_q) * rows, rows), rows), :]

        @pl.when(last & (j // half_q == rank))
        def _():
            pltpu.make_async_copy(ybuf, place, y_send_sem).start()

        @pl.when(last & (j // half_q != rank))
        def _():
            pltpu.make_async_remote_copy(ybuf, place, y_send_sem, out_recv_sem.at[u], device_id=peer, device_id_type=MESH).start()

    def up(u, phase, row0):
        def body(c, carry):
            slot = wait_chunk(u, phase, c)
            a = jnp.dot(hbuf[...], ring[slot], preferred_element_type=F32) + bup[c]
            t = jnp.tanh(0.7978845608028654 * (a + 0.044715 * (a * a * a)))
            ubuf[pl.ds(row0, rows), pl.ds(pl.multiple_of(c * CW, CW), CW)] = (0.5 * a * (1.0 + t)).astype(BF16)
            prefetch(u, phase, c)
            return carry

        lax.fori_loop(0, nu, body, 0)

    def unit(u, carry):
        mb = u // quarters
        j = lax.rem(u, quarters)
        slot2 = lax.rem(u, 2)

        send_x_in(u + half_q)
        local = first & (j // half_q == rank)

        @pl.when(local)
        def _():
            src = x_in.at[mb, rank, pl.ds(pl.multiple_of(lax.rem(j, half_q) * rows, rows), rows), :]
            pltpu.make_async_copy(src, xbuf, xload_sem).start()

        @pl.when(jnp.logical_not(local))
        def _():
            pltpu.make_async_remote_copy(ybuf, x_recv.at[u], y_send_sem, xrecv_sem.at[u], device_id=peer, device_id_type=MESH).wait_recv()
            pltpu.make_async_copy(x_recv.at[u], xbuf, xload_sem).start()

        pltpu.make_async_copy(x_recv.at[0], xbuf, xload_sem).wait()
        layer_norm(xbuf, hbuf, g1, s1)

        slot = wait_chunk(u, 0, 0)
        kv = jnp.dot(hbuf[...], ring[slot], preferred_element_type=F32) + bkv[...]
        at = pl.ds(pl.multiple_of(j * rows, rows), rows)
        kt[:, at] = kv[:, :HEAD].astype(BF16).astype(F32).T.astype(BF16)
        vbuf[at, :] = kv[:, HEAD:].astype(BF16)
        prefetch(u, 0, 0)

        @pl.when(u == 0)
        def _():
            weight_copy(2).wait_recv()
            for i in range(3):
                weight_copy(i).wait_send()

            @pl.when(even)
            def _():
                pl.semaphore_signal(go_sem, inc=1, device_id=nxt, device_id_type=MESH)

        def q_body(c, carry):
            slot = wait_chunk(u, 0, c + 1)
            a = jnp.dot(hbuf[...], ring[slot], preferred_element_type=F32)
            qbuf[2 * c] = (a[:, :HEAD] + bq_all[2 * c]).astype(BF16)
            qbuf[2 * c + 1] = (a[:, HEAD:] + bq_all[2 * c + 1]).astype(BF16)
            prefetch(u, 0, c + 1)
            return carry

        lax.fori_loop(0, nq, q_body, 0)
        attention(j)

        @pl.when(u > 0)
        def _():
            whole(x1own, x1recv.at[slot2], x1_send_sem, x1_recv_sem.at[slot2]).wait_send()

        def o_body(c, carry):
            slot = wait_chunk(u, 1, c)
            cols = pl.ds(pl.multiple_of(c * CW, CW), CW)
            a = jnp.dot(cbuf[...], ring[slot], preferred_element_type=F32)
            x1own[:, cols] = (xbuf[:, cols].astype(F32) + a + bo[c]).astype(BF16)

            @pl.when(c > 0)
            def _():
                x1_copy(slot2, c - 1).start()

            prefetch(u, 1, c)
            return carry

        lax.fori_loop(0, nq, o_body, 0)
        layer_norm(x1own, hbuf, g2, s2)
        x1_copy(slot2, nq - 1).start()

        up(u, 2, 0)

        @pl.when(u > 0)
        def _():
            finish(u - 1)

        whole(x1own, x1recv.at[slot2], x1_send_sem, x1_recv_sem.at[slot2]).wait_recv()
        layer_norm(x1recv.at[slot2], hbuf, g2, s2)
        up(u, 3, rows)

        @pl.when(u > 0)
        def _():
            whole(psend, precv.at[slot2], p_send_sem, p_recv_sem.at[slot2]).wait_send()

        def down_body(c, carry):
            cols = pl.ds(pl.multiple_of(c * CW, CW), CW)
            slot_a = wait_chunk(u, 4, 2 * c)
            slot_b = wait_chunk(u, 4, 2 * c + 1)
            a = (jnp.dot(ubuf[:, :hidden], ring[slot_a], preferred_element_type=F32)
                 + jnp.dot(ubuf[:, hidden:], ring[slot_b], preferred_element_type=F32))
            zbuf[:, cols] = x1own[:, cols].astype(F32) + a[:rows] + bdn[c]
            psend[:, cols] = a[rows:].astype(BF16)

            @pl.when(c > 0)
            def _():
                p_copy(slot2, c - 1).start()

            prefetch(u, 4, 2 * c)
            prefetch(u, 4, 2 * c + 1)
            return carry

        lax.fori_loop(0, nq, down_body, 0)
        p_copy(slot2, nq - 1).start()
        return carry

    lax.fori_loop(0, n_units, unit, 0)
    end = n_units - 1
    finish(jnp.int32(end))

    whole(x1own, x1recv.at[end % 2], x1_send_sem, x1_recv_sem.at[end % 2]).wait_send()
    whole(psend, precv.at[end % 2], p_send_sem, p_recv_sem.at[end % 2]).wait_send()
    pltpu.make_async_copy(ybuf, x_recv.at[0], y_send_sem).wait()

    def drain(t, carry):
        j = lax.rem(t, quarters)
        mine = j // half_q == rank

        @pl.when(first & mine)
        def _():
            pltpu.make_async_remote_copy(ybuf, x_recv.at[t], xin_send_sem.at[t], xrecv_sem.at[t], device_id=peer, device_id_type=MESH).wait_send()

        @pl.when(last & mine)
        def _():
            place = out.at[t // quarters, 1 - rank, pl.ds(pl.multiple_of(lax.rem(j, half_q) * rows, rows), rows), :]
            pltpu.make_async_remote_copy(ybuf, place, y_send_sem, out_recv_sem.at[t], device_id=peer, device_id_type=MESH).wait_recv()

        return carry

    lax.fori_loop(0, n_units, drain, 0)


def run_stage(x_loc, params, n_stages):
    (ln1_gain, ln1_bias, w_q, b_q, w_kv, b_kv, w_o, b_o, ln2_gain, ln2_bias, w_up, b_up, w_down, b_down) = params
    n_micro, _, seq_loc, hidden = x_loc.shape
    ffn_loc = w_up.shape[2]
    rows = min(UNIT_ROWS, seq_loc // 2)
    quarters = 2 * seq_loc // rows
    n_units = n_micro * quarters
    nq = hidden // CW
    nu = ffn_loc // CW
    heads_half = hidden // 2 // HEAD
    cfg = (n_stages, n_units, quarters, rows, hidden, ffn_loc)
    vmem = pl.BlockSpec(memory_space=pltpu.VMEM)
    anym = pl.BlockSpec(memory_space=pl.ANY)
    args = (
        x_loc, ln1_gain, ln1_bias, w_q, b_q.reshape(heads_half, 1, HEAD), w_kv, b_kv, w_o, b_o.reshape(nq, 1, CW),
        ln2_gain, ln2_bias, w_up, b_up.reshape(nu, 1, CW), w_down, b_down.reshape(nq, 1, CW),
    )
    in_specs = [anym, vmem, vmem, anym, vmem, anym, vmem, anym, vmem, vmem, vmem, anym, vmem, anym, vmem]
    out_shape = (
        jax.ShapeDtypeStruct(x_loc.shape, BF16),
        jax.ShapeDtypeStruct((n_units, rows, hidden), BF16),
        jax.ShapeDtypeStruct((hidden, hidden // 2), BF16),
        jax.ShapeDtypeStruct((hidden // 2, hidden), BF16),
    )
    dma = pltpu.SemaphoreType.DMA
    scratch = [
        pltpu.VMEM((SLOTS, hidden, CW), BF16),
        pltpu.VMEM((rows, hidden), BF16),
        pltpu.VMEM((rows, hidden), BF16),
        pltpu.VMEM((2 * heads_half, rows, HEAD), BF16),
        pltpu.VMEM((rows, hidden), BF16),
        pltpu.VMEM((rows, hidden), BF16),
        pltpu.VMEM((2, rows, hidden), BF16),
        pltpu.VMEM((2 * rows, ffn_loc), BF16),
        pltpu.VMEM((rows, hidden), F32),
        pltpu.VMEM((rows, hidden), BF16),
        pltpu.VMEM((2, rows, hidden), BF16),
        pltpu.VMEM((rows, hidden), BF16),
        pltpu.VMEM((HEAD, quarters * rows), BF16),
        pltpu.VMEM((quarters * rows, HEAD), BF16),
        pltpu.VMEM((2 * heads_half, 1, HEAD), F32),
        dma((SLOTS,)),
        dma,
        dma((n_units,)),
        dma((n_units,)),
        dma((3,)),
        dma((3,)),
        dma,
        dma((2,)),
        dma,
        dma((2,)),
        dma,
        dma((n_units,)),
        pltpu.SemaphoreType.REGULAR,
    ]
    return pl.pallas_call(
        functools.partial(stage_kernel, cfg),
        out_shape=out_shape,
        in_specs=in_specs,
        out_specs=(anym,) * 4,
        scratch_shapes=scratch,
        compiler_params=pltpu.CompilerParams(collective_id=0, has_side_effects=True, vmem_limit_bytes=60 * 2 ** 20),
        name='stage_loop',
    )(*args)[0]


def solution(mesh):
    pp_size = mesh.shape['pp']

    def stage_program(x_loc, *params):
        result = run_stage(x_loc, params, pp_size)
        is_last = lax.axis_index('pp') == pp_size - 1
        return jnp.where(is_last, result, jnp.zeros_like(result))[None]

    return jax.shard_map(stage_program, mesh=mesh, in_specs=(P(None, 'dp', 'tp', None),) + PARAM_SPECS, out_specs=P('pp', None, 'dp', 'tp', None), check_vma=False)
```

```python
import functools

import jax
import jax.numpy as jnp
from jax import lax
from jax.experimental import pallas as pl
from jax.experimental.pallas import tpu as pltpu
from jax.sharding import PartitionSpec as P

F32 = jnp.float32
BF16 = jnp.bfloat16
MESH = pl.DeviceIdType.MESH

PARAM_SPECS = (P('pp', None), P('pp', None), P('pp', None, 'tp'), P('pp', 'tp'), P('pp', None, None), P('pp', None), P('pp', 'tp', None), P('pp', None), P('pp', None), P('pp', None), P('pp', None, 'tp'), P('pp', 'tp'), P('pp', 'tp', None), P('pp', None))

CW = 256
HEAD = 128
UNIT_ROWS = 256
SLOTS = 10
LN_ROWS = 32
WO_PARTS = 4


def scoped(name, fn, *args):
    with jax.named_scope(name):
        return fn(*args)


def stage_kernel(cfg, x_in, g1, s1, wq, bq, wkv, bkv, wo, bo, g2, s2, wup, bup, wdn, bdn,
                 out, x_recv, wq_peer, wo_peer, relay_a, relay_b,
                 ring, xbuf, hbuf, h2buf, qbuf, cbuf, x1own, x1recv, ubuf, zbuf, psend, precv, ybuf, kt, vones, bq_all,
                 ring_sem, xload_sem, xrecv_sem, xin_send_sem, w_send_sem, w_recv_sem, wo_send_sem, wo_recv_sem,
                 ra_recv_sem, rb_send_sem, rb_recv_sem, rc_send_sem,
                 x1_send_sem, x1_recv_sem, p_send_sem, p_recv_sem, y_send_sem, out_recv_sem, go_sem):
    (n_stages, n_units, quarters, rows, hidden, ffn_loc) = cfg
    half_q = quarters // 2
    half = hidden // 2
    nq = hidden // CW
    nu = ffn_loc // CW
    heads_half = half // HEAD
    n_heads = 2 * heads_half
    stage = lax.axis_index('pp')
    rank = lax.axis_index('tp')
    peer = {'tp': 1 - rank}
    nxt = {'pp': jnp.minimum(stage + 1, n_stages - 1)}
    prv = {'pp': jnp.maximum(stage - 1, 0)}
    across = {'pp': 2 - stage}
    first = stage == 0
    third = stage == 2
    last = stage == n_stages - 1
    even = lax.rem(stage, 2) == 0

    KVQ, O, DOWN, UP = 0, 1, 2, 3
    counts = (1 + nq, nq, 2 * nq, nu)
    total = sum(counts)

    def base(u, phase):
        skipped = jnp.where(u > 0, counts[DOWN], 0)
        if phase == KVQ:
            return u * total - skipped
        if phase == O:
            return u * total - skipped + counts[KVQ]
        if phase == DOWN:
            absent = jnp.where(u == n_units, counts[KVQ] + counts[O], 0)
            return u * total - counts[DOWN] + counts[KVQ] + counts[O] - absent
        return u * total + counts[KVQ] + counts[O]

    def slot_at(g):
        return lax.rem(g, SLOTS)

    def start_chunk(u, phase, idx):
        slot = slot_at(base(u, phase) + idx)
        dst = ring.at[slot]
        sem = ring_sem.at[slot]

        def cols(c, width):
            return pl.ds(pl.multiple_of(c * width, width), width)

        if phase == KVQ:
            @pl.when(idx == 0)
            def _():
                pltpu.make_async_copy(wkv.at[0], dst, sem).start()

            for b in range(2):
                block = (idx - 1) * 2 + b
                piece = dst.at[:, pl.ds(b * HEAD, HEAD)]

                @pl.when((idx > 0) & (block < heads_half))
                def _():
                    pltpu.make_async_copy(wq.at[0, :, cols(block, HEAD)], piece, sem).start()

                @pl.when((idx > 0) & (block >= heads_half))
                def _():
                    pltpu.make_async_copy(wq_peer.at[:, cols(block - heads_half, HEAD)], piece, sem).start()
        elif phase == O:
            pltpu.make_async_copy(wo.at[0, :, cols(idx, CW)], dst.at[pl.ds(0, half), :], sem).start()
            pltpu.make_async_copy(wo_peer.at[:, cols(idx, CW)], dst.at[pl.ds(half, half), :], sem).start()
        elif phase == UP:
            pltpu.make_async_copy(wup.at[0, :, cols(idx, CW)], dst, sem).start()
        else:
            part = lax.rem(idx, 2)
            pltpu.make_async_copy(
                wdn.at[0, pl.ds(pl.multiple_of(part * hidden, hidden), hidden), cols(idx // 2, CW)], dst, sem).start()

    def prefetch(u, phase, idx):
        ahead = idx + SLOTS
        n = counts[phase]

        @pl.when(ahead < n)
        def _():
            start_chunk(u, phase, ahead)

        over = ahead - n
        if phase == KVQ:
            @pl.when(over >= 0)
            def _():
                start_chunk(u, O, over)
        elif phase == O:
            @pl.when((over >= 0) & (u > 0))
            def _():
                start_chunk(u, DOWN, over)

            @pl.when((over >= 0) & (u == 0))
            def _():
                start_chunk(u, UP, over)
        elif phase == DOWN:
            @pl.when((over >= 0) & (u < n_units))
            def _():
                start_chunk(u, UP, over)
        else:
            @pl.when((over >= 0) & (u + 1 < n_units))
            def _():
                start_chunk(u + 1, KVQ, over)

            @pl.when((over >= 0) & (u + 1 == n_units))
            def _():
                start_chunk(u + 1, DOWN, over)

    def wait_chunk(g):
        slot = slot_at(g)
        pltpu.make_async_copy(wkv.at[0], ring.at[slot], ring_sem.at[slot]).wait()

    def ln_rows(src, dst, gain, shift, r, to):
        v = src[r, :].astype(F32)
        mean = jnp.mean(v, axis=-1, keepdims=True)
        cen = v - mean
        var = jnp.mean(cen * cen, axis=-1, keepdims=True)
        dst[to, :] = (cen * lax.rsqrt(var + 1e-5) * gain[...] + shift[...]).astype(BF16)

    def layer_norm(src, dst, gain, shift, row0=0):
        def body(i, carry):
            at = pl.multiple_of(i * LN_ROWS, LN_ROWS)
            ln_rows(src, dst, gain, shift, pl.ds(at, LN_ROWS), pl.ds(row0 + at, LN_ROWS))
            return carry

        lax.fori_loop(0, rows // LN_ROWS, body, 0)

    def send_x_in(t):
        mb = t // quarters
        j = lax.rem(t, quarters)

        @pl.when(first & (t < n_units) & (j // half_q == rank))
        def _():
            src = x_in.at[mb, 1 - rank, pl.ds(pl.multiple_of(lax.rem(j, half_q) * rows, rows), rows), :]
            remote(src, x_recv.at[t], xin_send_sem.at[t], xrecv_sem.at[t]).start()

    def remote(src, dst, send_sem, recv_sem, to=peer):
        return pltpu.make_async_remote_copy(src, dst, send_sem, recv_sem, device_id=to, device_id_type=MESH)

    def signal(sem, to):
        pl.semaphore_signal(sem, inc=1, device_id=to, device_id_type=MESH)

    def wq_copy():
        return remote(wq.at[0], wq_peer, w_send_sem.at[0], w_recv_sem.at[0])

    def bq_copy():
        return remote(bq, bq_all.at[pl.ds(heads_half, heads_half)], w_send_sem.at[1], w_recv_sem.at[1])

    def part_rows(i):
        return pl.ds(i * (half // WO_PARTS), half // WO_PARTS)

    def wo_copy(i):
        return remote(wo.at[0, part_rows(i), :], wo_peer.at[part_rows(i), :], wo_send_sem.at[i], wo_recv_sem.at[i])

    def hop_a(i):
        return remote(wo.at[0, part_rows(i), :], relay_a.at[part_rows(i), :], wo_send_sem.at[i], ra_recv_sem.at[i], across)

    def hop_b(i):
        return remote(relay_a.at[part_rows(i), :], relay_b.at[part_rows(i), :], rb_send_sem.at[i], rb_recv_sem.at[i])

    def hop_c(i):
        return remote(relay_b.at[part_rows(i), :], wo_peer.at[part_rows(i), :], rc_send_sem.at[i], wo_recv_sem.at[i], across)

    barrier = pltpu.get_barrier_semaphore()
    signal(barrier, peer)

    @pl.when(stage > 0)
    def _():
        signal(barrier, prv)

    @pl.when(jnp.logical_not(last))
    def _():
        signal(barrier, nxt)

    @pl.when(even)
    def _():
        signal(barrier, across)

    pl.semaphore_wait(barrier, 1 + (stage > 0).astype(jnp.int32) + (stage < n_stages - 1).astype(jnp.int32) + even.astype(jnp.int32))

    for t in range(half_q):
        send_x_in(jnp.int32(t))

    @pl.when(first)
    def _():
        for i in range(WO_PARTS):
            hop_a(i).start()

    @pl.when(third)
    def _():
        for i in range(WO_PARTS + 1):
            if i < WO_PARTS:
                hop_a(i).wait_recv()
                hop_b(i).start()
            if i > 0:
                hop_b(i - 1).wait_recv()
                hop_c(i - 1).start()

    @pl.when(jnp.logical_not(even))
    def _():
        scoped('go_wait', pl.semaphore_wait, go_sem, 1)

    bq_copy().start()
    wq_copy().start()

    @pl.when(jnp.logical_not(first))
    def _():
        for i in range(WO_PARTS):
            wo_copy(i).start()

    bq_all[pl.ds(0, heads_half)] = bq[...]
    vones[:, HEAD:] = jnp.ones((quarters * rows, HEAD), BF16)

    own_chunks = 1 + heads_half // 2
    zero = jnp.int32(0)
    for i in range(min(SLOTS, own_chunks)):
        start_chunk(zero, KVQ, jnp.int32(i))
    bq_copy().wait_recv()
    scoped('wq_wait', wq_copy().wait_recv)
    for i in range(min(SLOTS, own_chunks), SLOTS):
        start_chunk(zero, KVQ, jnp.int32(i))
    bq_copy().wait_send()
    wq_copy().wait_send()

    @pl.when(third)
    def _():
        for i in range(WO_PARTS):
            wo_copy(i).wait_send()

    @pl.when(even)
    def _():
        signal(go_sem, nxt)

    with jax.named_scope('wo_wait'):
        for i in range(WO_PARTS):
            wo_copy(i).wait_recv()
    wait_chunk(0)
    wait_chunk(1)

    def attention(j):
        factor = HEAD ** -0.5 * 1.4426950408889634

        def two_heads(jj, i):
            q = qbuf[pl.ds(2 * i, 2)].reshape(2 * rows, HEAD)
            sd = jnp.dot(q, kt[:, jj * rows:(jj + 1) * rows], preferred_element_type=F32)
            row = jnp.bitwise_and(lax.broadcasted_iota(jnp.int32, (2 * rows, rows), 0), rows - 1)
            col = lax.broadcasted_iota(jnp.int32, (2 * rows, rows), 1)
            sd = jnp.where(col <= row, sd, -1e30)
            top = jnp.max(sd, axis=-1, keepdims=True)
            if jj:
                so = jnp.dot(q, kt[:, :jj * rows], preferred_element_type=F32)
                top = jnp.maximum(top, jnp.max(so, axis=-1, keepdims=True))
            pd = jnp.exp2((sd - top) * factor).astype(BF16)
            acc = jnp.dot(pd, vones[jj * rows:(jj + 1) * rows, :], preferred_element_type=F32)
            if jj:
                po = jnp.exp2((so - top) * factor).astype(BF16)
                acc = acc + jnp.dot(po, vones[:jj * rows, :], preferred_element_type=F32)
            c = (acc[:, :HEAD] / acc[:, HEAD:]).astype(BF16)
            at = pl.multiple_of(i * 2 * HEAD, 2 * HEAD)
            cbuf[:, pl.ds(at, HEAD)] = c[:rows]
            cbuf[:, pl.ds(at + HEAD, HEAD)] = c[rows:]

        for jj in range(quarters):
            @pl.when(j == jj)
            def _():
                def body(i, carry):
                    two_heads(jj, i)
                    return carry

                lax.fori_loop(0, n_heads // 2, body, 0)

    def x1_copy(slot, start, width):
        cols = pl.ds(start, width)
        return remote(x1own.at[slot, :, cols], x1recv.at[slot, :, cols], x1_send_sem, x1_recv_sem.at[slot])

    def p_copy(slot, c):
        cols = pl.ds(pl.multiple_of(c * CW, CW), CW)
        return remote(psend.at[:, cols], precv.at[slot, :, cols], p_send_sem, p_recv_sem.at[slot])

    def attend(u):
        mb = u // quarters
        j = lax.rem(u, quarters)
        slot2 = lax.rem(u, 2)
        at_kvq = base(u, KVQ)
        at_o = base(u, O)
        send_x_in(u + half_q)
        local = first & (j // half_q == rank)

        @pl.when(local)
        def _():
            src = x_in.at[mb, rank, pl.ds(pl.multiple_of(lax.rem(j, half_q) * rows, rows), rows), :]
            pltpu.make_async_copy(src, xbuf, xload_sem).start()

        @pl.when(jnp.logical_not(local))
        def _():
            scoped('x_wait', remote(ybuf, x_recv.at[u], y_send_sem, xrecv_sem.at[u]).wait_recv)
            pltpu.make_async_copy(x_recv.at[u], xbuf, xload_sem).start()

        scoped('xload', pltpu.make_async_copy(x_recv.at[0], xbuf, xload_sem).wait)
        scoped('ln1', layer_norm, xbuf, hbuf, g1, s1)

        def q_heads(c, slot):
            a = jnp.dot(hbuf[...], ring[slot], preferred_element_type=F32)
            qbuf[2 * c] = (a[:, :HEAD] + bq_all[2 * c]).astype(BF16)
            qbuf[2 * c + 1] = (a[:, HEAD:] + bq_all[2 * c + 1]).astype(BF16)

        wait_chunk(at_kvq + 2)
        wait_chunk(at_kvq + 3)
        kv = jnp.dot(hbuf[...], ring[slot_at(at_kvq)], preferred_element_type=F32) + bkv[...]
        at = pl.ds(pl.multiple_of(j * rows, rows), rows)
        kt[:, at] = kv[:, :HEAD].astype(BF16).astype(F32).T.astype(BF16)
        vones[at, :HEAD] = kv[:, HEAD:].astype(BF16)
        q_heads(0, slot_at(at_kvq + 1))
        prefetch(u, KVQ, 0)
        prefetch(u, KVQ, 1)

        def q_body(i, carry):
            g = at_kvq + 2 * i
            wait_chunk(g + 2)
            wait_chunk(g + 3)
            q_heads(2 * i - 1, slot_at(g))
            q_heads(2 * i, slot_at(g + 1))
            prefetch(u, KVQ, 2 * i)
            prefetch(u, KVQ, 2 * i + 1)
            return carry

        scoped('q', lax.fori_loop, 1, (nq + 1) // 2, q_body, 0)
        scoped('attn', attention, j)

        @pl.when(u > 0)
        def _():
            remote(x1own.at[slot2], x1recv.at[slot2], x1_send_sem, x1_recv_sem.at[slot2]).wait_send()

        def o_cols(c, slot):
            cols = pl.ds(pl.multiple_of(c * CW, CW), CW)
            a = jnp.dot(cbuf[...], ring[slot], preferred_element_type=F32)
            x1own[slot2, :, cols] = (xbuf[:, cols].astype(F32) + a + bo[c]).astype(BF16)

        def o_body(i, carry):
            g = at_o + 2 * i
            wait_chunk(g + 2)
            wait_chunk(g + 3)
            o_cols(2 * i, slot_at(g))
            o_cols(2 * i + 1, slot_at(g + 1))

            @pl.when(i > 0)
            def _():
                x1_copy(slot2, pl.multiple_of((i - 1) * 2 * CW, CW), 2 * CW).start()

            prefetch(u, O, 2 * i)
            prefetch(u, O, 2 * i + 1)
            return carry

        scoped('o', lax.fori_loop, 0, nq // 2, o_body, 0)
        wait_chunk(at_o + nq + 1)
        o_cols(nq - 1, slot_at(at_o + nq - 1))
        prefetch(u, O, jnp.int32(nq - 1))
        tail = (nq // 2 - 1) * 2 * CW
        x1_copy(slot2, tail, hidden - tail).start()

    def down(u, v):
        slot2 = lax.rem(v, 2)
        nslot = lax.rem(u, 2)
        at_d = base(u, DOWN)
        steps = rows // LN_ROWS

        @pl.when(v > 0)
        def _():
            remote(psend, precv.at[slot2], p_send_sem, p_recv_sem.at[slot2]).wait_send()

        def body(c, carry):
            g = at_d + 2 * c

            @pl.when((u < n_units) | (c < nq - 1))
            def _():
                wait_chunk(g + 2)
                wait_chunk(g + 3)

            cols = pl.ds(pl.multiple_of(c * CW, CW), CW)
            a = (jnp.dot(ubuf[:, :hidden], ring[slot_at(g)], preferred_element_type=F32)
                 + jnp.dot(ubuf[:, hidden:], ring[slot_at(g + 1)], preferred_element_type=F32))
            for k in range(-(-steps // nq)):
                at = pl.ds(pl.multiple_of(jnp.minimum(c + k * nq, steps - 1) * LN_ROWS, LN_ROWS), LN_ROWS)
                ln_rows(x1own.at[nslot], h2buf, g2, s2, at, at)
            zbuf[:, cols] = x1own[slot2, :, cols].astype(F32) + a[:rows] + bdn[c]
            psend[:, cols] = a[rows:].astype(BF16)

            @pl.when(c > 0)
            def _():
                p_copy(slot2, c - 1).start()

            prefetch(u, DOWN, 2 * c)
            prefetch(u, DOWN, 2 * c + 1)
            return carry

        scoped('down', lax.fori_loop, 0, nq, body, 0)
        p_copy(slot2, nq - 1).start()

    def up(u):
        slot2 = lax.rem(u, 2)
        at_u = base(u, UP)
        scoped('x1_wait', remote(x1own.at[slot2], x1recv.at[slot2], x1_send_sem, x1_recv_sem.at[slot2]).wait_recv)
        scoped('ln_peer', layer_norm, x1recv.at[slot2], h2buf, g2, s2, rows)

        def cols_of(c, slot):
            a = jnp.dot(h2buf[...], ring[slot], preferred_element_type=F32) + bup[c]
            t = jnp.tanh(0.7978845608028654 * (a + 0.044715 * (a * a * a)))
            ubuf[:, pl.ds(pl.multiple_of(c * CW, CW), CW)] = (0.5 * a * (1.0 + t)).astype(BF16)

        def body(i, carry):
            g = at_u + 2 * i
            wait_chunk(g + 2)
            wait_chunk(g + 3)
            cols_of(2 * i, slot_at(g))
            cols_of(2 * i + 1, slot_at(g + 1))
            prefetch(u, UP, 2 * i)
            prefetch(u, UP, 2 * i + 1)
            return carry

        scoped('up', lax.fori_loop, 0, nu // 2, body, 0)

    def finish(v):
        slot = lax.rem(v, 2)
        mb = v // quarters
        j = lax.rem(v, quarters)
        scoped('p_wait', remote(psend, precv.at[slot], p_send_sem, p_recv_sem.at[slot]).wait_recv)

        @pl.when(v > 0)
        def _():
            scoped('y_wait', pltpu.make_async_copy(ybuf, x_recv.at[0], y_send_sem).wait)

        block = 32

        def body(i, carry):
            r = pl.ds(pl.multiple_of(i * block, block), block)
            ybuf[r, :] = (zbuf[r, :] + precv[slot, r, :].astype(F32)).astype(BF16)
            return carry

        lax.fori_loop(0, rows // block, body, 0)

        @pl.when(jnp.logical_not(last))
        def _():
            remote(ybuf, x_recv.at[v], y_send_sem, xrecv_sem.at[v], nxt).start()

        place = out.at[mb, rank, pl.ds(pl.multiple_of(lax.rem(j, half_q) * rows, rows), rows), :]

        @pl.when(last & (j // half_q == rank))
        def _():
            pltpu.make_async_copy(ybuf, place, y_send_sem).start()

        @pl.when(last & (j // half_q != rank))
        def _():
            remote(ybuf, place, y_send_sem, out_recv_sem.at[v]).start()

    def step(u, carry):
        @pl.when(u < n_units)
        def _():
            attend(u)

        @pl.when(u == 0)
        def _():
            layer_norm(x1own.at[0], h2buf, g2, s2)

        @pl.when(u > 0)
        def _():
            down(u, u - 1)

        @pl.when(u < n_units)
        def _():
            up(u)

        @pl.when(u > 0)
        def _():
            finish(u - 1)

        return carry

    lax.fori_loop(0, n_units + 1, step, 0)

    end = (n_units - 1) % 2
    remote(x1own.at[end], x1recv.at[end], x1_send_sem, x1_recv_sem.at[end]).wait_send()
    remote(psend, precv.at[end], p_send_sem, p_recv_sem.at[end]).wait_send()
    pltpu.make_async_copy(ybuf, x_recv.at[0], y_send_sem).wait()

    @pl.when(jnp.logical_not(third))
    def _():
        for i in range(WO_PARTS):
            wo_copy(i).wait_send()

    @pl.when(third)
    def _():
        for i in range(WO_PARTS):
            hop_b(i).wait_send()
            hop_c(i).wait_send()

    def drain(t, carry):
        j = lax.rem(t, quarters)
        mine = j // half_q == rank

        @pl.when(first & mine)
        def _():
            remote(ybuf, x_recv.at[t], xin_send_sem.at[t], xrecv_sem.at[t]).wait_send()

        @pl.when(last & mine)
        def _():
            place = out.at[t // quarters, 1 - rank, pl.ds(pl.multiple_of(lax.rem(j, half_q) * rows, rows), rows), :]
            remote(ybuf, place, y_send_sem, out_recv_sem.at[t]).wait_recv()

        return carry

    lax.fori_loop(0, n_units, drain, 0)


def run_stage(x_loc, params, n_stages):
    (ln1_gain, ln1_bias, w_q, b_q, w_kv, b_kv, w_o, b_o, ln2_gain, ln2_bias, w_up, b_up, w_down, b_down) = params
    n_micro, _, seq_loc, hidden = x_loc.shape
    ffn_loc = w_up.shape[2]
    rows = min(UNIT_ROWS, seq_loc // 2)
    quarters = 2 * seq_loc // rows
    n_units = n_micro * quarters
    nq = hidden // CW
    nu = ffn_loc // CW
    heads_half = hidden // 2 // HEAD
    cfg = (n_stages, n_units, quarters, rows, hidden, ffn_loc)
    vmem = pl.BlockSpec(memory_space=pltpu.VMEM)
    anym = pl.BlockSpec(memory_space=pl.ANY)
    args = (
        x_loc, ln1_gain, ln1_bias, w_q, b_q.reshape(heads_half, 1, HEAD), w_kv, b_kv, w_o, b_o.reshape(nq, 1, CW),
        ln2_gain, ln2_bias, w_up, b_up.reshape(nu, 1, CW), w_down, b_down.reshape(nq, 1, CW),
    )
    in_specs = [anym, vmem, vmem, anym, vmem, anym, vmem, anym, vmem, vmem, vmem, anym, vmem, anym, vmem]
    half = hidden // 2
    out_shape = (
        jax.ShapeDtypeStruct(x_loc.shape, BF16),
        jax.ShapeDtypeStruct((n_units, rows, hidden), BF16),
        jax.ShapeDtypeStruct((hidden, half), BF16),
        jax.ShapeDtypeStruct((half, hidden), BF16),
        jax.ShapeDtypeStruct((half, hidden), BF16),
        jax.ShapeDtypeStruct((half, hidden), BF16),
    )
    dma = pltpu.SemaphoreType.DMA
    scratch = [
        pltpu.VMEM((SLOTS, hidden, CW), BF16),
        pltpu.VMEM((rows, hidden), BF16),
        pltpu.VMEM((rows, hidden), BF16),
        pltpu.VMEM((2 * rows, hidden), BF16),
        pltpu.VMEM((2 * heads_half, rows, HEAD), BF16),
        pltpu.VMEM((rows, hidden), BF16),
        pltpu.VMEM((2, rows, hidden), BF16),
        pltpu.VMEM((2, rows, hidden), BF16),
        pltpu.VMEM((2 * rows, ffn_loc), BF16),
        pltpu.VMEM((rows, hidden), F32),
        pltpu.VMEM((rows, hidden), BF16),
        pltpu.VMEM((2, rows, hidden), BF16),
        pltpu.VMEM((rows, hidden), BF16),
        pltpu.VMEM((HEAD, quarters * rows), BF16),
        pltpu.VMEM((quarters * rows, 2 * HEAD), BF16),
        pltpu.VMEM((2 * heads_half, 1, HEAD), F32),
        dma((SLOTS,)),
        dma,
        dma((n_units,)),
        dma((n_units,)),
        dma((2,)),
        dma((2,)),
        dma((WO_PARTS,)),
        dma((WO_PARTS,)),
        dma((WO_PARTS,)),
        dma((WO_PARTS,)),
        dma((WO_PARTS,)),
        dma((WO_PARTS,)),
        dma,
        dma((2,)),
        dma,
        dma((2,)),
        dma,
        dma((n_units,)),
        pltpu.SemaphoreType.REGULAR,
    ]
    return pl.pallas_call(
        functools.partial(stage_kernel, cfg),
        out_shape=out_shape,
        in_specs=in_specs,
        out_specs=(anym,) * 6,
        scratch_shapes=scratch,
        compiler_params=pltpu.CompilerParams(collective_id=0, has_side_effects=True, vmem_limit_bytes=60 * 2 ** 20),
        name='stage_loop',
    )(*args)[0]


def solution(mesh):
    pp_size = mesh.shape['pp']

    def stage_program(x_loc, *params):
        result = run_stage(x_loc, params, pp_size)
        is_last = lax.axis_index('pp') == pp_size - 1
        return jnp.where(is_last, result, jnp.zeros_like(result))[None]

    return jax.shard_map(stage_program, mesh=mesh, in_specs=(P(None, 'dp', 'tp', None),) + PARAM_SPECS, out_specs=P('pp', None, 'dp', 'tp', None), check_vma=False)
```

```python
import functools

import jax
import jax.numpy as jnp
from jax import lax
from jax.experimental import pallas as pl
from jax.experimental.pallas import tpu as pltpu
from jax.sharding import PartitionSpec as P

F32 = jnp.float32
BF16 = jnp.bfloat16
MESH = pl.DeviceIdType.MESH

PARAM_SPECS = (P('pp', None), P('pp', None), P('pp', None, 'tp'), P('pp', 'tp'), P('pp', None, None), P('pp', None), P('pp', 'tp', None), P('pp', None), P('pp', None), P('pp', None), P('pp', None, 'tp'), P('pp', 'tp'), P('pp', 'tp', None), P('pp', None))

CW = 256
HEAD = 128
UNIT_ROWS = 256
SLOTS = 10
WO_PARTS = 4


def scoped(name, fn, *args):
    with jax.named_scope(name):
        return fn(*args)


def stage_kernel(cfg, x_in, g1, s1, wq, bq, wkv, bkv, wo, bo, g2, s2, wup, bup, wdn, bdn,
                 out, x_recv, wq_peer, wo_peer, relay_a, relay_b,
                 ring, xbuf, hbuf, h2buf, qbuf, cbuf, x1own, x1recv, ubuf, zbuf, psend, precv, ybuf, kt, vones, bq_all,
                 ring_sem, xload_sem, xrecv_sem, xin_send_sem, w_send_sem, w_recv_sem, wo_send_sem, wo_recv_sem,
                 ra_recv_sem, rb_send_sem, rb_recv_sem, rc_send_sem,
                 x1_send_sem, x1_recv_sem, p_send_sem, p_recv_sem, y_send_sem, out_recv_sem, go_sem):
    (n_stages, n_units, quarters, rows, hidden, ffn_loc) = cfg
    half_q = quarters // 2
    half = hidden // 2
    nq = hidden // CW
    nu = ffn_loc // CW
    heads_half = half // HEAD
    n_heads = 2 * heads_half
    stage = lax.axis_index('pp')
    rank = lax.axis_index('tp')
    peer = {'tp': 1 - rank}
    nxt = {'pp': jnp.minimum(stage + 1, n_stages - 1)}
    prv = {'pp': jnp.maximum(stage - 1, 0)}
    across = {'pp': 4 - stage}
    first = stage == 0
    second = stage == 1
    last = stage == n_stages - 1
    even = lax.rem(stage, 2) == 0

    KVQ, O, UP, UP2, DOWN = 0, 1, 2, 3, 4
    counts = (1 + nq, nq, nu, nu, 2 * nq)
    total = sum(counts)

    def base(u, phase):
        return u * total + sum(counts[:phase])

    def slot_at(g):
        return lax.rem(g, SLOTS)

    def start_chunk(u, phase, idx):
        slot = slot_at(base(u, phase) + idx)
        dst = ring.at[slot]
        sem = ring_sem.at[slot]

        def cols(c, width):
            return pl.ds(pl.multiple_of(c * width, width), width)

        if phase == KVQ:
            @pl.when(idx == 0)
            def _():
                pltpu.make_async_copy(wkv.at[0], dst, sem).start()

            for b in range(2):
                block = (idx - 1) * 2 + b
                piece = dst.at[:, pl.ds(b * HEAD, HEAD)]

                @pl.when((idx > 0) & (block < heads_half))
                def _():
                    pltpu.make_async_copy(wq.at[0, :, cols(block, HEAD)], piece, sem).start()

                @pl.when((idx > 0) & (block >= heads_half))
                def _():
                    pltpu.make_async_copy(wq_peer.at[:, cols(block - heads_half, HEAD)], piece, sem).start()
        elif phase == O:
            pltpu.make_async_copy(wo.at[0, :, cols(idx, CW)], dst.at[pl.ds(0, half), :], sem).start()
            pltpu.make_async_copy(wo_peer.at[:, cols(idx, CW)], dst.at[pl.ds(half, half), :], sem).start()
        elif phase in (UP, UP2):
            pltpu.make_async_copy(wup.at[0, :, cols(idx, CW)], dst, sem).start()
        else:
            part = lax.rem(idx, 2)
            pltpu.make_async_copy(
                wdn.at[0, pl.ds(pl.multiple_of(part * hidden, hidden), hidden), cols(idx // 2, CW)], dst, sem).start()

    def prefetch(u, phase, idx):
        ahead = idx + SLOTS
        n = counts[phase]

        @pl.when(ahead < n)
        def _():
            start_chunk(u, phase, ahead)

        if phase == DOWN:
            @pl.when((ahead >= n) & (u + 1 < n_units))
            def _():
                start_chunk(u + 1, KVQ, ahead - n)
        else:
            @pl.when(ahead >= n)
            def _():
                start_chunk(u, phase + 1, ahead - n)

    def wait_chunk(g):
        slot = slot_at(g)
        pltpu.make_async_copy(wkv.at[0], ring.at[slot], ring_sem.at[slot]).wait()

    def layer_norm(src, dst, gain, shift, row0=0, block=32):
        def body(i, carry):
            at = pl.multiple_of(i * block, block)
            v = src[pl.ds(at, block), :].astype(F32)
            mean = jnp.mean(v, axis=-1, keepdims=True)
            cen = v - mean
            var = jnp.mean(cen * cen, axis=-1, keepdims=True)
            dst[pl.ds(row0 + at, block), :] = (cen * lax.rsqrt(var + 1e-5) * gain[...] + shift[...]).astype(BF16)
            return carry

        lax.fori_loop(0, rows // block, body, 0)

    def layer_norm_cols(src, dst, gain, shift, row0=0, block=64):
        pieces = [pl.ds(k * CW, CW) for k in range(hidden // CW)]

        def body(i, carry):
            at = pl.multiple_of(i * block, block)
            r = pl.ds(at, block)
            total = src[r, pieces[0]].astype(F32)
            for p in pieces[1:]:
                total = total + src[r, p].astype(F32)
            mean = jnp.sum(total, axis=-1, keepdims=True) * (1.0 / hidden)
            square = None
            for p in pieces:
                cen = src[r, p].astype(F32) - mean
                square = cen * cen if square is None else square + cen * cen
            inv = lax.rsqrt(jnp.sum(square, axis=-1, keepdims=True) * (1.0 / hidden) + 1e-5)
            for p in pieces:
                cen = src[r, p].astype(F32) - mean
                dst[pl.ds(row0 + at, block), p] = (cen * inv * gain[:, p] + shift[:, p]).astype(BF16)
            return carry

        lax.fori_loop(0, rows // block, body, 0)

    def send_x_in(t):
        mb = t // quarters
        j = lax.rem(t, quarters)

        @pl.when(first & (t < n_units) & (j // half_q == rank))
        def _():
            src = x_in.at[mb, 1 - rank, pl.ds(pl.multiple_of(lax.rem(j, half_q) * rows, rows), rows), :]
            remote(src, x_recv.at[t], xin_send_sem.at[t], xrecv_sem.at[t]).start()

    def remote(src, dst, send_sem, recv_sem, to=peer):
        return pltpu.make_async_remote_copy(src, dst, send_sem, recv_sem, device_id=to, device_id_type=MESH)

    def signal(sem, to):
        pl.semaphore_signal(sem, inc=1, device_id=to, device_id_type=MESH)

    def wq_copy():
        return remote(wq.at[0], wq_peer, w_send_sem.at[0], w_recv_sem.at[0])

    def bq_copy():
        return remote(bq, bq_all.at[pl.ds(heads_half, heads_half)], w_send_sem.at[1], w_recv_sem.at[1])

    def part_rows(i):
        return pl.ds(i * (half // WO_PARTS), half // WO_PARTS)

    def wo_copy(i):
        return remote(wo.at[0, part_rows(i), :], wo_peer.at[part_rows(i), :], wo_send_sem.at[i], wo_recv_sem.at[i])

    def hop_a(i):
        return remote(wo.at[0, part_rows(i), :], relay_a.at[part_rows(i), :], wo_send_sem.at[i], ra_recv_sem.at[i], across)

    def hop_b(i):
        return remote(relay_a.at[part_rows(i), :], relay_b.at[part_rows(i), :], rb_send_sem.at[i], rb_recv_sem.at[i])

    def hop_c(i):
        return remote(relay_b.at[part_rows(i), :], wo_peer.at[part_rows(i), :], rc_send_sem.at[i], wo_recv_sem.at[i], across)

    barrier = pltpu.get_barrier_semaphore()
    signal(barrier, peer)

    @pl.when(stage > 0)
    def _():
        signal(barrier, prv)

    @pl.when(jnp.logical_not(last))
    def _():
        signal(barrier, nxt)

    @pl.when(jnp.logical_not(even))
    def _():
        signal(barrier, across)

    pl.semaphore_wait(barrier, 1 + (stage > 0).astype(jnp.int32) + (stage < n_stages - 1).astype(jnp.int32) + 1 - even.astype(jnp.int32))

    @pl.when(second)
    def _():
        for i in range(WO_PARTS):
            hop_a(i).start()

    @pl.when(last)
    def _():
        for i in range(WO_PARTS + 1):
            if i < WO_PARTS:
                hop_a(i).wait_recv()
                hop_b(i).start()
            if i > 0:
                hop_b(i - 1).wait_recv()
                hop_c(i - 1).start()

    @pl.when(second)
    def _():
        scoped('go_wait', pl.semaphore_wait, go_sem, 1)

    bq_copy().start()
    wq_copy().start()
    send_x_in(jnp.int32(0))

    @pl.when(jnp.logical_not(second))
    def _():
        for i in range(WO_PARTS):
            wo_copy(i).start()

    for t in range(1, half_q):
        send_x_in(jnp.int32(t))

    bq_all[pl.ds(0, heads_half)] = bq[...]
    vones[:, HEAD:] = jnp.ones((quarters * rows, HEAD), BF16)

    own_chunks = 1 + heads_half // 2
    zero = jnp.int32(0)
    for i in range(min(SLOTS, own_chunks)):
        start_chunk(zero, KVQ, jnp.int32(i))
    bq_copy().wait_recv()
    scoped('wq_wait', wq_copy().wait_recv)
    for i in range(min(SLOTS, own_chunks), SLOTS):
        start_chunk(zero, KVQ, jnp.int32(i))
    bq_copy().wait_send()
    wq_copy().wait_send()

    @pl.when(first)
    def _():
        for i in range(WO_PARTS):
            wo_copy(i).wait_send()
        signal(go_sem, nxt)

    with jax.named_scope('wo_wait'):
        for i in range(WO_PARTS):
            wo_copy(i).wait_recv()
    wait_chunk(0)
    wait_chunk(1)

    def attention(j):
        factor = HEAD ** -0.5 * 1.4426950408889634

        def two_heads(jj, i):
            q = qbuf[pl.ds(2 * i, 2)].reshape(2 * rows, HEAD)
            sd = jnp.dot(q, kt[:, jj * rows:(jj + 1) * rows], preferred_element_type=F32)
            row = jnp.bitwise_and(lax.broadcasted_iota(jnp.int32, (2 * rows, rows), 0), rows - 1)
            col = lax.broadcasted_iota(jnp.int32, (2 * rows, rows), 1)
            sd = jnp.where(col <= row, sd, -1e30)
            top = jnp.max(sd, axis=-1, keepdims=True)
            if jj:
                so = jnp.dot(q, kt[:, :jj * rows], preferred_element_type=F32)
                top = jnp.maximum(top, jnp.max(so, axis=-1, keepdims=True))
            pd = jnp.exp2((sd - top) * factor).astype(BF16)
            acc = jnp.dot(pd, vones[jj * rows:(jj + 1) * rows, :], preferred_element_type=F32)
            if jj:
                po = jnp.exp2((so - top) * factor).astype(BF16)
                acc = acc + jnp.dot(po, vones[:jj * rows, :], preferred_element_type=F32)
            c = (acc[:, :HEAD] / acc[:, HEAD:]).astype(BF16)
            at = pl.multiple_of(i * 2 * HEAD, 2 * HEAD)
            cbuf[:, pl.ds(at, HEAD)] = c[:rows]
            cbuf[:, pl.ds(at + HEAD, HEAD)] = c[rows:]

        for jj in range(quarters):
            @pl.when(j == jj)
            def _():
                def body(i, carry):
                    two_heads(jj, i)
                    return carry

                lax.fori_loop(0, n_heads // 2, body, 0)

    def x1_copy(slot, start, width):
        cols = pl.ds(start, width)
        return remote(x1own.at[slot, :, cols], x1recv.at[slot, :, cols], x1_send_sem, x1_recv_sem.at[slot])

    def p_copy(slot, c):
        cols = pl.ds(pl.multiple_of(c * CW, CW), CW)
        return remote(psend.at[:, cols], precv.at[slot, :, cols], p_send_sem, p_recv_sem.at[slot])

    def attend(u):
        mb = u // quarters
        j = lax.rem(u, quarters)
        slot2 = lax.rem(u, 2)
        at_kvq = base(u, KVQ)
        at_o = base(u, O)
        send_x_in(u + half_q)
        local = first & (j // half_q == rank)

        @pl.when(local)
        def _():
            src = x_in.at[mb, rank, pl.ds(pl.multiple_of(lax.rem(j, half_q) * rows, rows), rows), :]
            pltpu.make_async_copy(src, xbuf, xload_sem).start()

        @pl.when(jnp.logical_not(local))
        def _():
            scoped('x_wait', remote(ybuf, x_recv.at[u], y_send_sem, xrecv_sem.at[u]).wait_recv)
            pltpu.make_async_copy(x_recv.at[u], xbuf, xload_sem).start()

        scoped('xload', pltpu.make_async_copy(x_recv.at[0], xbuf, xload_sem).wait)
        scoped('ln1', layer_norm, xbuf, hbuf, g1, s1, 0, 16)

        def q_heads(c, slot):
            a = jnp.dot(hbuf[...], ring[slot], preferred_element_type=F32)
            qbuf[2 * c] = (a[:, :HEAD] + bq_all[2 * c]).astype(BF16)
            qbuf[2 * c + 1] = (a[:, HEAD:] + bq_all[2 * c + 1]).astype(BF16)

        wait_chunk(at_kvq + 2)
        wait_chunk(at_kvq + 3)
        kv = jnp.dot(hbuf[...], ring[slot_at(at_kvq)], preferred_element_type=F32) + bkv[...]
        at = pl.ds(pl.multiple_of(j * rows, rows), rows)
        kt[:, at] = kv[:, :HEAD].astype(BF16).astype(F32).T.astype(BF16)
        vones[at, :HEAD] = kv[:, HEAD:].astype(BF16)
        q_heads(0, slot_at(at_kvq + 1))
        prefetch(u, KVQ, 0)
        prefetch(u, KVQ, 1)

        def q_body(i, carry):
            g = at_kvq + 2 * i
            wait_chunk(g + 2)
            wait_chunk(g + 3)
            q_heads(2 * i - 1, slot_at(g))
            q_heads(2 * i, slot_at(g + 1))
            prefetch(u, KVQ, 2 * i)
            prefetch(u, KVQ, 2 * i + 1)
            return carry

        scoped('q', lax.fori_loop, 1, (nq + 1) // 2, q_body, 0)

        @pl.when(u > 0)
        def _():
            finish(u - 1)

        scoped('attn', attention, j)

        @pl.when(u > 0)
        def _():
            remote(x1own.at[slot2], x1recv.at[slot2], x1_send_sem, x1_recv_sem.at[slot2]).wait_send()

        def o_cols(c, slot):
            cols = pl.ds(pl.multiple_of(c * CW, CW), CW)
            a = jnp.dot(cbuf[...], ring[slot], preferred_element_type=F32)
            x1own[slot2, :, cols] = (xbuf[:, cols].astype(F32) + a + bo[c]).astype(BF16)

        def o_body(i, carry):
            g = at_o + 2 * i
            wait_chunk(g + 2)
            wait_chunk(g + 3)
            o_cols(2 * i, slot_at(g))
            o_cols(2 * i + 1, slot_at(g + 1))

            @pl.when(i > 0)
            def _():
                x1_copy(slot2, pl.multiple_of((i - 1) * 2 * CW, CW), 2 * CW).start()

            prefetch(u, O, 2 * i)
            prefetch(u, O, 2 * i + 1)
            return carry

        scoped('o', lax.fori_loop, 0, nq // 2, o_body, 0)
        wait_chunk(at_o + nq + 1)
        o_cols(nq - 1, slot_at(at_o + nq - 1))
        prefetch(u, O, jnp.int32(nq - 1))
        tail = (nq // 2 - 1) * 2 * CW
        x1_copy(slot2, tail, hidden - tail).start()

    def down(u):
        slot2 = lax.rem(u, 2)
        at_d = base(u, DOWN)

        @pl.when(u > 0)
        def _():
            remote(psend, precv.at[slot2], p_send_sem, p_recv_sem.at[slot2]).wait_send()

        def body(c, carry):
            g = at_d + 2 * c

            @pl.when((u + 1 < n_units) | (c < nq - 1))
            def _():
                wait_chunk(g + 2)
                wait_chunk(g + 3)

            cols = pl.ds(pl.multiple_of(c * CW, CW), CW)
            a = (jnp.dot(ubuf[:, :hidden], ring[slot_at(g)], preferred_element_type=F32)
                 + jnp.dot(ubuf[:, hidden:], ring[slot_at(g + 1)], preferred_element_type=F32))
            zbuf[:, cols] = x1own[slot2, :, cols].astype(F32) + a[:rows] + bdn[c]
            psend[:, cols] = a[rows:].astype(BF16)

            @pl.when(c > 0)
            def _():
                p_copy(slot2, c - 1).start()

            prefetch(u, DOWN, 2 * c)
            prefetch(u, DOWN, 2 * c + 1)
            return carry

        scoped('down', lax.fori_loop, 0, nq, body, 0)
        p_copy(slot2, nq - 1).start()

    def up(u, phase, row0):
        at_u = base(u, phase)

        def cols_of(c, slot):
            a = jnp.dot(h2buf[pl.ds(row0, rows), :], ring[slot], preferred_element_type=F32) + bup[c]
            t = jnp.tanh(0.7978845608028654 * (a + 0.044715 * (a * a * a)))
            ubuf[pl.ds(row0, rows), pl.ds(pl.multiple_of(c * CW, CW), CW)] = (0.5 * a * (1.0 + t)).astype(BF16)

        def body(i, carry):
            g = at_u + 2 * i
            wait_chunk(g + 2)
            wait_chunk(g + 3)
            cols_of(2 * i, slot_at(g))
            cols_of(2 * i + 1, slot_at(g + 1))
            prefetch(u, phase, 2 * i)
            prefetch(u, phase, 2 * i + 1)
            return carry

        scoped('up', lax.fori_loop, 0, nu // 2, body, 0)

    def finish(v):
        slot = lax.rem(v, 2)
        mb = v // quarters
        j = lax.rem(v, quarters)
        scoped('p_wait', remote(psend, precv.at[slot], p_send_sem, p_recv_sem.at[slot]).wait_recv)

        @pl.when(v > 0)
        def _():
            scoped('y_wait', pltpu.make_async_copy(ybuf, x_recv.at[0], y_send_sem).wait)

        block = 32

        def body(i, carry):
            r = pl.ds(pl.multiple_of(i * block, block), block)
            ybuf[r, :] = (zbuf[r, :] + precv[slot, r, :].astype(F32)).astype(BF16)
            return carry

        lax.fori_loop(0, rows // block, body, 0)

        @pl.when(jnp.logical_not(last))
        def _():
            remote(ybuf, x_recv.at[v], y_send_sem, xrecv_sem.at[v], nxt).start()

        place = out.at[mb, rank, pl.ds(pl.multiple_of(lax.rem(j, half_q) * rows, rows), rows), :]

        @pl.when(last & (j // half_q == rank))
        def _():
            pltpu.make_async_copy(ybuf, place, y_send_sem).start()

        @pl.when(last & (j // half_q != rank))
        def _():
            remote(ybuf, place, y_send_sem, out_recv_sem.at[v]).start()

    def step(u, carry):
        slot2 = lax.rem(u, 2)
        attend(u)
        scoped('ln2', layer_norm_cols, x1own.at[slot2], h2buf, g2, s2)
        up(u, UP, 0)
        scoped('x1_wait', remote(x1own.at[slot2], x1recv.at[slot2], x1_send_sem, x1_recv_sem.at[slot2]).wait_recv)
        scoped('ln_peer', layer_norm, x1recv.at[slot2], h2buf, g2, s2, rows)
        up(u, UP2, rows)
        down(u)
        return carry

    lax.fori_loop(0, n_units, step, 0)
    finish(jnp.int32(n_units - 1))

    end = (n_units - 1) % 2
    remote(x1own.at[end], x1recv.at[end], x1_send_sem, x1_recv_sem.at[end]).wait_send()
    remote(psend, precv.at[end], p_send_sem, p_recv_sem.at[end]).wait_send()
    pltpu.make_async_copy(ybuf, x_recv.at[0], y_send_sem).wait()

    @pl.when(jnp.logical_not(first))
    def _():
        for i in range(WO_PARTS):
            wo_copy(i).wait_send()

    @pl.when(last)
    def _():
        for i in range(WO_PARTS):
            hop_b(i).wait_send()
            hop_c(i).wait_send()

    def drain(t, carry):
        j = lax.rem(t, quarters)
        mine = j // half_q == rank

        @pl.when(first & mine)
        def _():
            remote(ybuf, x_recv.at[t], xin_send_sem.at[t], xrecv_sem.at[t]).wait_send()

        @pl.when(last & mine)
        def _():
            place = out.at[t // quarters, 1 - rank, pl.ds(pl.multiple_of(lax.rem(j, half_q) * rows, rows), rows), :]
            remote(ybuf, place, y_send_sem, out_recv_sem.at[t]).wait_recv()

        return carry

    lax.fori_loop(0, n_units, drain, 0)


def run_stage(x_loc, params, n_stages):
    (ln1_gain, ln1_bias, w_q, b_q, w_kv, b_kv, w_o, b_o, ln2_gain, ln2_bias, w_up, b_up, w_down, b_down) = params
    n_micro, _, seq_loc, hidden = x_loc.shape
    ffn_loc = w_up.shape[2]
    rows = min(UNIT_ROWS, seq_loc // 2)
    quarters = 2 * seq_loc // rows
    n_units = n_micro * quarters
    nq = hidden // CW
    nu = ffn_loc // CW
    heads_half = hidden // 2 // HEAD
    cfg = (n_stages, n_units, quarters, rows, hidden, ffn_loc)
    vmem = pl.BlockSpec(memory_space=pltpu.VMEM)
    anym = pl.BlockSpec(memory_space=pl.ANY)
    args = (
        x_loc, ln1_gain, ln1_bias, w_q, b_q.reshape(heads_half, 1, HEAD), w_kv, b_kv, w_o, b_o.reshape(nq, 1, CW),
        ln2_gain, ln2_bias, w_up, b_up.reshape(nu, 1, CW), w_down, b_down.reshape(nq, 1, CW),
    )
    in_specs = [anym, vmem, vmem, anym, vmem, anym, vmem, anym, vmem, vmem, vmem, anym, vmem, anym, vmem]
    half = hidden // 2
    out_shape = (
        jax.ShapeDtypeStruct(x_loc.shape, BF16),
        jax.ShapeDtypeStruct((n_units, rows, hidden), BF16),
        jax.ShapeDtypeStruct((hidden, half), BF16),
        jax.ShapeDtypeStruct((half, hidden), BF16),
        jax.ShapeDtypeStruct((half, hidden), BF16),
        jax.ShapeDtypeStruct((half, hidden), BF16),
    )
    dma = pltpu.SemaphoreType.DMA
    scratch = [
        pltpu.VMEM((SLOTS, hidden, CW), BF16),
        pltpu.VMEM((rows, hidden), BF16),
        pltpu.VMEM((rows, hidden), BF16),
        pltpu.VMEM((2 * rows, hidden), BF16),
        pltpu.VMEM((2 * heads_half, rows, HEAD), BF16),
        pltpu.VMEM((rows, hidden), BF16),
        pltpu.VMEM((2, rows, hidden), BF16),
        pltpu.VMEM((2, rows, hidden), BF16),
        pltpu.VMEM((2 * rows, ffn_loc), BF16),
        pltpu.VMEM((rows, hidden), F32),
        pltpu.VMEM((rows, hidden), BF16),
        pltpu.VMEM((2, rows, hidden), BF16),
        pltpu.VMEM((rows, hidden), BF16),
        pltpu.VMEM((HEAD, quarters * rows), BF16),
        pltpu.VMEM((quarters * rows, 2 * HEAD), BF16),
        pltpu.VMEM((2 * heads_half, 1, HEAD), F32),
        dma((SLOTS,)),
        dma,
        dma((n_units,)),
        dma((n_units,)),
        dma((2,)),
        dma((2,)),
        dma((WO_PARTS,)),
        dma((WO_PARTS,)),
        dma((WO_PARTS,)),
        dma((WO_PARTS,)),
        dma((WO_PARTS,)),
        dma((WO_PARTS,)),
        dma,
        dma((2,)),
        dma,
        dma((2,)),
        dma,
        dma((n_units,)),
        pltpu.SemaphoreType.REGULAR,
    ]
    return pl.pallas_call(
        functools.partial(stage_kernel, cfg),
        out_shape=out_shape,
        in_specs=in_specs,
        out_specs=(anym,) * 6,
        scratch_shapes=scratch,
        compiler_params=pltpu.CompilerParams(collective_id=0, has_side_effects=True, vmem_limit_bytes=60 * 2 ** 20),
        name='stage_loop',
    )(*args)[0]


def solution(mesh):
    pp_size = mesh.shape['pp']

    def stage_program(x_loc, *params):
        result = run_stage(x_loc, params, pp_size)
        is_last = lax.axis_index('pp') == pp_size - 1
        return jnp.where(is_last, result, jnp.zeros_like(result))[None]

    return jax.shard_map(stage_program, mesh=mesh, in_specs=(P(None, 'dp', 'tp', None),) + PARAM_SPECS, out_specs=P('pp', None, 'dp', 'tp', None), check_vma=False)
```

```python
import functools

import jax
import jax.numpy as jnp
from jax import lax
from jax.experimental import pallas as pl
from jax.experimental.pallas import tpu as pltpu
from jax.sharding import PartitionSpec as P

F32 = jnp.float32
BF16 = jnp.bfloat16
MESH = pl.DeviceIdType.MESH

PARAM_SPECS = (P('pp', None), P('pp', None), P('pp', None, 'tp'), P('pp', 'tp'), P('pp', None, None), P('pp', None), P('pp', 'tp', None), P('pp', None), P('pp', None), P('pp', None), P('pp', None, 'tp'), P('pp', 'tp'), P('pp', 'tp', None), P('pp', None))

CW = 256
HEAD = 128
UNIT_ROWS = 256
SLOTS = 10
WO_PARTS = 4


def scoped(name, fn, *args):
    with jax.named_scope(name):
        return fn(*args)


def stage_kernel(cfg, x_in, g1, s1, wq, bq, wkv, bkv, wo, bo, g2, s2, wup, bup, wdn, bdn,
                 out, x_recv, wq_peer, wo_peer, relay_a, relay_b,
                 ring, xbuf, hbuf, qbuf, cbuf, x1own, x1recv, ubuf, zbuf, psend, precv, ybuf, kt, vones, bq_all,
                 ring_sem, xload_sem, xslot_sem, xrecv_sem, xin_send_sem, w_send_sem, w_recv_sem, wo_send_sem, wo_recv_sem,
                 ra_recv_sem, rb_send_sem, rb_recv_sem, rc_send_sem,
                 x1_send_sem, x1_recv_sem, p_send_sem, p_recv_sem, y_send_sem, out_recv_sem, go_sem, credit_sem):
    (n_stages, n_units, quarters, rows, hidden, ffn_loc) = cfg
    half_q = quarters // 2
    half = hidden // 2
    nq = hidden // CW
    nu = ffn_loc // CW
    heads_half = half // HEAD
    n_heads = 2 * heads_half
    stage = lax.axis_index('pp')
    rank = lax.axis_index('tp')
    peer = {'tp': 1 - rank}
    nxt = {'pp': jnp.minimum(stage + 1, n_stages - 1)}
    prv = {'pp': jnp.maximum(stage - 1, 0)}
    across = {'pp': 4 - stage}
    first = stage == 0
    second = stage == 1
    last = stage == n_stages - 1
    even = lax.rem(stage, 2) == 0

    KVQ, O, UP, DOWN, UP2, DOWN2 = 0, 1, 2, 3, 4, 5
    counts = (1 + nq, nq, nu, 2 * nq, nu, 2 * nq)
    total = sum(counts)

    def base(u, phase):
        return u * total + sum(counts[:phase])

    def slot_at(g):
        return lax.rem(g, SLOTS)

    def start_chunk(u, phase, idx):
        slot = slot_at(base(u, phase) + idx)
        dst = ring.at[slot]
        sem = ring_sem.at[slot]

        def cols(c, width):
            return pl.ds(pl.multiple_of(c * width, width), width)

        if phase == KVQ:
            @pl.when(idx == 0)
            def _():
                pltpu.make_async_copy(wkv.at[0], dst, sem).start()

            for b in range(2):
                block = (idx - 1) * 2 + b
                piece = dst.at[:, pl.ds(b * HEAD, HEAD)]

                @pl.when((idx > 0) & (block < heads_half))
                def _():
                    pltpu.make_async_copy(wq.at[0, :, cols(block, HEAD)], piece, sem).start()

                @pl.when((idx > 0) & (block >= heads_half))
                def _():
                    pltpu.make_async_copy(wq_peer.at[:, cols(block - heads_half, HEAD)], piece, sem).start()
        elif phase == O:
            pltpu.make_async_copy(wo.at[0, :, cols(idx, CW)], dst.at[pl.ds(0, half), :], sem).start()
            pltpu.make_async_copy(wo_peer.at[:, cols(idx, CW)], dst.at[pl.ds(half, half), :], sem).start()
        elif phase in (UP, UP2):
            pltpu.make_async_copy(wup.at[0, :, cols(idx, CW)], dst, sem).start()
        else:
            part = lax.rem(idx, 2)
            pltpu.make_async_copy(
                wdn.at[0, pl.ds(pl.multiple_of(part * hidden, hidden), hidden), cols(idx // 2, CW)], dst, sem).start()

    def prefetch(u, phase, idx):
        ahead = idx + SLOTS
        n = counts[phase]

        @pl.when(ahead < n)
        def _():
            start_chunk(u, phase, ahead)

        if phase == DOWN2:
            @pl.when((ahead >= n) & (u + 1 < n_units))
            def _():
                start_chunk(u + 1, KVQ, ahead - n)
        else:
            @pl.when(ahead >= n)
            def _():
                start_chunk(u, phase + 1, ahead - n)

    def wait_chunk(g):
        slot = slot_at(g)
        pltpu.make_async_copy(wkv.at[0], ring.at[slot], ring_sem.at[slot]).wait()

    def layer_norm(src, dst, gain, shift, block=64):
        pieces = [pl.ds(k * CW, CW) for k in range(hidden // CW)]

        def body(i, carry):
            at = pl.multiple_of(i * block, block)
            r = pl.ds(at, block)
            total = src[r, pieces[0]].astype(F32)
            for p in pieces[1:]:
                total = total + src[r, p].astype(F32)
            mean = jnp.sum(total, axis=-1, keepdims=True) * (1.0 / hidden)
            square = None
            for p in pieces:
                cen = src[r, p].astype(F32) - mean
                square = cen * cen if square is None else square + cen * cen
            inv = lax.rsqrt(jnp.sum(square, axis=-1, keepdims=True) * (1.0 / hidden) + 1e-5)
            for p in pieces:
                cen = src[r, p].astype(F32) - mean
                dst[r, p] = (cen * inv * gain[:, p] + shift[:, p]).astype(BF16)
            return carry

        lax.fori_loop(0, rows // block, body, 0)

    def send_x_in(t):
        mb = t // quarters
        j = lax.rem(t, quarters)

        @pl.when(first & (t < n_units) & (j // half_q == rank))
        def _():
            src = x_in.at[mb, 1 - rank, pl.ds(pl.multiple_of(lax.rem(j, half_q) * rows, rows), rows), :]
            remote(src, x_recv.at[t], xin_send_sem.at[t], xrecv_sem.at[t]).start()

    def load_x(t):
        mb = t // quarters
        j = lax.rem(t, quarters)
        local = j // half_q == rank

        @pl.when(first & (t < n_units) & local)
        def _():
            src = x_in.at[mb, rank, pl.ds(pl.multiple_of(lax.rem(j, half_q) * rows, rows), rows), :]
            pltpu.make_async_copy(src, xbuf.at[lax.rem(t, 2)], xload_sem).start()

        @pl.when(first & (t < n_units) & jnp.logical_not(local))
        def _():
            remote(ybuf, x_recv.at[t], y_send_sem, xrecv_sem.at[t]).wait_recv()
            pltpu.make_async_copy(x_recv.at[t], xbuf.at[lax.rem(t, 2)], xload_sem).start()

    def remote(src, dst, send_sem, recv_sem, to=peer):
        return pltpu.make_async_remote_copy(src, dst, send_sem, recv_sem, device_id=to, device_id_type=MESH)

    def signal(sem, to):
        pl.semaphore_signal(sem, inc=1, device_id=to, device_id_type=MESH)

    def wq_copy():
        return remote(wq.at[0], wq_peer, w_send_sem.at[0], w_recv_sem.at[0])

    def bq_copy():
        return remote(bq, bq_all.at[pl.ds(heads_half, heads_half)], w_send_sem.at[1], w_recv_sem.at[1])

    def part_rows(i):
        return pl.ds(i * (half // WO_PARTS), half // WO_PARTS)

    def wo_copy(i):
        return remote(wo.at[0, part_rows(i), :], wo_peer.at[part_rows(i), :], wo_send_sem.at[i], wo_recv_sem.at[i])

    def hop_a(i):
        return remote(wo.at[0, part_rows(i), :], relay_a.at[part_rows(i), :], wo_send_sem.at[i], ra_recv_sem.at[i], across)

    def hop_b(i):
        return remote(relay_a.at[part_rows(i), :], relay_b.at[part_rows(i), :], rb_send_sem.at[i], rb_recv_sem.at[i])

    def hop_c(i):
        return remote(relay_b.at[part_rows(i), :], wo_peer.at[part_rows(i), :], rc_send_sem.at[i], wo_recv_sem.at[i], across)

    barrier = pltpu.get_barrier_semaphore()
    signal(barrier, peer)

    @pl.when(stage > 0)
    def _():
        signal(barrier, prv)

    @pl.when(jnp.logical_not(last))
    def _():
        signal(barrier, nxt)

    @pl.when(jnp.logical_not(even))
    def _():
        signal(barrier, across)

    pl.semaphore_wait(barrier, 1 + (stage > 0).astype(jnp.int32) + (stage < n_stages - 1).astype(jnp.int32) + 1 - even.astype(jnp.int32))

    @pl.when(second)
    def _():
        for i in range(WO_PARTS):
            hop_a(i).start()

    @pl.when(last)
    def _():
        for i in range(WO_PARTS + 1):
            if i < WO_PARTS:
                hop_a(i).wait_recv()
                hop_b(i).start()
            if i > 0:
                hop_b(i - 1).wait_recv()
                hop_c(i - 1).start()

    @pl.when(second)
    def _():
        scoped('go_wait', pl.semaphore_wait, go_sem, 1)

    bq_copy().start()
    wq_copy().start()
    send_x_in(jnp.int32(0))

    @pl.when(jnp.logical_not(second))
    def _():
        for i in range(WO_PARTS):
            wo_copy(i).start()

    for t in range(1, half_q):
        send_x_in(jnp.int32(t))

    bq_all[pl.ds(0, heads_half)] = bq[...]
    vones[:, HEAD:] = jnp.ones((quarters * rows, HEAD), BF16)

    own_chunks = 1 + heads_half // 2
    zero = jnp.int32(0)
    for i in range(min(SLOTS, own_chunks)):
        start_chunk(zero, KVQ, jnp.int32(i))
    bq_copy().wait_recv()
    scoped('wq_wait', wq_copy().wait_recv)
    for i in range(min(SLOTS, own_chunks), SLOTS):
        start_chunk(zero, KVQ, jnp.int32(i))
    bq_copy().wait_send()
    wq_copy().wait_send()

    @pl.when(first)
    def _():
        for i in range(WO_PARTS):
            wo_copy(i).wait_send()
        signal(go_sem, nxt)

    with jax.named_scope('wo_wait'):
        for i in range(WO_PARTS):
            wo_copy(i).wait_recv()
    load_x(zero)
    wait_chunk(0)
    wait_chunk(1)

    def attention(j):
        factor = HEAD ** -0.5 * 1.4426950408889634

        def two_heads(jj, i):
            q = qbuf[pl.ds(2 * i, 2)].reshape(2 * rows, HEAD)
            sd = jnp.dot(q, kt[:, jj * rows:(jj + 1) * rows], preferred_element_type=F32)
            row = jnp.bitwise_and(lax.broadcasted_iota(jnp.int32, (2 * rows, rows), 0), rows - 1)
            col = lax.broadcasted_iota(jnp.int32, (2 * rows, rows), 1)
            sd = jnp.where(col <= row, sd, -1e30)
            top = jnp.max(sd, axis=-1, keepdims=True)
            if jj:
                so = jnp.dot(q, kt[:, :jj * rows], preferred_element_type=F32)
                top = jnp.maximum(top, jnp.max(so, axis=-1, keepdims=True))
            pd = jnp.exp2((sd - top) * factor).astype(BF16)
            acc = jnp.dot(pd, vones[jj * rows:(jj + 1) * rows, :], preferred_element_type=F32)
            if jj:
                po = jnp.exp2((so - top) * factor).astype(BF16)
                acc = acc + jnp.dot(po, vones[:jj * rows, :], preferred_element_type=F32)
            c = (acc[:, :HEAD] / acc[:, HEAD:]).astype(BF16)
            at = pl.multiple_of(i * 2 * HEAD, 2 * HEAD)
            cbuf[:, pl.ds(at, HEAD)] = c[:rows]
            cbuf[:, pl.ds(at + HEAD, HEAD)] = c[rows:]

        for jj in range(quarters):
            @pl.when(j == jj)
            def _():
                def body(i, carry):
                    two_heads(jj, i)
                    return carry

                lax.fori_loop(0, n_heads // 2, body, 0)

    def x1_copy(slot, start, width):
        cols = pl.ds(start, width)
        return remote(x1own.at[:, cols], x1recv.at[slot, :, cols], x1_send_sem, x1_recv_sem.at[slot])

    def p_copy(slot, c):
        cols = pl.ds(pl.multiple_of(c * CW, CW), CW)
        return remote(psend.at[:, cols], precv.at[slot, :, cols], p_send_sem, p_recv_sem.at[slot])

    def attend(u):
        mb = u // quarters
        j = lax.rem(u, quarters)
        slot2 = lax.rem(u, 2)
        at_kvq = base(u, KVQ)
        at_o = base(u, O)
        send_x_in(u + half_q)

        @pl.when(first)
        def _():
            pltpu.make_async_copy(x_recv.at[0], xbuf.at[slot2], xload_sem).wait()

        @pl.when(jnp.logical_not(first))
        def _():
            scoped('x_wait', remote(ybuf, xbuf.at[slot2], y_send_sem, xslot_sem.at[slot2], nxt).wait_recv)

        scoped('ln1', layer_norm, xbuf.at[slot2], hbuf, g1, s1, 128)

        def q_heads(c, slot):
            a = jnp.dot(hbuf[...], ring[slot], preferred_element_type=F32)
            qbuf[2 * c] = (a[:, :HEAD] + bq_all[2 * c]).astype(BF16)
            qbuf[2 * c + 1] = (a[:, HEAD:] + bq_all[2 * c + 1]).astype(BF16)

        wait_chunk(at_kvq + 2)
        wait_chunk(at_kvq + 3)
        kv = jnp.dot(hbuf[...], ring[slot_at(at_kvq)], preferred_element_type=F32) + bkv[...]
        at = pl.ds(pl.multiple_of(j * rows, rows), rows)
        kt[:, at] = kv[:, :HEAD].astype(BF16).astype(F32).T.astype(BF16)
        vones[at, :HEAD] = kv[:, HEAD:].astype(BF16)
        q_heads(0, slot_at(at_kvq + 1))
        prefetch(u, KVQ, 0)
        prefetch(u, KVQ, 1)

        def q_body(i, carry):
            g = at_kvq + 2 * i
            wait_chunk(g + 2)
            wait_chunk(g + 3)
            q_heads(2 * i - 1, slot_at(g))
            q_heads(2 * i, slot_at(g + 1))
            prefetch(u, KVQ, 2 * i)
            prefetch(u, KVQ, 2 * i + 1)
            return carry

        scoped('q', lax.fori_loop, 1, (nq + 1) // 2, q_body, 0)
        scoped('attn', attention, j)

        @pl.when(u > 0)
        def _():
            remote(x1own, x1recv.at[slot2], x1_send_sem, x1_recv_sem.at[slot2]).wait_send()

        def o_cols(c, slot):
            cols = pl.ds(pl.multiple_of(c * CW, CW), CW)
            a = jnp.dot(cbuf[...], ring[slot], preferred_element_type=F32)
            x1own[:, cols] = (xbuf[slot2, :, cols].astype(F32) + a + bo[c]).astype(BF16)

        def o_body(i, carry):
            g = at_o + 2 * i
            wait_chunk(g + 2)
            wait_chunk(g + 3)
            o_cols(2 * i, slot_at(g))
            o_cols(2 * i + 1, slot_at(g + 1))

            @pl.when(i > 0)
            def _():
                x1_copy(slot2, pl.multiple_of((i - 1) * 2 * CW, CW), 2 * CW).start()

            prefetch(u, O, 2 * i)
            prefetch(u, O, 2 * i + 1)
            return carry

        scoped('o', lax.fori_loop, 0, nq // 2, o_body, 0)
        wait_chunk(at_o + nq + 1)
        o_cols(nq - 1, slot_at(at_o + nq - 1))
        prefetch(u, O, jnp.int32(nq - 1))
        tail = (nq // 2 - 1) * 2 * CW
        x1_copy(slot2, tail, hidden - tail).start()

        @pl.when((stage > 0) & (u + 2 < n_units))
        def _():
            signal(credit_sem, prv)


    def down(u, phase):
        slot2 = lax.rem(u, 2)
        at_d = base(u, phase)
        own = phase == DOWN

        if own:
            @pl.when(u > 0)
            def _():
                remote(psend, precv.at[slot2], p_send_sem, p_recv_sem.at[slot2]).wait_send()

        def body(c, carry):
            g = at_d + 2 * c

            def waits():
                wait_chunk(g + 2)
                wait_chunk(g + 3)

            if own:
                waits()
            else:
                pl.when((u + 1 < n_units) | (c < nq - 1))(waits)

            cols = pl.ds(pl.multiple_of(c * CW, CW), CW)
            a = (jnp.dot(ubuf[:, :hidden], ring[slot_at(g)], preferred_element_type=F32)
                 + jnp.dot(ubuf[:, hidden:], ring[slot_at(g + 1)], preferred_element_type=F32))
            if own:
                psend[:, cols] = a.astype(BF16)

                @pl.when(c > 0)
                def _():
                    p_copy(slot2, c - 1).start()
            else:
                zbuf[:, cols] = x1recv[slot2, :, cols].astype(F32) + a + bdn[c]

            prefetch(u, phase, 2 * c)
            prefetch(u, phase, 2 * c + 1)
            return carry

        scoped('down' if own else 'down_peer', lax.fori_loop, 0, nq, body, 0)
        if own:
            p_copy(slot2, nq - 1).start()

    def up(u, phase):
        at_u = base(u, phase)

        def cols_of(c, slot):
            a = jnp.dot(hbuf[...], ring[slot], preferred_element_type=F32) + bup[c]
            t = jnp.tanh(0.7978845608028654 * (a + 0.044715 * (a * a * a)))
            ubuf[:, pl.ds(pl.multiple_of(c * CW, CW), CW)] = (0.5 * a * (1.0 + t)).astype(BF16)

        def body(i, carry):
            g = at_u + 2 * i
            wait_chunk(g + 2)
            wait_chunk(g + 3)
            cols_of(2 * i, slot_at(g))
            cols_of(2 * i + 1, slot_at(g + 1))
            prefetch(u, phase, 2 * i)
            prefetch(u, phase, 2 * i + 1)
            return carry

        scoped('up' if phase == UP else 'up_peer', lax.fori_loop, 0, nu // 2, body, 0)

    def finish(v):
        slot = lax.rem(v, 2)
        mb = v // quarters
        j = lax.rem(v, quarters)
        scoped('p_wait', remote(psend, precv.at[slot], p_send_sem, p_recv_sem.at[slot]).wait_recv)

        @pl.when(v > 0)
        def _():
            scoped('y_wait', pltpu.make_async_copy(ybuf, x_recv.at[0], y_send_sem).wait)

        block = 32

        def body(i, carry):
            r = pl.ds(pl.multiple_of(i * block, block), block)
            ybuf[r, :] = (zbuf[r, :] + precv[slot, r, :].astype(F32)).astype(BF16)
            return carry

        lax.fori_loop(0, rows // block, body, 0)

        @pl.when(jnp.logical_not(last))
        def _():
            @pl.when(v >= 2)
            def _():
                pl.semaphore_wait(credit_sem, 1)

            remote(ybuf, xbuf.at[slot], y_send_sem, xslot_sem.at[slot], nxt).start()

        place = out.at[mb, rank, pl.ds(pl.multiple_of(lax.rem(j, half_q) * rows, rows), rows), :]

        @pl.when(last & (j // half_q == rank))
        def _():
            pltpu.make_async_copy(ybuf, place, y_send_sem).start()

        @pl.when(last & (j // half_q != rank))
        def _():
            remote(ybuf, place, y_send_sem, out_recv_sem.at[v]).start()

    def step(u, carry):
        slot2 = lax.rem(u, 2)
        attend(u)
        scoped('ln2', layer_norm, x1own, hbuf, g2, s2)
        up(u, UP)
        load_x(u + 1)
        down(u, DOWN)
        scoped('x1_wait', remote(x1own, x1recv.at[slot2], x1_send_sem, x1_recv_sem.at[slot2]).wait_recv)
        scoped('ln_peer', layer_norm, x1recv.at[slot2], hbuf, g2, s2, 32)
        up(u, UP2)
        down(u, DOWN2)
        finish(u)
        return carry

    lax.fori_loop(0, n_units, step, 0)

    end = (n_units - 1) % 2
    remote(x1own, x1recv.at[end], x1_send_sem, x1_recv_sem.at[end]).wait_send()
    remote(psend, precv.at[end], p_send_sem, p_recv_sem.at[end]).wait_send()
    pltpu.make_async_copy(ybuf, x_recv.at[0], y_send_sem).wait()

    @pl.when(jnp.logical_not(first))
    def _():
        for i in range(WO_PARTS):
            wo_copy(i).wait_send()

    @pl.when(last)
    def _():
        for i in range(WO_PARTS):
            hop_b(i).wait_send()
            hop_c(i).wait_send()

    def drain(t, carry):
        j = lax.rem(t, quarters)
        mine = j // half_q == rank

        @pl.when(first & mine)
        def _():
            remote(ybuf, x_recv.at[t], xin_send_sem.at[t], xrecv_sem.at[t]).wait_send()

        @pl.when(last & mine)
        def _():
            place = out.at[t // quarters, 1 - rank, pl.ds(pl.multiple_of(lax.rem(j, half_q) * rows, rows), rows), :]
            remote(ybuf, place, y_send_sem, out_recv_sem.at[t]).wait_recv()

        return carry

    lax.fori_loop(0, n_units, drain, 0)


def run_stage(x_loc, params, n_stages):
    (ln1_gain, ln1_bias, w_q, b_q, w_kv, b_kv, w_o, b_o, ln2_gain, ln2_bias, w_up, b_up, w_down, b_down) = params
    n_micro, _, seq_loc, hidden = x_loc.shape
    ffn_loc = w_up.shape[2]
    rows = min(UNIT_ROWS, seq_loc // 2)
    quarters = 2 * seq_loc // rows
    n_units = n_micro * quarters
    nq = hidden // CW
    nu = ffn_loc // CW
    heads_half = hidden // 2 // HEAD
    cfg = (n_stages, n_units, quarters, rows, hidden, ffn_loc)
    vmem = pl.BlockSpec(memory_space=pltpu.VMEM)
    anym = pl.BlockSpec(memory_space=pl.ANY)
    args = (
        x_loc, ln1_gain, ln1_bias, w_q, b_q.reshape(heads_half, 1, HEAD), w_kv, b_kv, w_o, b_o.reshape(nq, 1, CW),
        ln2_gain, ln2_bias, w_up, b_up.reshape(nu, 1, CW), w_down, b_down.reshape(nq, 1, CW),
    )
    in_specs = [anym, vmem, vmem, anym, vmem, anym, vmem, anym, vmem, vmem, vmem, anym, vmem, anym, vmem]
    half = hidden // 2
    out_shape = (
        jax.ShapeDtypeStruct(x_loc.shape, BF16),
        jax.ShapeDtypeStruct((n_units, rows, hidden), BF16),
        jax.ShapeDtypeStruct((hidden, half), BF16),
        jax.ShapeDtypeStruct((half, hidden), BF16),
        jax.ShapeDtypeStruct((half, hidden), BF16),
        jax.ShapeDtypeStruct((half, hidden), BF16),
    )
    dma = pltpu.SemaphoreType.DMA
    scratch = [
        pltpu.VMEM((SLOTS, hidden, CW), BF16),
        pltpu.VMEM((2, rows, hidden), BF16),
        pltpu.VMEM((rows, hidden), BF16),
        pltpu.VMEM((2 * heads_half, rows, HEAD), BF16),
        pltpu.VMEM((rows, hidden), BF16),
        pltpu.VMEM((rows, hidden), BF16),
        pltpu.VMEM((2, rows, hidden), BF16),
        pltpu.VMEM((rows, ffn_loc), BF16),
        pltpu.VMEM((rows, hidden), F32),
        pltpu.VMEM((rows, hidden), BF16),
        pltpu.VMEM((2, rows, hidden), BF16),
        pltpu.VMEM((rows, hidden), BF16),
        pltpu.VMEM((HEAD, quarters * rows), BF16),
        pltpu.VMEM((quarters * rows, 2 * HEAD), BF16),
        pltpu.VMEM((2 * heads_half, 1, HEAD), F32),
        dma((SLOTS,)),
        dma,
        dma((2,)),
        dma((n_units,)),
        dma((n_units,)),
        dma((2,)),
        dma((2,)),
        dma((WO_PARTS,)),
        dma((WO_PARTS,)),
        dma((WO_PARTS,)),
        dma((WO_PARTS,)),
        dma((WO_PARTS,)),
        dma((WO_PARTS,)),
        dma,
        dma((2,)),
        dma,
        dma((2,)),
        dma,
        dma((n_units,)),
        pltpu.SemaphoreType.REGULAR,
        pltpu.SemaphoreType.REGULAR,
    ]
    return pl.pallas_call(
        functools.partial(stage_kernel, cfg),
        out_shape=out_shape,
        in_specs=in_specs,
        out_specs=(anym,) * 6,
        scratch_shapes=scratch,
        compiler_params=pltpu.CompilerParams(collective_id=0, has_side_effects=True, vmem_limit_bytes=60 * 2 ** 20),
        name='stage_loop',
    )(*args)[0]


def solution(mesh):
    pp_size = mesh.shape['pp']

    def stage_program(x_loc, *params):
        result = run_stage(x_loc, params, pp_size)
        is_last = lax.axis_index('pp') == pp_size - 1
        return jnp.where(is_last, result, jnp.zeros_like(result))[None]

    return jax.shard_map(stage_program, mesh=mesh, in_specs=(P(None, 'dp', 'tp', None),) + PARAM_SPECS, out_specs=P('pp', None, 'dp', 'tp', None), check_vma=False)
```

```python
import functools

import jax
import jax.numpy as jnp
from jax import lax
from jax.experimental import pallas as pl
from jax.experimental.pallas import tpu as pltpu
from jax.sharding import PartitionSpec as P

F32 = jnp.float32
BF16 = jnp.bfloat16
MESH = pl.DeviceIdType.MESH

PARAM_SPECS = (P('pp', None), P('pp', None), P('pp', None, 'tp'), P('pp', 'tp'), P('pp', None, None), P('pp', None), P('pp', 'tp', None), P('pp', None), P('pp', None), P('pp', None), P('pp', None, 'tp'), P('pp', 'tp'), P('pp', 'tp', None), P('pp', None))

CW = 256
HEAD = 128
SLOTS = 10
WO_PARTS = 4


def scoped(name, fn, *args):
    with jax.named_scope(name):
        return fn(*args)


def stage_kernel(cfg, x_in, g1, s1, wq, bq, wkv, bkv, wo, bo, g2, s2, wup, bup, wdn, bdn,
                 out, wq_peer, wo_peer, relay_a, relay_b,
                 ring, xbuf, hbuf, qbuf, cbuf, x1own, x1recv, ubuf, zbuf, psend, precv, ybuf, kt, vones, bq_all,
                 ring_sem, xload_sem, xslot_sem, w_send_sem, w_recv_sem, wo_send_sem, wo_recv_sem,
                 ra_recv_sem, rb_send_sem, rb_recv_sem, rc_send_sem, kv_send_sem, k_recv_sem, v_recv_sem,
                 x1_send_sem, x1_recv_sem, p_send_sem, p_recv_sem, y_send_sem, go_sem, credit_sem):
    (n_stages, n_blocks, rows, hidden, ffn_loc) = cfg
    half = hidden // 2
    nq = hidden // CW
    nu = ffn_loc // CW
    heads_half = half // HEAD
    n_heads = 2 * heads_half
    stage = lax.axis_index('pp')
    rank = lax.axis_index('tp')
    peer = {'tp': 1 - rank}
    nxt = {'pp': jnp.minimum(stage + 1, n_stages - 1)}
    prv = {'pp': jnp.maximum(stage - 1, 0)}
    across = {'pp': 4 - stage}
    first = stage == 0
    second = stage == 1
    last = stage == n_stages - 1
    even = lax.rem(stage, 2) == 0

    leads = lax.rem(rank + stage, 2) == 0
    lag = 1 - leads.astype(jnp.int32)
    n_steps = n_blocks + 1

    def own_block(k):
        return k - lag

    def peer_block(k):
        return k - 1 + lag

    def valid(b):
        return (b >= 0) & (b < n_blocks)

    KVQ, O, UP, DOWN, UP2, DOWN2 = 0, 1, 2, 3, 4, 5
    counts = (1 + nq, nq, nu, 2 * nq, nu, 2 * nq)
    own_count = sum(counts[:4])
    peer_count = sum(counts[4:])

    def base(k, phase):
        start = k * (own_count + peer_count) - jnp.where(k > 0, jnp.where(leads, peer_count, own_count), 0)
        if phase < UP2:
            return start + sum(counts[:phase])
        return start + jnp.where(valid(own_block(k)), own_count, 0) + sum(counts[UP2:phase])

    def slot_at(g):
        return lax.rem(g, SLOTS)

    def start_chunk(u, phase, idx):
        slot = slot_at(base(u, phase) + idx)
        dst = ring.at[slot]
        sem = ring_sem.at[slot]

        def cols(c, width):
            return pl.ds(pl.multiple_of(c * width, width), width)

        if phase == KVQ:
            @pl.when(idx == 0)
            def _():
                pltpu.make_async_copy(wkv.at[0], dst, sem).start()

            for b in range(2):
                block = (idx - 1) * 2 + b
                piece = dst.at[:, pl.ds(b * HEAD, HEAD)]

                @pl.when((idx > 0) & (block < heads_half))
                def _():
                    pltpu.make_async_copy(wq.at[0, :, cols(block, HEAD)], piece, sem).start()

                @pl.when((idx > 0) & (block >= heads_half))
                def _():
                    pltpu.make_async_copy(wq_peer.at[:, cols(block - heads_half, HEAD)], piece, sem).start()
        elif phase == O:
            pltpu.make_async_copy(wo.at[0, :, cols(idx, CW)], dst.at[pl.ds(0, half), :], sem).start()
            pltpu.make_async_copy(wo_peer.at[:, cols(idx, CW)], dst.at[pl.ds(half, half), :], sem).start()
        elif phase in (UP, UP2):
            pltpu.make_async_copy(wup.at[0, :, cols(idx, CW)], dst, sem).start()
        else:
            part = lax.rem(idx, 2)
            pltpu.make_async_copy(
                wdn.at[0, pl.ds(pl.multiple_of(part * hidden, hidden), hidden), cols(idx // 2, CW)], dst, sem).start()

    def prefetch(u, phase, idx):
        ahead = idx + SLOTS
        n = counts[phase]

        @pl.when(ahead < n)
        def _():
            start_chunk(u, phase, ahead)

        over = ahead - n
        past = over >= 0
        if phase == DOWN:
            @pl.when(past & valid(peer_block(u)))
            def _():
                start_chunk(u, UP2, over)

            @pl.when(past & jnp.logical_not(valid(peer_block(u))) & (u + 1 < n_steps))
            def _():
                start_chunk(u + 1, KVQ, over)
        elif phase == DOWN2:
            @pl.when(past & (u + 1 < n_steps) & valid(own_block(u + 1)))
            def _():
                start_chunk(u + 1, KVQ, over)

            @pl.when(past & (u + 1 < n_steps) & jnp.logical_not(valid(own_block(u + 1))))
            def _():
                start_chunk(u + 1, UP2, over)
        else:
            @pl.when(past)
            def _():
                start_chunk(u, phase + 1, over)

    def wait_chunk(g):
        slot = slot_at(g)
        pltpu.make_async_copy(wkv.at[0], ring.at[slot], ring_sem.at[slot]).wait()

    def layer_norm(src, dst, gain, shift):
        block = min(128, rows)
        pieces = [pl.ds(k * CW, CW) for k in range(hidden // CW)]

        def body(i, carry):
            at = pl.multiple_of(i * block, block)
            r = pl.ds(at, block)
            total = src[r, pieces[0]].astype(F32)
            for p in pieces[1:]:
                total = total + src[r, p].astype(F32)
            mean = jnp.sum(total, axis=-1, keepdims=True) * (1.0 / hidden)
            square = None
            for p in pieces:
                cen = src[r, p].astype(F32) - mean
                square = cen * cen if square is None else square + cen * cen
            inv = lax.rsqrt(jnp.sum(square, axis=-1, keepdims=True) * (1.0 / hidden) + 1e-5)
            for p in pieces:
                cen = src[r, p].astype(F32) - mean
                dst[r, p] = (cen * inv * gain[:, p] + shift[:, p]).astype(BF16)
            return carry

        lax.fori_loop(0, rows // block, body, 0)

    def place(b):
        return b // 4, lax.rem(b // 2, 2), pl.ds(pl.multiple_of(lax.rem(b, 2) * rows, rows), rows)

    def load_x(b):
        @pl.when(first & (b < n_blocks))
        def _():
            mb, seq, r = place(b)
            pltpu.make_async_copy(x_in.at[mb, seq, r, :], xbuf.at[lax.rem(b, 2)], xload_sem).start()

    def remote(src, dst, send_sem, recv_sem, to=peer):
        return pltpu.make_async_remote_copy(src, dst, send_sem, recv_sem, device_id=to, device_id_type=MESH)

    def signal(sem, to):
        pl.semaphore_signal(sem, inc=1, device_id=to, device_id_type=MESH)

    def wq_copy():
        return remote(wq.at[0], wq_peer, w_send_sem.at[0], w_recv_sem.at[0])

    def bq_copy():
        return remote(bq, bq_all.at[pl.ds(heads_half, heads_half)], w_send_sem.at[1], w_recv_sem.at[1])

    def part_rows(i):
        return pl.ds(i * (half // WO_PARTS), half // WO_PARTS)

    def wo_copy(i):
        return remote(wo.at[0, part_rows(i), :], wo_peer.at[part_rows(i), :], wo_send_sem.at[i], wo_recv_sem.at[i])

    def hop_a(i):
        return remote(wo.at[0, part_rows(i), :], relay_a.at[part_rows(i), :], wo_send_sem.at[i], ra_recv_sem.at[i], across)

    def hop_b(i):
        return remote(relay_a.at[part_rows(i), :], relay_b.at[part_rows(i), :], rb_send_sem.at[i], rb_recv_sem.at[i])

    def hop_c(i):
        return remote(relay_b.at[part_rows(i), :], wo_peer.at[part_rows(i), :], rc_send_sem.at[i], wo_recv_sem.at[i], across)

    barrier = pltpu.get_barrier_semaphore()
    signal(barrier, peer)

    @pl.when(stage > 0)
    def _():
        signal(barrier, prv)

    @pl.when(jnp.logical_not(last))
    def _():
        signal(barrier, nxt)

    @pl.when(jnp.logical_not(even))
    def _():
        signal(barrier, across)

    pl.semaphore_wait(barrier, 1 + (stage > 0).astype(jnp.int32) + (stage < n_stages - 1).astype(jnp.int32) + 1 - even.astype(jnp.int32))

    @pl.when(second)
    def _():
        for i in range(WO_PARTS):
            hop_a(i).start()

    @pl.when(last)
    def _():
        for i in range(WO_PARTS + 1):
            if i < WO_PARTS:
                hop_a(i).wait_recv()
                hop_b(i).start()
            if i > 0:
                hop_b(i - 1).wait_recv()
                hop_c(i - 1).start()

    @pl.when(second)
    def _():
        scoped('go_wait', pl.semaphore_wait, go_sem, 1)

    bq_copy().start()
    wq_copy().start()

    @pl.when(jnp.logical_not(second))
    def _():
        for i in range(WO_PARTS):
            wo_copy(i).start()

    bq_all[pl.ds(0, heads_half)] = bq[...]
    vones[:, :, HEAD:] = jnp.ones((2, 4 * rows, HEAD), BF16)

    own_chunks = 1 + heads_half // 2
    zero = jnp.int32(0)

    @pl.when(leads)
    def _():
        for i in range(min(SLOTS, own_chunks)):
            start_chunk(zero, KVQ, jnp.int32(i))

    @pl.when(jnp.logical_not(leads))
    def _():
        for i in range(SLOTS):
            start_chunk(zero, UP2, jnp.int32(i))

    load_x(zero)
    bq_copy().wait_recv()
    scoped('wq_wait', wq_copy().wait_recv)

    @pl.when(leads)
    def _():
        for i in range(min(SLOTS, own_chunks), SLOTS):
            start_chunk(zero, KVQ, jnp.int32(i))

    bq_copy().wait_send()
    wq_copy().wait_send()

    @pl.when(first)
    def _():
        for i in range(WO_PARTS):
            wo_copy(i).wait_send()
        signal(go_sem, nxt)

    with jax.named_scope('wo_wait'):
        for i in range(WO_PARTS):
            wo_copy(i).wait_recv()
    wait_chunk(0)
    wait_chunk(1)

    def attention(j, seq):
        factor = HEAD ** -0.5 * 1.4426950408889634

        def two_heads(jj, i):
            kts, vs = kt.at[seq], vones.at[seq]
            q = qbuf[pl.ds(2 * i, 2)].reshape(2 * rows, HEAD)
            sd = jnp.dot(q, kts[:, jj * rows:(jj + 1) * rows], preferred_element_type=F32)
            row = jnp.bitwise_and(lax.broadcasted_iota(jnp.int32, (2 * rows, rows), 0), rows - 1)
            col = lax.broadcasted_iota(jnp.int32, (2 * rows, rows), 1)
            sd = jnp.where(col <= row, sd, -1e30)
            top = jnp.max(sd, axis=-1, keepdims=True)
            if jj:
                so = jnp.dot(q, kts[:, :jj * rows], preferred_element_type=F32)
                top = jnp.maximum(top, jnp.max(so, axis=-1, keepdims=True))
            pd = jnp.exp2((sd - top) * factor).astype(BF16)
            acc = jnp.dot(pd, vs[jj * rows:(jj + 1) * rows, :], preferred_element_type=F32)
            if jj:
                po = jnp.exp2((so - top) * factor).astype(BF16)
                acc = acc + jnp.dot(po, vs[:jj * rows, :], preferred_element_type=F32)
            c = (acc[:, :HEAD] / acc[:, HEAD:]).astype(BF16)
            at = pl.multiple_of(i * 2 * HEAD, 2 * HEAD)
            cbuf[:, pl.ds(at, HEAD)] = c[:rows]
            cbuf[:, pl.ds(at + HEAD, HEAD)] = c[rows:]

        for jj in range(4):
            @pl.when(j == jj)
            def _():
                def body(i, carry):
                    two_heads(jj, i)
                    return carry

                lax.fori_loop(0, n_heads // 2, body, 0)

    def x1_copy(slot, start, width):
        cols = pl.ds(start, width)
        return remote(x1own.at[:, cols], x1recv.at[slot, :, cols], x1_send_sem, x1_recv_sem.at[slot])

    def p_copy(slot, c):
        cols = pl.ds(pl.multiple_of(c * CW, CW), CW)
        return remote(psend.at[:, cols], precv.at[slot, :, cols], p_send_sem, p_recv_sem.at[slot])

    def kv_copies(seq, part):
        at = pl.ds(pl.multiple_of(part * rows, rows), rows)
        sem = 2 * seq + part
        return (remote(kt.at[seq, :, at], kt.at[seq, :, at], kv_send_sem.at[0], k_recv_sem.at[sem]),
                remote(vones.at[seq, at, pl.ds(0, HEAD)], vones.at[seq, at, pl.ds(0, HEAD)], kv_send_sem.at[1], v_recv_sem.at[sem]))

    def attend(u):
        b = own_block(u)
        seq = lax.rem(b // 2, 2)
        part = lax.rem(b, 2)
        j = part + 2 * lag
        slot2 = lax.rem(u, 2)
        xslot = lax.rem(b, 2)
        at_kvq = base(u, KVQ)
        at_o = base(u, O)

        @pl.when(first)
        def _():
            pltpu.make_async_copy(x_in.at[0, 0, pl.ds(0, rows), :], xbuf.at[xslot], xload_sem).wait()

        @pl.when(jnp.logical_not(first))
        def _():
            scoped('x_wait', remote(ybuf, xbuf.at[xslot], y_send_sem, xslot_sem.at[xslot], nxt).wait_recv)

        scoped('ln1', layer_norm, xbuf.at[xslot], hbuf, g1, s1)

        @pl.when(leads & (b > 0))
        def _():
            for copy in kv_copies(seq, part):
                copy.wait_send()

        def q_heads(c, slot):
            a = jnp.dot(hbuf[...], ring[slot], preferred_element_type=F32)
            qbuf[2 * c] = (a[:, :HEAD] + bq_all[2 * c]).astype(BF16)
            qbuf[2 * c + 1] = (a[:, HEAD:] + bq_all[2 * c + 1]).astype(BF16)

        wait_chunk(at_kvq + 2)
        wait_chunk(at_kvq + 3)
        kv = jnp.dot(hbuf[...], ring[slot_at(at_kvq)], preferred_element_type=F32) + bkv[...]
        at = pl.ds(pl.multiple_of(j * rows, rows), rows)
        kt[seq, :, at] = kv[:, :HEAD].astype(BF16).astype(F32).T.astype(BF16)
        vones[seq, at, :HEAD] = kv[:, HEAD:].astype(BF16)
        q_heads(0, slot_at(at_kvq + 1))

        @pl.when(leads)
        def _():
            for copy in kv_copies(seq, part):
                copy.start()

        prefetch(u, KVQ, zero)
        prefetch(u, KVQ, zero + 1)

        def q_body(i, carry):
            g = at_kvq + 2 * i
            wait_chunk(g + 2)
            wait_chunk(g + 3)
            q_heads(2 * i - 1, slot_at(g))
            q_heads(2 * i, slot_at(g + 1))
            prefetch(u, KVQ, 2 * i)
            prefetch(u, KVQ, 2 * i + 1)
            return carry

        scoped('q', lax.fori_loop, 1, (nq + 1) // 2, q_body, 0)

        @pl.when(jnp.logical_not(leads) & (part == 0))
        def _():
            with jax.named_scope('kv_wait'):
                for p in range(2):
                    for copy in kv_copies(seq, jnp.int32(p)):
                        copy.wait_recv()

        scoped('attn', attention, j, seq)


        @pl.when(b > 0)
        def _():
            remote(x1own, x1recv.at[slot2], x1_send_sem, x1_recv_sem.at[slot2]).wait_send()

        def o_cols(c, slot):
            cols = pl.ds(pl.multiple_of(c * CW, CW), CW)
            a = jnp.dot(cbuf[...], ring[slot], preferred_element_type=F32)
            x1own[:, cols] = (xbuf[xslot, :, cols].astype(F32) + a + bo[c]).astype(BF16)

        def o_body(i, carry):
            g = at_o + 2 * i
            wait_chunk(g + 2)
            wait_chunk(g + 3)
            o_cols(2 * i, slot_at(g))
            o_cols(2 * i + 1, slot_at(g + 1))

            @pl.when(i > 0)
            def _():
                x1_copy(slot2, pl.multiple_of((i - 1) * 2 * CW, CW), 2 * CW).start()

            prefetch(u, O, 2 * i)
            prefetch(u, O, 2 * i + 1)
            return carry

        scoped('o', lax.fori_loop, 0, nq // 2, o_body, 0)
        wait_chunk(at_o + nq + 1)
        o_cols(nq - 1, slot_at(at_o + nq - 1))
        prefetch(u, O, jnp.int32(nq - 1))
        tail = (nq // 2 - 1) * 2 * CW
        x1_copy(slot2, tail, hidden - tail).start()

        @pl.when((stage > 0) & (b + 2 < n_blocks))
        def _():
            signal(credit_sem, prv)


    def down(u, phase):
        slot2 = lax.rem(u, 2)
        at_d = base(u, phase)
        own = phase == DOWN

        if own:
            @pl.when(own_block(u) > 0)
            def _():
                remote(psend, precv.at[slot2], p_send_sem, p_recv_sem.at[slot2]).wait_send()

        def body(c, carry):
            g = at_d + 2 * c

            def waits():
                wait_chunk(g + 2)
                wait_chunk(g + 3)

            pl.when((u + 1 < n_steps) | (c < nq - 1))(waits)

            cols = pl.ds(pl.multiple_of(c * CW, CW), CW)
            a = (jnp.dot(ubuf[:, :hidden], ring[slot_at(g)], preferred_element_type=F32)
                 + jnp.dot(ubuf[:, hidden:], ring[slot_at(g + 1)], preferred_element_type=F32))
            if own:
                psend[:, cols] = a.astype(BF16)

                @pl.when(c > 0)
                def _():
                    p_copy(slot2, c - 1).start()
            else:
                zbuf[:, cols] = x1recv[slot2, :, cols].astype(F32) + a + bdn[c]

            prefetch(u, phase, 2 * c)
            prefetch(u, phase, 2 * c + 1)
            return carry

        scoped('down' if own else 'down_peer', lax.fori_loop, 0, nq, body, 0)
        if own:
            p_copy(slot2, nq - 1).start()

    def up(u, phase):
        at_u = base(u, phase)

        def cols_of(c, slot):
            a = jnp.dot(hbuf[...], ring[slot], preferred_element_type=F32) + bup[c]
            t = jnp.tanh(0.7978845608028654 * (a + 0.044715 * (a * a * a)))
            ubuf[:, pl.ds(pl.multiple_of(c * CW, CW), CW)] = (0.5 * a * (1.0 + t)).astype(BF16)

        def body(i, carry):
            g = at_u + 2 * i
            wait_chunk(g + 2)
            wait_chunk(g + 3)
            cols_of(2 * i, slot_at(g))
            cols_of(2 * i + 1, slot_at(g + 1))
            prefetch(u, phase, 2 * i)
            prefetch(u, phase, 2 * i + 1)
            return carry

        scoped('up' if phase == UP else 'up_peer', lax.fori_loop, 0, nu // 2, body, 0)

    def finish(u):
        v = peer_block(u)
        slot = lax.rem(u, 2)
        scoped('p_wait', remote(psend, precv.at[slot], p_send_sem, p_recv_sem.at[slot]).wait_recv)

        @pl.when(v > 0)
        def _():
            scoped('y_wait', pltpu.make_async_copy(ybuf, out.at[0, 0, pl.ds(0, rows), :], y_send_sem).wait)

        block = 32

        def body(i, carry):
            r = pl.ds(pl.multiple_of(i * block, block), block)
            ybuf[r, :] = (zbuf[r, :] + precv[slot, r, :].astype(F32)).astype(BF16)
            return carry

        lax.fori_loop(0, rows // block, body, 0)

        @pl.when(jnp.logical_not(last))
        def _():
            @pl.when(v >= 2)
            def _():
                pl.semaphore_wait(credit_sem, 1)

            to = lax.rem(v, 2)
            remote(ybuf, xbuf.at[to], y_send_sem, xslot_sem.at[to], nxt).start()

        @pl.when(last)
        def _():
            mb, seq, r = place(v)
            pltpu.make_async_copy(ybuf, out.at[mb, seq, r, :], y_send_sem).start()

    def step(u, carry):
        slot2 = lax.rem(u, 2)

        @pl.when(valid(own_block(u)))
        def _():
            attend(u)
            scoped('ln2', layer_norm, x1own, hbuf, g2, s2)
            up(u, UP)
            load_x(own_block(u) + 1)
            down(u, DOWN)

        @pl.when(valid(peer_block(u)))
        def _():
            scoped('x1_wait', remote(x1own, x1recv.at[slot2], x1_send_sem, x1_recv_sem.at[slot2]).wait_recv)
            scoped('ln_peer', layer_norm, x1recv.at[slot2], hbuf, g2, s2)
            up(u, UP2)
            down(u, DOWN2)
            finish(u)

        return carry

    lax.fori_loop(0, n_steps, step, 0)

    remote(x1own, x1recv.at[0], x1_send_sem, x1_recv_sem.at[0]).wait_send()
    remote(psend, precv.at[0], p_send_sem, p_recv_sem.at[0]).wait_send()
    pltpu.make_async_copy(ybuf, out.at[0, 0, pl.ds(0, rows), :], y_send_sem).wait()

    @pl.when(leads)
    def _():
        for copy in kv_copies(zero, zero):
            copy.wait_send()

    @pl.when(jnp.logical_not(first))
    def _():
        for i in range(WO_PARTS):
            wo_copy(i).wait_send()

    @pl.when(last)
    def _():
        for i in range(WO_PARTS):
            hop_b(i).wait_send()
            hop_c(i).wait_send()


def run_stage(x_loc, params, n_stages):
    (ln1_gain, ln1_bias, w_q, b_q, w_kv, b_kv, w_o, b_o, ln2_gain, ln2_bias, w_up, b_up, w_down, b_down) = params
    n_micro, _, seq_loc, hidden = x_loc.shape
    ffn_loc = w_up.shape[2]
    rows = seq_loc // 2
    n_blocks = 4 * n_micro
    nq = hidden // CW
    nu = ffn_loc // CW
    heads_half = hidden // 2 // HEAD
    cfg = (n_stages, n_blocks, rows, hidden, ffn_loc)
    vmem = pl.BlockSpec(memory_space=pltpu.VMEM)
    anym = pl.BlockSpec(memory_space=pl.ANY)
    args = (
        x_loc, ln1_gain, ln1_bias, w_q, b_q.reshape(heads_half, 1, HEAD), w_kv, b_kv, w_o, b_o.reshape(nq, 1, CW),
        ln2_gain, ln2_bias, w_up, b_up.reshape(nu, 1, CW), w_down, b_down.reshape(nq, 1, CW),
    )
    in_specs = [anym, vmem, vmem, anym, vmem, anym, vmem, anym, vmem, vmem, vmem, anym, vmem, anym, vmem]
    half = hidden // 2
    out_shape = (
        jax.ShapeDtypeStruct(x_loc.shape, BF16),
        jax.ShapeDtypeStruct((hidden, half), BF16),
        jax.ShapeDtypeStruct((half, hidden), BF16),
        jax.ShapeDtypeStruct((half, hidden), BF16),
        jax.ShapeDtypeStruct((half, hidden), BF16),
    )
    dma = pltpu.SemaphoreType.DMA
    scratch = [
        pltpu.VMEM((SLOTS, hidden, CW), BF16),
        pltpu.VMEM((2, rows, hidden), BF16),
        pltpu.VMEM((rows, hidden), BF16),
        pltpu.VMEM((2 * heads_half, rows, HEAD), BF16),
        pltpu.VMEM((rows, hidden), BF16),
        pltpu.VMEM((rows, hidden), BF16),
        pltpu.VMEM((2, rows, hidden), BF16),
        pltpu.VMEM((rows, ffn_loc), BF16),
        pltpu.VMEM((rows, hidden), F32),
        pltpu.VMEM((rows, hidden), BF16),
        pltpu.VMEM((2, rows, hidden), BF16),
        pltpu.VMEM((rows, hidden), BF16),
        pltpu.VMEM((2, HEAD, 4 * rows), BF16),
        pltpu.VMEM((2, 4 * rows, 2 * HEAD), BF16),
        pltpu.VMEM((2 * heads_half, 1, HEAD), F32),
        dma((SLOTS,)),
        dma,
        dma((2,)),
        dma((2,)),
        dma((2,)),
        dma((WO_PARTS,)),
        dma((WO_PARTS,)),
        dma((WO_PARTS,)),
        dma((WO_PARTS,)),
        dma((WO_PARTS,)),
        dma((WO_PARTS,)),
        dma((2,)),
        dma((4,)),
        dma((4,)),
        dma,
        dma((2,)),
        dma,
        dma((2,)),
        dma,
        pltpu.SemaphoreType.REGULAR,
        pltpu.SemaphoreType.REGULAR,
    ]
    return pl.pallas_call(
        functools.partial(stage_kernel, cfg),
        out_shape=out_shape,
        in_specs=in_specs,
        out_specs=(anym,) * 5,
        scratch_shapes=scratch,
        compiler_params=pltpu.CompilerParams(collective_id=0, has_side_effects=True, vmem_limit_bytes=60 * 2 ** 20),
        name='stage_loop',
    )(*args)[0]


def solution(mesh):
    pp_size = mesh.shape['pp']

    def stage_program(x_loc, *params):
        result = run_stage(x_loc, params, pp_size)
        is_last = lax.axis_index('pp') == pp_size - 1
        return jnp.where(is_last, result, jnp.zeros_like(result))[None]

    return jax.shard_map(stage_program, mesh=mesh, in_specs=(P(None, 'dp', 'tp', None),) + PARAM_SPECS, out_specs=P('pp', None, 'dp', 'tp', None), check_vma=False)
```

```python
import functools

import jax
import jax.numpy as jnp
from jax import lax
from jax.experimental import pallas as pl
from jax.experimental.pallas import tpu as pltpu
from jax.sharding import PartitionSpec as P

F32 = jnp.float32
BF16 = jnp.bfloat16
MESH = pl.DeviceIdType.MESH

PARAM_SPECS = (P('pp', None), P('pp', None), P('pp', None, 'tp'), P('pp', 'tp'), P('pp', None, None), P('pp', None), P('pp', 'tp', None), P('pp', None), P('pp', None), P('pp', None), P('pp', None, 'tp'), P('pp', 'tp'), P('pp', 'tp', None), P('pp', None))

CW = 256
HEAD = 128
SLOTS = 16
AHEAD = 4
PARTS = 4
RELAYED = 5


def scoped(name, fn, *args):
    with jax.named_scope(name):
        return fn(*args)


def stage_kernel(cfg, x_in, g1, s1, wq, bq, wkv, bkv, wo, bo, g2, s2, wup, bup, wdn, bdn,
                 out, wq_peer, wo_peer, qa, qb, oa, ob,
                 ring, xbuf, hbuf, qbuf, cbuf, x1own, x1recv, ubuf, zbuf, psend, precv, ybuf, kt, vones, bq_all,
                 ring_sem, xload_sem, xslot_sem, bq_sem, w_send_sem, w_recv_sem, ra_recv_sem, rb_send_sem, rb_recv_sem, rc_send_sem,
                 kv_send_sem, k_recv_sem, v_recv_sem,
                 x1_send_sem, x1_recv_sem, p_send_sem, p_recv_sem, y_send_sem, go_sem, clear_sem, credit_sem):
    (n_stages, n_blocks, rows, hidden, ffn_loc) = cfg
    half = hidden // 2
    nq = hidden // CW
    nu = ffn_loc // CW
    heads_half = half // HEAD
    n_heads = 2 * heads_half
    stage = lax.axis_index('pp')
    rank = lax.axis_index('tp')
    peer = {'tp': 1 - rank}
    nxt = {'pp': jnp.minimum(stage + 1, n_stages - 1)}
    prv = {'pp': jnp.maximum(stage - 1, 0)}
    across = {'pp': 4 - stage}
    first = stage == 0
    second = stage == 1
    third = stage == 2
    last = stage == n_stages - 1
    even = lax.rem(stage, 2) == 0

    leads = lax.rem(rank + stage, 2) == 0
    lag = 1 - leads.astype(jnp.int32)
    n_steps = n_blocks + 1

    def own_block(k):
        return k - lag

    def peer_block(k):
        return k - 1 + lag

    def valid(b):
        return (b >= 0) & (b < n_blocks)

    KVQ, O, UP, DOWN, UP2, DOWN2 = 0, 1, 2, 3, 4, 5
    counts = (1 + nq, nq, nu, 2 * nq, nu, 2 * nq)
    own_count = sum(counts[:4])
    peer_count = sum(counts[4:])

    def base(k, phase):
        start = k * (own_count + peer_count) - jnp.where(k > 0, jnp.where(leads, peer_count, own_count), 0)
        if phase < UP2:
            return start + sum(counts[:phase])
        return start + jnp.where(valid(own_block(k)), own_count, 0) + sum(counts[UP2:phase])

    def slot_at(g):
        return lax.rem(g, SLOTS)

    def start_chunk(u, phase, idx):
        slot = slot_at(base(u, phase) + idx)
        dst = ring.at[slot]
        sem = ring_sem.at[slot]

        def cols(c, width):
            return pl.ds(pl.multiple_of(c * width, width), width)

        if phase == KVQ:
            @pl.when(idx == 0)
            def _():
                pltpu.make_async_copy(wkv.at[0], dst, sem).start()

            for b in range(2):
                block = (idx - 1) * 2 + b
                piece = dst.at[:, pl.ds(b * HEAD, HEAD)]

                @pl.when((idx > 0) & (block < heads_half))
                def _():
                    pltpu.make_async_copy(wq.at[0, :, cols(block, HEAD)], piece, sem).start()

                @pl.when((idx > 0) & (block >= heads_half))
                def _():
                    pltpu.make_async_copy(wq_peer.at[:, cols(block - heads_half, HEAD)], piece, sem).start()
        elif phase == O:
            pltpu.make_async_copy(wo.at[0, :, cols(idx, CW)], dst.at[pl.ds(0, half), :], sem).start()
            pltpu.make_async_copy(wo_peer.at[:, cols(idx, CW)], dst.at[pl.ds(half, half), :], sem).start()
        elif phase in (UP, UP2):
            pltpu.make_async_copy(wup.at[0, :, cols(idx, CW)], dst, sem).start()
        else:
            part = lax.rem(idx, 2)
            pltpu.make_async_copy(
                wdn.at[0, pl.ds(pl.multiple_of(part * hidden, hidden), hidden), cols(idx // 2, CW)], dst, sem).start()

    def start_at(u, part, pos, phases):
        firsts = KVQ if part == 0 else UP2
        for i, phase in enumerate(phases):
            low = sum(counts[firsts:phase])
            inside = (pos >= low) & (pos < low + counts[phase])

            @pl.when(inside)
            def _():
                start_chunk(u, phase, pos - low)

    def prefetch(u, phase, idx):
        part = 0 if phase < UP2 else 1
        length = (own_count, peer_count)[part]
        low = sum(counts[KVQ if part == 0 else UP2:phase])
        pos = idx + low + SLOTS
        last_phase = DOWN if part == 0 else DOWN2
        reach = [p for p in range(phase, last_phase + 1)]
        start_at(u, part, pos, reach[:3])
        if phase == last_phase:
            past = pos >= length
            peer_next = valid(peer_block(u)) if part == 0 else (u + 1 < n_steps) & jnp.logical_not(valid(own_block(u + 1)))
            own_next = (jnp.logical_not(valid(peer_block(u))) if part == 0 else True) & (u + 1 < n_steps) & valid(own_block(u + 1))

            @pl.when(past & peer_next)
            def _():
                start_at(u if part == 0 else u + 1, 1, pos - length, (UP2, DOWN2))

            @pl.when(past & own_next)
            def _():
                start_at(u + 1, 0, pos - length, (KVQ, O, UP))

    def wait_chunk(g):
        slot = slot_at(g)
        pltpu.make_async_copy(wkv.at[0], ring.at[slot], ring_sem.at[slot]).wait()

    def layer_norm(src, dst, gain, shift):
        block = min(128, rows)
        pieces = [pl.ds(k * CW, CW) for k in range(hidden // CW)]

        def body(i, carry):
            at = pl.multiple_of(i * block, block)
            r = pl.ds(at, block)
            total = src[r, pieces[0]].astype(F32)
            for p in pieces[1:]:
                total = total + src[r, p].astype(F32)
            mean = jnp.sum(total, axis=-1, keepdims=True) * (1.0 / hidden)
            square = None
            for p in pieces:
                cen = src[r, p].astype(F32) - mean
                square = cen * cen if square is None else square + cen * cen
            inv = lax.rsqrt(jnp.sum(square, axis=-1, keepdims=True) * (1.0 / hidden) + 1e-5)
            for p in pieces:
                cen = src[r, p].astype(F32) - mean
                dst[r, p] = (cen * inv * gain[:, p] + shift[:, p]).astype(BF16)
            return carry

        lax.fori_loop(0, rows // block, body, 0)

    def place(b):
        return b // 4, lax.rem(b // 2, 2), pl.ds(pl.multiple_of(lax.rem(b, 2) * rows, rows), rows)

    def load_x(b):
        @pl.when(first & (b < n_blocks))
        def _():
            mb, seq, r = place(b)
            pltpu.make_async_copy(x_in.at[mb, seq, r, :], xbuf.at[lax.rem(b, 2)], xload_sem).start()

    def remote(src, dst, send_sem, recv_sem, to=peer):
        return pltpu.make_async_remote_copy(src, dst, send_sem, recv_sem, device_id=to, device_id_type=MESH)

    def signal(sem, to):
        pl.semaphore_signal(sem, inc=1, device_id=to, device_id_type=MESH)

    def bq_copy():
        return remote(bq, bq_all.at[pl.ds(heads_half, heads_half)], bq_sem.at[0], bq_sem.at[1])

    def piece(i, kind):
        ref = {'here': (wq.at[0], wo.at[0]), 'there': (wq_peer, wo_peer), 'a': (qa, oa), 'b': (qb, ob)}[kind][i // PARTS]
        n = (hidden, half)[i // PARTS] // PARTS
        return ref.at[pl.ds((i % PARTS) * n, n), :]

    def w_copy(i):
        return remote(piece(i, 'here'), piece(i, 'there'), w_send_sem.at[i], w_recv_sem.at[i])

    def hop_a(i):
        return remote(piece(i, 'here'), piece(i, 'a'), w_send_sem.at[i], ra_recv_sem.at[i], across)

    def hop_b(i):
        return remote(piece(i, 'a'), piece(i, 'b'), rb_send_sem.at[i], rb_recv_sem.at[i])

    def hop_c(i):
        return remote(piece(i, 'b'), piece(i, 'there'), rc_send_sem.at[i], w_recv_sem.at[i], across)

    barrier = pltpu.get_barrier_semaphore()
    signal(barrier, peer)

    @pl.when(stage > 0)
    def _():
        signal(barrier, prv)

    @pl.when(jnp.logical_not(last))
    def _():
        signal(barrier, nxt)

    @pl.when(jnp.logical_not(even))
    def _():
        signal(barrier, across)

    pl.semaphore_wait(barrier, 1 + (stage > 0).astype(jnp.int32) + (stage < n_stages - 1).astype(jnp.int32) + 1 - even.astype(jnp.int32))

    bq_copy().start()

    @pl.when(second)
    def _():
        for i in range(RELAYED):
            hop_a(i).start()
        scoped('go_wait', pl.semaphore_wait, go_sem, 1)
        for i in range(RELAYED, 2 * PARTS):
            w_copy(i).start()

    @pl.when(last)
    def _():
        for i in range(RELAYED + 1):
            if i < RELAYED:
                hop_a(i).wait_recv()
                hop_b(i).start()
            if i > 0:
                hop_b(i - 1).wait_recv()
                hop_c(i - 1).start()
        for i in range(RELAYED):
            hop_b(i).wait_send()
        signal(clear_sem, prv)
        scoped('go_wait', pl.semaphore_wait, go_sem, 1)

    @pl.when(third)
    def _():
        scoped('go_wait', pl.semaphore_wait, clear_sem, 1)

    @pl.when(jnp.logical_not(second))
    def _():
        for i in range(2 * PARTS):
            w_copy(i).start()

    bq_all[pl.ds(0, heads_half)] = bq[...]
    vones[:, :, HEAD:] = jnp.ones((2, 4 * rows, HEAD), BF16)

    zero = jnp.int32(0)
    own_chunks = 1 + heads_half // 2

    @pl.when(leads)
    def _():
        for i in range(min(SLOTS, own_chunks)):
            start_chunk(zero, KVQ, jnp.int32(i))

    @pl.when(jnp.logical_not(leads))
    def _():
        for i in range(SLOTS):
            start_chunk(zero, UP2, jnp.int32(i))

    load_x(zero)
    bq_copy().wait_recv()
    with jax.named_scope('wq_wait'):
        for i in range(PARTS):
            w_copy(i).wait_recv()

    @pl.when(leads)
    def _():
        for i in range(min(SLOTS, own_chunks), min(SLOTS, counts[KVQ])):
            start_chunk(zero, KVQ, jnp.int32(i))

    bq_copy().wait_send()

    @pl.when(even)
    def _():
        for i in range(2 * PARTS):
            w_copy(i).wait_send()
        signal(go_sem, nxt)

    with jax.named_scope('wo_wait'):
        for i in range(PARTS, 2 * PARTS):
            w_copy(i).wait_recv()

    @pl.when(leads)
    def _():
        for i in range(counts[KVQ], SLOTS):
            start_chunk(zero, O, jnp.int32(i - counts[KVQ]))

    for i in range(AHEAD):
        wait_chunk(zero + i)

    def attention(j, seq):
        factor = HEAD ** -0.5 * 1.4426950408889634

        def two_heads(jj, i):
            kts, vs = kt.at[seq], vones.at[seq]
            q = qbuf[pl.ds(2 * i, 2)].reshape(2 * rows, HEAD)
            sd = jnp.dot(q, kts[:, jj * rows:(jj + 1) * rows], preferred_element_type=F32)
            row = jnp.bitwise_and(lax.broadcasted_iota(jnp.int32, (2 * rows, rows), 0), rows - 1)
            col = lax.broadcasted_iota(jnp.int32, (2 * rows, rows), 1)
            sd = jnp.where(col <= row, sd, -1e30)
            top = jnp.max(sd, axis=-1, keepdims=True)
            if jj:
                so = jnp.dot(q, kts[:, :jj * rows], preferred_element_type=F32)
                top = jnp.maximum(top, jnp.max(so, axis=-1, keepdims=True))
            pd = jnp.exp2((sd - top) * factor).astype(BF16)
            acc = jnp.dot(pd, vs[jj * rows:(jj + 1) * rows, :], preferred_element_type=F32)
            if jj:
                po = jnp.exp2((so - top) * factor).astype(BF16)
                acc = acc + jnp.dot(po, vs[:jj * rows, :], preferred_element_type=F32)
            c = (acc[:, :HEAD] / acc[:, HEAD:]).astype(BF16)
            at = pl.multiple_of(i * 2 * HEAD, 2 * HEAD)
            cbuf[:, pl.ds(at, HEAD)] = c[:rows]
            cbuf[:, pl.ds(at + HEAD, HEAD)] = c[rows:]

        for jj in range(4):
            @pl.when(j == jj)
            def _():
                def body(i, carry):
                    two_heads(jj, i)
                    return carry

                lax.fori_loop(0, n_heads // 2, body, 0)

    def x1_copy(slot, start, width):
        cols = pl.ds(start, width)
        return remote(x1own.at[:, cols], x1recv.at[slot, :, cols], x1_send_sem, x1_recv_sem.at[slot])

    def p_copy(slot, c, n):
        cols = pl.ds(pl.multiple_of(c * CW, CW), n * CW)
        return remote(psend.at[:, cols], precv.at[slot, :, cols], p_send_sem, p_recv_sem.at[slot])

    def kv_copies(seq, part):
        at = pl.ds(pl.multiple_of(part * rows, rows), rows)
        sem = 2 * seq + part
        return (remote(kt.at[seq, :, at], kt.at[seq, :, at], kv_send_sem.at[0], k_recv_sem.at[sem]),
                remote(vones.at[seq, at, pl.ds(0, HEAD)], vones.at[seq, at, pl.ds(0, HEAD)], kv_send_sem.at[1], v_recv_sem.at[sem]))

    def attend(u):
        b = own_block(u)
        seq = lax.rem(b // 2, 2)
        part = lax.rem(b, 2)
        j = part + 2 * lag
        slot2 = lax.rem(u, 2)
        xslot = lax.rem(b, 2)
        at_kvq = base(u, KVQ)
        at_o = base(u, O)

        @pl.when(first)
        def _():
            pltpu.make_async_copy(x_in.at[0, 0, pl.ds(0, rows), :], xbuf.at[xslot], xload_sem).wait()

        @pl.when(jnp.logical_not(first))
        def _():
            scoped('x_wait', remote(ybuf, xbuf.at[xslot], y_send_sem, xslot_sem.at[xslot], nxt).wait_recv)

        scoped('ln1', layer_norm, xbuf.at[xslot], hbuf, g1, s1)

        @pl.when(leads & (b > 0))
        def _():
            for copy in kv_copies(seq, part):
                copy.wait_send()

        def q_heads(c, slot):
            a = jnp.dot(hbuf[...], ring[slot], preferred_element_type=F32)
            qbuf[2 * c] = (a[:, :HEAD] + bq_all[2 * c]).astype(BF16)
            qbuf[2 * c + 1] = (a[:, HEAD:] + bq_all[2 * c + 1]).astype(BF16)

        wait_chunk(at_kvq + 4)
        wait_chunk(at_kvq + 5)
        kv = jnp.dot(hbuf[...], ring[slot_at(at_kvq)], preferred_element_type=F32) + bkv[...]
        at = pl.ds(pl.multiple_of(j * rows, rows), rows)
        kt[seq, :, at] = kv[:, :HEAD].astype(BF16).astype(F32).T.astype(BF16)
        vones[seq, at, :HEAD] = kv[:, HEAD:].astype(BF16)
        q_heads(0, slot_at(at_kvq + 1))

        @pl.when(leads)
        def _():
            for copy in kv_copies(seq, part):
                copy.start()

        prefetch(u, KVQ, zero)
        prefetch(u, KVQ, zero + 1)

        def q_body(i, carry):
            g = at_kvq + 2 * i
            wait_chunk(g + 4)
            wait_chunk(g + 5)
            q_heads(2 * i - 1, slot_at(g))
            q_heads(2 * i, slot_at(g + 1))
            prefetch(u, KVQ, 2 * i)
            prefetch(u, KVQ, 2 * i + 1)
            return carry

        scoped('q', lax.fori_loop, 1, (nq + 1) // 2, q_body, 0)

        @pl.when(jnp.logical_not(leads) & (part == 0))
        def _():
            with jax.named_scope('kv_wait'):
                for p in range(2):
                    for copy in kv_copies(seq, jnp.int32(p)):
                        copy.wait_recv()

        scoped('attn', attention, j, seq)


        @pl.when((u > 0) & valid(peer_block(u - 1)))
        def _():
            finish(u - 1)

        @pl.when(b > 0)
        def _():
            remote(x1own, x1recv.at[slot2], x1_send_sem, x1_recv_sem.at[slot2]).wait_send()

        def o_cols(c, slot):
            cols = pl.ds(pl.multiple_of(c * CW, CW), CW)
            a = jnp.dot(cbuf[...], ring[slot], preferred_element_type=F32)
            x1own[:, cols] = (xbuf[xslot, :, cols].astype(F32) + a + bo[c]).astype(BF16)

        def o_body(i, carry):
            g = at_o + 2 * i
            wait_chunk(g + 4)
            wait_chunk(g + 5)
            o_cols(2 * i, slot_at(g))
            o_cols(2 * i + 1, slot_at(g + 1))

            @pl.when(i > 0)
            def _():
                x1_copy(slot2, pl.multiple_of((i - 1) * 2 * CW, CW), 2 * CW).start()

            prefetch(u, O, 2 * i)
            prefetch(u, O, 2 * i + 1)
            return carry

        scoped('o', lax.fori_loop, 0, nq // 2, o_body, 0)
        wait_chunk(at_o + nq + 3)
        o_cols(nq - 1, slot_at(at_o + nq - 1))
        prefetch(u, O, jnp.int32(nq - 1))
        tail = (nq // 2 - 1) * 2 * CW
        x1_copy(slot2, tail, hidden - tail).start()

        @pl.when((stage > 0) & (b + 2 < n_blocks))
        def _():
            signal(credit_sem, prv)


    def down(u, phase):
        slot2 = lax.rem(u, 2)
        at_d = base(u, phase)
        own = phase == DOWN

        if own:
            @pl.when(own_block(u) > 0)
            def _():
                remote(psend, precv.at[slot2], p_send_sem, p_recv_sem.at[slot2]).wait_send()

        def column(c, g):
            cols = pl.ds(pl.multiple_of(c * CW, CW), CW)
            a = (jnp.dot(ubuf[:, :hidden], ring[slot_at(g)], preferred_element_type=F32)
                 + jnp.dot(ubuf[:, hidden:], ring[slot_at(g + 1)], preferred_element_type=F32))
            if own:
                psend[:, cols] = a.astype(BF16)
            else:
                zbuf[:, cols] = x1recv[slot2, :, cols].astype(F32) + a + bdn[c]

        more = u + 1 < n_steps
        full = nq // 2

        def body(i, carry):
            g = at_d + 4 * i
            wait_chunk(g + 4)
            wait_chunk(g + 5)

            @pl.when(more | (i < full - 1))
            def _():
                wait_chunk(g + 6)
                wait_chunk(g + 7)

            column(2 * i, g)
            column(2 * i + 1, g + 2)
            if own:
                @pl.when(i > 0)
                def _():
                    p_copy(slot2, 2 * i - 2, 2).start()

            for k in range(4):
                prefetch(u, phase, 4 * i + k)
            return carry

        def rest():
            g = at_d + 4 * full

            @pl.when(more)
            def _():
                wait_chunk(g + 4)
                wait_chunk(g + 5)

            column(zero + 2 * full, g)
            for k in range(2):
                prefetch(u, phase, zero + 4 * full + k)

        assert nq % 2 == 1 and nu % 4 == 2
        with jax.named_scope('down' if own else 'down_peer'):
            lax.fori_loop(0, full, body, 0)
            rest()
        if own:
            p_copy(slot2, zero + 2 * full - 2, 3).start()

    def up(u, phase):
        at_u = base(u, phase)

        def cols_of(c, slot):
            a = jnp.dot(hbuf[...], ring[slot], preferred_element_type=F32) + bup[c]
            t = jnp.tanh(0.7978845608028654 * (a + 0.044715 * (a * a * a)))
            ubuf[:, pl.ds(pl.multiple_of(c * CW, CW), CW)] = (0.5 * a * (1.0 + t)).astype(BF16)

        def body(i, carry):
            g = at_u + 4 * i
            for k in range(4, 8):
                wait_chunk(g + k)
            for k in range(4):
                cols_of(4 * i + k, slot_at(g + k))
            for k in range(4):
                prefetch(u, phase, 4 * i + k)
            return carry

        def rest():
            for k in range(4, 4 + nu % 4):
                wait_chunk(at_u + full * 4 + k)
            for k in range(nu % 4):
                cols_of(zero + full * 4 + k, slot_at(at_u + full * 4 + k))
            for k in range(nu % 4):
                prefetch(u, phase, zero + full * 4 + k)

        full = nu // 4
        with jax.named_scope('up' if phase == UP else 'up_peer'):
            lax.fori_loop(0, full, body, 0)
            rest()

    def finish(u):
        v = peer_block(u)
        slot = lax.rem(u, 2)
        scoped('p_wait', remote(psend, precv.at[slot], p_send_sem, p_recv_sem.at[slot]).wait_recv)

        @pl.when(v > 0)
        def _():
            scoped('y_wait', pltpu.make_async_copy(ybuf, out.at[0, 0, pl.ds(0, rows), :], y_send_sem).wait)

        block = 32

        def body(i, carry):
            r = pl.ds(pl.multiple_of(i * block, block), block)
            ybuf[r, :] = (zbuf[r, :] + precv[slot, r, :].astype(F32)).astype(BF16)
            return carry

        lax.fori_loop(0, rows // block, body, 0)

        @pl.when(jnp.logical_not(last))
        def _():
            @pl.when(v >= 2)
            def _():
                pl.semaphore_wait(credit_sem, 1)

            to = lax.rem(v, 2)
            remote(ybuf, xbuf.at[to], y_send_sem, xslot_sem.at[to], nxt).start()

        @pl.when(last)
        def _():
            mb, seq, r = place(v)
            pltpu.make_async_copy(ybuf, out.at[mb, seq, r, :], y_send_sem).start()

    def step(u, carry):
        slot2 = lax.rem(u, 2)

        @pl.when(valid(own_block(u)))
        def _():
            attend(u)
            scoped('ln2', layer_norm, x1own, hbuf, g2, s2)
            up(u, UP)
            load_x(own_block(u) + 1)
            down(u, DOWN)

        @pl.when(leads & (u == n_steps - 1))
        def _():
            finish(u - 1)

        @pl.when(valid(peer_block(u)))
        def _():
            scoped('x1_wait', remote(x1own, x1recv.at[slot2], x1_send_sem, x1_recv_sem.at[slot2]).wait_recv)
            scoped('ln_peer', layer_norm, x1recv.at[slot2], hbuf, g2, s2)
            up(u, UP2)
            down(u, DOWN2)

        return carry

    lax.fori_loop(0, n_steps, step, 0)

    @pl.when(leads)
    def _():
        finish(zero + n_steps - 1)


    remote(x1own, x1recv.at[0], x1_send_sem, x1_recv_sem.at[0]).wait_send()
    remote(psend, precv.at[0], p_send_sem, p_recv_sem.at[0]).wait_send()
    pltpu.make_async_copy(ybuf, out.at[0, 0, pl.ds(0, rows), :], y_send_sem).wait()

    @pl.when(leads)
    def _():
        for copy in kv_copies(zero, zero):
            copy.wait_send()

    @pl.when(jnp.logical_not(even))
    def _():
        for i in range(2 * PARTS):
            w_copy(i).wait_send()

    @pl.when(last)
    def _():
        for i in range(RELAYED):
            hop_c(i).wait_send()


def run_stage(x_loc, params, n_stages):
    (ln1_gain, ln1_bias, w_q, b_q, w_kv, b_kv, w_o, b_o, ln2_gain, ln2_bias, w_up, b_up, w_down, b_down) = params
    n_micro, _, seq_loc, hidden = x_loc.shape
    ffn_loc = w_up.shape[2]
    rows = seq_loc // 2
    n_blocks = 4 * n_micro
    nq = hidden // CW
    nu = ffn_loc // CW
    heads_half = hidden // 2 // HEAD
    cfg = (n_stages, n_blocks, rows, hidden, ffn_loc)
    vmem = pl.BlockSpec(memory_space=pltpu.VMEM)
    anym = pl.BlockSpec(memory_space=pl.ANY)
    args = (
        x_loc, ln1_gain, ln1_bias, w_q, b_q.reshape(heads_half, 1, HEAD), w_kv, b_kv, w_o, b_o.reshape(nq, 1, CW),
        ln2_gain, ln2_bias, w_up, b_up.reshape(nu, 1, CW), w_down, b_down.reshape(nq, 1, CW),
    )
    in_specs = [anym, vmem, vmem, anym, vmem, anym, vmem, anym, vmem, vmem, vmem, anym, vmem, anym, vmem]
    half = hidden // 2
    out_shape = (
        jax.ShapeDtypeStruct(x_loc.shape, BF16),
        jax.ShapeDtypeStruct((hidden, half), BF16),
        jax.ShapeDtypeStruct((half, hidden), BF16),
        jax.ShapeDtypeStruct((hidden, half), BF16),
        jax.ShapeDtypeStruct((hidden, half), BF16),
        jax.ShapeDtypeStruct((half, hidden), BF16),
        jax.ShapeDtypeStruct((half, hidden), BF16),
    )
    dma = pltpu.SemaphoreType.DMA
    scratch = [
        pltpu.VMEM((SLOTS, hidden, CW), BF16),
        pltpu.VMEM((2, rows, hidden), BF16),
        pltpu.VMEM((rows, hidden), BF16),
        pltpu.VMEM((2 * heads_half, rows, HEAD), BF16),
        pltpu.VMEM((rows, hidden), BF16),
        pltpu.VMEM((rows, hidden), BF16),
        pltpu.VMEM((2, rows, hidden), BF16),
        pltpu.VMEM((rows, ffn_loc), BF16),
        pltpu.VMEM((rows, hidden), F32),
        pltpu.VMEM((rows, hidden), BF16),
        pltpu.VMEM((2, rows, hidden), BF16),
        pltpu.VMEM((rows, hidden), BF16),
        pltpu.VMEM((2, HEAD, 4 * rows), BF16),
        pltpu.VMEM((2, 4 * rows, 2 * HEAD), BF16),
        pltpu.VMEM((2 * heads_half, 1, HEAD), F32),
        dma((SLOTS,)),
        dma,
        dma((2,)),
        dma((2,)),
        dma((2 * PARTS,)),
        dma((2 * PARTS,)),
        dma((RELAYED,)),
        dma((RELAYED,)),
        dma((RELAYED,)),
        dma((RELAYED,)),
        dma((2,)),
        dma((4,)),
        dma((4,)),
        dma,
        dma((2,)),
        dma,
        dma((2,)),
        dma,
        pltpu.SemaphoreType.REGULAR,
        pltpu.SemaphoreType.REGULAR,
        pltpu.SemaphoreType.REGULAR,
    ]
    return pl.pallas_call(
        functools.partial(stage_kernel, cfg),
        out_shape=out_shape,
        in_specs=in_specs,
        out_specs=(anym,) * 7,
        scratch_shapes=scratch,
        compiler_params=pltpu.CompilerParams(collective_id=0, has_side_effects=True, vmem_limit_bytes=60 * 2 ** 20),
        name='stage_loop',
    )(*args)[0]


def solution(mesh):
    pp_size = mesh.shape['pp']

    def stage_program(x_loc, *params):
        result = run_stage(x_loc, params, pp_size)
        is_last = lax.axis_index('pp') == pp_size - 1
        return jnp.where(is_last, result, jnp.zeros_like(result))[None]

    return jax.shard_map(stage_program, mesh=mesh, in_specs=(P(None, 'dp', 'tp', None),) + PARAM_SPECS, out_specs=P('pp', None, 'dp', 'tp', None), check_vma=False)
```

```python
import functools

import jax
import jax.numpy as jnp
from jax import lax
from jax.experimental import pallas as pl
from jax.experimental.pallas import tpu as pltpu
from jax.sharding import PartitionSpec as P

F32 = jnp.float32
BF16 = jnp.bfloat16
MESH = pl.DeviceIdType.MESH

PARAM_SPECS = (P('pp', None), P('pp', None), P('pp', None, 'tp'), P('pp', 'tp'), P('pp', None, None), P('pp', None), P('pp', 'tp', None), P('pp', None), P('pp', None), P('pp', None), P('pp', None, 'tp'), P('pp', 'tp'), P('pp', 'tp', None), P('pp', None))

CW = 256
HEAD = 128
SLOTS = 14
KEPT = 8
AHEAD = 4
PARTS = 4
RELAYED = 4


def scoped(name, fn, *args):
    with jax.named_scope(name):
        return fn(*args)


def stage_kernel(cfg, x_in, g1, s1, wq, bq, wkv, bkv, wo, bo, g2, s2, wup, bup, wdn, bdn,
                 out, wq_peer, wo_peer, qa, qb, oa, ob,
                 ring, kept, xbuf, hbuf, qbuf, cbuf, x1own, x1recv, ubuf, zbuf, psend, precv, ybuf, kt, vones, bq_all,
                 ring_sem, kept_sem, xload_sem, xslot_sem, bq_sem, w_send_sem, w_recv_sem, ra_recv_sem, rb_send_sem, rb_recv_sem, rc_send_sem,
                 kv_send_sem, k_recv_sem, v_recv_sem,
                 x1_send_sem, x1_recv_sem, p_send_sem, p_recv_sem, y_send_sem, go_sem, clear_sem, credit_sem):
    (n_stages, n_blocks, rows, hidden, ffn_loc) = cfg
    half = hidden // 2
    nq = hidden // CW
    nu = ffn_loc // CW
    heads_half = half // HEAD
    n_heads = 2 * heads_half
    stage = lax.axis_index('pp')
    rank = lax.axis_index('tp')
    peer = {'tp': 1 - rank}
    nxt = {'pp': jnp.minimum(stage + 1, n_stages - 1)}
    prv = {'pp': jnp.maximum(stage - 1, 0)}
    across = {'pp': 4 - stage}
    first = stage == 0
    second = stage == 1
    third = stage == 2
    last = stage == n_stages - 1
    even = lax.rem(stage, 2) == 0

    leads = lax.rem(rank + stage, 2) == 0
    lag = 1 - leads.astype(jnp.int32)
    n_steps = n_blocks + 1

    def own_block(k):
        return k - lag

    def peer_block(k):
        return k - 1 + lag

    def valid(b):
        return (b >= 0) & (b < n_blocks)

    KVQ, O, UP, DOWN, UP2, DOWN2 = 0, 1, 2, 3, 4, 5
    ns = nu - KEPT
    counts = (1 + nq, nq, ns, 2 * nq, ns, 2 * nq)
    own_count = sum(counts[:4])
    peer_count = sum(counts[4:])

    def base(k, phase):
        start = k * (own_count + peer_count) - jnp.where(k > 0, jnp.where(leads, peer_count, own_count), 0)
        if phase < UP2:
            return start + sum(counts[:phase])
        return start + jnp.where(valid(own_block(k)), own_count, 0) + sum(counts[UP2:phase])

    def slot_at(g):
        return lax.rem(g, SLOTS)

    def start_chunk(u, phase, idx):
        slot = slot_at(base(u, phase) + idx)
        dst = ring.at[slot]
        sem = ring_sem.at[slot]

        def cols(c, width):
            return pl.ds(pl.multiple_of(c * width, width), width)

        if phase == KVQ:
            @pl.when(idx == 0)
            def _():
                pltpu.make_async_copy(wkv.at[0], dst, sem).start()

            for b in range(2):
                block = (idx - 1) * 2 + b
                piece = dst.at[:, pl.ds(b * HEAD, HEAD)]

                @pl.when((idx > 0) & (block < heads_half))
                def _():
                    pltpu.make_async_copy(wq.at[0, :, cols(block, HEAD)], piece, sem).start()

                @pl.when((idx > 0) & (block >= heads_half))
                def _():
                    pltpu.make_async_copy(wq_peer.at[:, cols(block - heads_half, HEAD)], piece, sem).start()
        elif phase == O:
            pltpu.make_async_copy(wo.at[0, :, cols(idx, CW)], dst.at[pl.ds(0, half), :], sem).start()
            pltpu.make_async_copy(wo_peer.at[:, cols(idx, CW)], dst.at[pl.ds(half, half), :], sem).start()
        elif phase in (UP, UP2):
            pltpu.make_async_copy(wup.at[0, :, cols(idx + KEPT, CW)], dst, sem).start()
        else:
            part = lax.rem(idx, 2)
            pltpu.make_async_copy(
                wdn.at[0, pl.ds(pl.multiple_of(part * hidden, hidden), hidden), cols(idx // 2, CW)], dst, sem).start()

    def start_at(u, part, pos, phases):
        firsts = KVQ if part == 0 else UP2
        for i, phase in enumerate(phases):
            low = sum(counts[firsts:phase])
            inside = (pos >= low) & (pos < low + counts[phase])

            @pl.when(inside)
            def _():
                start_chunk(u, phase, pos - low)

    def prefetch(u, phase, idx):
        part = 0 if phase < UP2 else 1
        length = (own_count, peer_count)[part]
        low = sum(counts[KVQ if part == 0 else UP2:phase])
        pos = idx + low + SLOTS
        last_phase = DOWN if part == 0 else DOWN2
        reach = [p for p in range(phase, last_phase + 1)]
        start_at(u, part, pos, reach[:3])
        if phase == last_phase:
            past = pos >= length
            peer_next = valid(peer_block(u)) if part == 0 else (u + 1 < n_steps) & jnp.logical_not(valid(own_block(u + 1)))
            own_next = (jnp.logical_not(valid(peer_block(u))) if part == 0 else True) & (u + 1 < n_steps) & valid(own_block(u + 1))

            @pl.when(past & peer_next)
            def _():
                start_at(u if part == 0 else u + 1, 1, pos - length, (UP2, DOWN2))

            @pl.when(past & own_next)
            def _():
                start_at(u + 1, 0, pos - length, (KVQ, O, UP))

    def wait_chunk(g):
        slot = slot_at(g)
        pltpu.make_async_copy(wkv.at[0], ring.at[slot], ring_sem.at[slot]).wait()

    def layer_norm(src, dst, gain, shift):
        block = min(128, rows)
        pieces = [pl.ds(k * CW, CW) for k in range(hidden // CW)]

        def body(i, carry):
            at = pl.multiple_of(i * block, block)
            r = pl.ds(at, block)
            total = src[r, pieces[0]].astype(F32)
            for p in pieces[1:]:
                total = total + src[r, p].astype(F32)
            mean = jnp.sum(total, axis=-1, keepdims=True) * (1.0 / hidden)
            square = None
            for p in pieces:
                cen = src[r, p].astype(F32) - mean
                square = cen * cen if square is None else square + cen * cen
            inv = lax.rsqrt(jnp.sum(square, axis=-1, keepdims=True) * (1.0 / hidden) + 1e-5)
            for p in pieces:
                cen = src[r, p].astype(F32) - mean
                dst[r, p] = (cen * inv * gain[:, p] + shift[:, p]).astype(BF16)
            return carry

        lax.fori_loop(0, rows // block, body, 0)

    def place(b):
        return b // 4, lax.rem(b // 2, 2), pl.ds(pl.multiple_of(lax.rem(b, 2) * rows, rows), rows)

    def load_x(b):
        @pl.when(first & (b < n_blocks))
        def _():
            mb, seq, r = place(b)
            pltpu.make_async_copy(x_in.at[mb, seq, r, :], xbuf.at[lax.rem(b, 2)], xload_sem).start()

    def remote(src, dst, send_sem, recv_sem, to=peer):
        return pltpu.make_async_remote_copy(src, dst, send_sem, recv_sem, device_id=to, device_id_type=MESH)

    def signal(sem, to):
        pl.semaphore_signal(sem, inc=1, device_id=to, device_id_type=MESH)

    def bq_copy():
        return remote(bq, bq_all.at[pl.ds(heads_half, heads_half)], bq_sem.at[0], bq_sem.at[1])

    def piece(i, kind):
        ref = {'here': (wq.at[0], wo.at[0]), 'there': (wq_peer, wo_peer), 'a': (qa, oa), 'b': (qb, ob)}[kind][i // PARTS]
        n = (hidden, half)[i // PARTS] // PARTS
        return ref.at[pl.ds((i % PARTS) * n, n), :]

    def w_copy(i):
        return remote(piece(i, 'here'), piece(i, 'there'), w_send_sem.at[i], w_recv_sem.at[i])

    def hop_a(i):
        return remote(piece(i, 'here'), piece(i, 'a'), w_send_sem.at[i], ra_recv_sem.at[i], across)

    def hop_b(i):
        return remote(piece(i, 'a'), piece(i, 'b'), rb_send_sem.at[i], rb_recv_sem.at[i])

    def hop_c(i):
        return remote(piece(i, 'b'), piece(i, 'there'), rc_send_sem.at[i], w_recv_sem.at[i], across)

    barrier = pltpu.get_barrier_semaphore()
    signal(barrier, peer)

    @pl.when(stage > 0)
    def _():
        signal(barrier, prv)

    @pl.when(jnp.logical_not(last))
    def _():
        signal(barrier, nxt)

    @pl.when(jnp.logical_not(even))
    def _():
        signal(barrier, across)

    pl.semaphore_wait(barrier, 1 + (stage > 0).astype(jnp.int32) + (stage < n_stages - 1).astype(jnp.int32) + 1 - even.astype(jnp.int32))

    bq_copy().start()

    @pl.when(second)
    def _():
        for i in range(RELAYED):
            hop_a(i).start()
        scoped('go_wait', pl.semaphore_wait, go_sem, 1)
        for i in range(RELAYED, 2 * PARTS):
            w_copy(i).start()

    @pl.when(last)
    def _():
        for i in range(RELAYED + 1):
            if i < RELAYED:
                hop_a(i).wait_recv()
                hop_b(i).start()
            if i > 0:
                hop_b(i - 1).wait_recv()
                hop_c(i - 1).start()
        for i in range(RELAYED):
            hop_b(i).wait_send()
        signal(clear_sem, prv)
        scoped('go_wait', pl.semaphore_wait, go_sem, 1)

    @pl.when(third)
    def _():
        scoped('go_wait', pl.semaphore_wait, clear_sem, 1)

    @pl.when(jnp.logical_not(second))
    def _():
        for i in range(2 * PARTS):
            w_copy(i).start()

    bq_all[pl.ds(0, heads_half)] = bq[...]
    vones[:, :, HEAD:] = jnp.ones((2, 4 * rows, HEAD), BF16)

    zero = jnp.int32(0)
    own_chunks = 1 + heads_half // 2

    @pl.when(leads)
    def _():
        for i in range(min(SLOTS, own_chunks)):
            start_chunk(zero, KVQ, jnp.int32(i))

    @pl.when(jnp.logical_not(leads))
    def _():
        for i in range(SLOTS):
            start_at(zero, 1, zero + i, (UP2, DOWN2))

    def kept_copy(i):
        return pltpu.make_async_copy(wup.at[0, :, pl.ds(i * CW, CW)], kept.at[i], kept_sem.at[i])

    for i in range(KEPT):
        kept_copy(i).start()

    load_x(zero)
    bq_copy().wait_recv()
    with jax.named_scope('wq_wait'):
        for i in range(PARTS):
            w_copy(i).wait_recv()

    @pl.when(leads)
    def _():
        for i in range(min(SLOTS, own_chunks), min(SLOTS, counts[KVQ])):
            start_chunk(zero, KVQ, jnp.int32(i))

    bq_copy().wait_send()

    @pl.when(even)
    def _():
        for i in range(2 * PARTS):
            w_copy(i).wait_send()
        signal(go_sem, nxt)

    with jax.named_scope('wo_wait'):
        for i in range(PARTS, 2 * PARTS):
            w_copy(i).wait_recv()

    for i in range(KEPT):
        kept_copy(i).wait()

    @pl.when(leads)
    def _():
        for i in range(counts[KVQ], SLOTS):
            start_chunk(zero, O, jnp.int32(i - counts[KVQ]))

    for i in range(AHEAD):
        wait_chunk(zero + i)

    def attention(j, seq):
        factor = HEAD ** -0.5 * 1.4426950408889634

        def two_heads(jj, i):
            kts, vs = kt.at[seq], vones.at[seq]
            q = qbuf[pl.ds(2 * i, 2)].reshape(2 * rows, HEAD)
            sd = jnp.dot(q, kts[:, jj * rows:(jj + 1) * rows], preferred_element_type=F32)
            row = jnp.bitwise_and(lax.broadcasted_iota(jnp.int32, (2 * rows, rows), 0), rows - 1)
            col = lax.broadcasted_iota(jnp.int32, (2 * rows, rows), 1)
            sd = jnp.where(col <= row, sd, -1e30)
            top = jnp.max(sd, axis=-1, keepdims=True)
            if jj:
                so = jnp.dot(q, kts[:, :jj * rows], preferred_element_type=F32)
                top = jnp.maximum(top, jnp.max(so, axis=-1, keepdims=True))
            pd = jnp.exp2((sd - top) * factor).astype(BF16)
            acc = jnp.dot(pd, vs[jj * rows:(jj + 1) * rows, :], preferred_element_type=F32)
            if jj:
                po = jnp.exp2((so - top) * factor).astype(BF16)
                acc = acc + jnp.dot(po, vs[:jj * rows, :], preferred_element_type=F32)
            c = (acc[:, :HEAD] / acc[:, HEAD:]).astype(BF16)
            at = pl.multiple_of(i * 2 * HEAD, 2 * HEAD)
            cbuf[:, pl.ds(at, HEAD)] = c[:rows]
            cbuf[:, pl.ds(at + HEAD, HEAD)] = c[rows:]

        for jj in range(4):
            @pl.when(j == jj)
            def _():
                def body(i, carry):
                    two_heads(jj, i)
                    return carry

                lax.fori_loop(0, n_heads // 2, body, 0)

    def x1_copy(slot, start, width):
        cols = pl.ds(start, width)
        return remote(x1own.at[:, cols], x1recv.at[slot, :, cols], x1_send_sem, x1_recv_sem.at[slot])

    def p_copy(slot, c, n):
        cols = pl.ds(pl.multiple_of(c * CW, CW), n * CW)
        return remote(psend.at[:, cols], precv.at[slot, :, cols], p_send_sem, p_recv_sem.at[slot])

    def kv_copies(seq, part):
        at = pl.ds(pl.multiple_of(part * rows, rows), rows)
        sem = 2 * seq + part
        return (remote(kt.at[seq, :, at], kt.at[seq, :, at], kv_send_sem.at[0], k_recv_sem.at[sem]),
                remote(vones.at[seq, at, pl.ds(0, HEAD)], vones.at[seq, at, pl.ds(0, HEAD)], kv_send_sem.at[1], v_recv_sem.at[sem]))

    def attend(u):
        b = own_block(u)
        seq = lax.rem(b // 2, 2)
        part = lax.rem(b, 2)
        j = part + 2 * lag
        slot2 = lax.rem(u, 2)
        xslot = lax.rem(b, 2)
        at_kvq = base(u, KVQ)
        at_o = base(u, O)

        @pl.when(first)
        def _():
            pltpu.make_async_copy(x_in.at[0, 0, pl.ds(0, rows), :], xbuf.at[xslot], xload_sem).wait()

        @pl.when(jnp.logical_not(first))
        def _():
            scoped('x_wait', remote(ybuf, xbuf.at[xslot], y_send_sem, xslot_sem.at[xslot], nxt).wait_recv)

        scoped('ln1', layer_norm, xbuf.at[xslot], hbuf, g1, s1)

        @pl.when(leads & (b > 0))
        def _():
            for copy in kv_copies(seq, part):
                copy.wait_send()

        def q_heads(c, slot):
            a = jnp.dot(hbuf[...], ring[slot], preferred_element_type=F32)
            qbuf[2 * c] = (a[:, :HEAD] + bq_all[2 * c]).astype(BF16)
            qbuf[2 * c + 1] = (a[:, HEAD:] + bq_all[2 * c + 1]).astype(BF16)

        wait_chunk(at_kvq + 4)
        wait_chunk(at_kvq + 5)
        kv = jnp.dot(hbuf[...], ring[slot_at(at_kvq)], preferred_element_type=F32) + bkv[...]
        at = pl.ds(pl.multiple_of(j * rows, rows), rows)
        kt[seq, :, at] = kv[:, :HEAD].astype(BF16).astype(F32).T.astype(BF16)
        vones[seq, at, :HEAD] = kv[:, HEAD:].astype(BF16)
        q_heads(0, slot_at(at_kvq + 1))

        @pl.when(leads)
        def _():
            for copy in kv_copies(seq, part):
                copy.start()

        prefetch(u, KVQ, zero)
        prefetch(u, KVQ, zero + 1)

        def q_group(first_q, n, waits):
            g = at_kvq + 1 + first_q
            for k in range(waits):
                wait_chunk(g + 4 + k)
            for k in range(n):
                q_heads(first_q + k, slot_at(g + k))
            for k in range(n):
                prefetch(u, KVQ, first_q + 1 + k)

        def q_body(i, carry):
            q_group(4 * i + 1, 4, 4)
            return carry

        with jax.named_scope('q'):
            lax.fori_loop(0, (nq - 1) // 4, q_body, 0)
            rest_q = (nq - 1) % 4
            if rest_q:
                q_group(zero + nq - rest_q, rest_q, rest_q)

        @pl.when(jnp.logical_not(leads) & (part == 0))
        def _():
            with jax.named_scope('kv_wait'):
                for p in range(2):
                    for copy in kv_copies(seq, jnp.int32(p)):
                        copy.wait_recv()

        scoped('attn', attention, j, seq)


        @pl.when((u > 0) & valid(peer_block(u - 1)))
        def _():
            finish(u - 1)

        @pl.when(b > 0)
        def _():
            remote(x1own, x1recv.at[slot2], x1_send_sem, x1_recv_sem.at[slot2]).wait_send()

        def o_cols(c, slot):
            cols = pl.ds(pl.multiple_of(c * CW, CW), CW)
            a = jnp.dot(cbuf[...], ring[slot], preferred_element_type=F32)
            x1own[:, cols] = (xbuf[xslot, :, cols].astype(F32) + a + bo[c]).astype(BF16)

        def o_group(c, n, waits):
            g = at_o + c
            for k in range(waits):
                wait_chunk(g + 4 + k)
            for k in range(n):
                o_cols(c + k, slot_at(g + k))

        def o_body(i, carry):
            o_group(4 * i, 4, 4)

            @pl.when(i > 0)
            def _():
                x1_copy(slot2, pl.multiple_of((i - 1) * 4 * CW, CW), 4 * CW).start()

            for k in range(4):
                prefetch(u, O, 4 * i + k)
            return carry

        with jax.named_scope('o'):
            lax.fori_loop(0, nq // 4, o_body, 0)
            tail = (nq // 4 - 1) * 4 * CW
            x1_copy(slot2, tail, 4 * CW).start()
            rest_o = nq % 4
            o_group(zero + nq - rest_o, rest_o, rest_o)
            for k in range(rest_o):
                prefetch(u, O, zero + nq - rest_o + k)
        x1_copy(slot2, tail + 4 * CW, rest_o * CW).start()

        @pl.when((stage > 0) & (b + 2 < n_blocks))
        def _():
            signal(credit_sem, prv)


    def down(u, phase):
        slot2 = lax.rem(u, 2)
        at_d = base(u, phase)
        own = phase == DOWN

        if own:
            @pl.when(own_block(u) > 0)
            def _():
                remote(psend, precv.at[slot2], p_send_sem, p_recv_sem.at[slot2]).wait_send()

        def column(c, g):
            cols = pl.ds(pl.multiple_of(c * CW, CW), CW)
            a = (jnp.dot(ubuf[:, :hidden], ring[slot_at(g)], preferred_element_type=F32)
                 + jnp.dot(ubuf[:, hidden:], ring[slot_at(g + 1)], preferred_element_type=F32))
            if own:
                psend[:, cols] = a.astype(BF16)
            else:
                zbuf[:, cols] = x1recv[slot2, :, cols].astype(F32) + a + bdn[c]

        more = u + 1 < n_steps
        full = nq // 2

        def body(i, carry):
            g = at_d + 4 * i
            wait_chunk(g + 4)
            wait_chunk(g + 5)

            @pl.when(more | (i < full - 1))
            def _():
                wait_chunk(g + 6)
                wait_chunk(g + 7)

            column(2 * i, g)
            column(2 * i + 1, g + 2)
            if own:
                @pl.when(i > 0)
                def _():
                    p_copy(slot2, 2 * i - 2, 2).start()

            for k in range(4):
                prefetch(u, phase, 4 * i + k)
            return carry

        def rest():
            g = at_d + 4 * full

            @pl.when(more)
            def _():
                wait_chunk(g + 4)
                wait_chunk(g + 5)

            column(zero + 2 * full, g)
            for k in range(2):
                prefetch(u, phase, zero + 4 * full + k)

        assert nq % 2 == 1 and ns % 4 == 2 and KEPT % 4 == 0
        with jax.named_scope('down' if own else 'down_peer'):
            lax.fori_loop(0, full, body, 0)
            rest()
        if own:
            p_copy(slot2, zero + 2 * full - 2, 3).start()

    def up(u, phase):
        at_u = base(u, phase)

        def cols_of(c, chunk):
            a = jnp.dot(hbuf[...], chunk, preferred_element_type=F32) + bup[c]
            t = jnp.tanh(0.7978845608028654 * (a + 0.044715 * (a * a * a)))
            ubuf[:, pl.ds(pl.multiple_of(c * CW, CW), CW)] = (0.5 * a * (1.0 + t)).astype(BF16)

        def body(i, carry):
            g = at_u + 4 * i
            for k in range(4, 8):
                wait_chunk(g + k)
            for k in range(4):
                cols_of(KEPT + 4 * i + k, ring[slot_at(g + k)])
            for k in range(4):
                prefetch(u, phase, 4 * i + k)
            return carry

        def rest():
            for k in range(4, 4 + ns % 4):
                wait_chunk(at_u + full * 4 + k)
            for k in range(ns % 4):
                cols_of(zero + KEPT + full * 4 + k, ring[slot_at(at_u + full * 4 + k)])
            for k in range(ns % 4):
                prefetch(u, phase, zero + full * 4 + k)

        def kept_body(i, carry):
            for k in range(4):
                cols_of(4 * i + k, kept[4 * i + k])
            return carry

        full = ns // 4
        with jax.named_scope('up' if phase == UP else 'up_peer'):
            lax.fori_loop(0, KEPT // 4, kept_body, 0)
            lax.fori_loop(0, full, body, 0)
            rest()

    def finish(u):
        v = peer_block(u)
        slot = lax.rem(u, 2)
        scoped('p_wait', remote(psend, precv.at[slot], p_send_sem, p_recv_sem.at[slot]).wait_recv)

        @pl.when(v > 0)
        def _():
            scoped('y_wait', pltpu.make_async_copy(ybuf, out.at[0, 0, pl.ds(0, rows), :], y_send_sem).wait)

        block = 32

        def body(i, carry):
            r = pl.ds(pl.multiple_of(i * block, block), block)
            ybuf[r, :] = (zbuf[r, :] + precv[slot, r, :].astype(F32)).astype(BF16)
            return carry

        lax.fori_loop(0, rows // block, body, 0)

        @pl.when(jnp.logical_not(last))
        def _():
            @pl.when(v >= 2)
            def _():
                pl.semaphore_wait(credit_sem, 1)

            to = lax.rem(v, 2)
            remote(ybuf, xbuf.at[to], y_send_sem, xslot_sem.at[to], nxt).start()

        @pl.when(last)
        def _():
            mb, seq, r = place(v)
            pltpu.make_async_copy(ybuf, out.at[mb, seq, r, :], y_send_sem).start()

    def step(u, carry):
        slot2 = lax.rem(u, 2)

        @pl.when(valid(own_block(u)))
        def _():
            attend(u)
            scoped('ln2', layer_norm, x1own, hbuf, g2, s2)
            up(u, UP)
            load_x(own_block(u) + 1)
            down(u, DOWN)

        @pl.when(leads & (u == n_steps - 1))
        def _():
            finish(u - 1)

        @pl.when(valid(peer_block(u)))
        def _():
            scoped('x1_wait', remote(x1own, x1recv.at[slot2], x1_send_sem, x1_recv_sem.at[slot2]).wait_recv)
            scoped('ln_peer', layer_norm, x1recv.at[slot2], hbuf, g2, s2)
            up(u, UP2)
            down(u, DOWN2)

        return carry

    lax.fori_loop(0, n_steps, step, 0)

    @pl.when(leads)
    def _():
        finish(zero + n_steps - 1)


    remote(x1own, x1recv.at[0], x1_send_sem, x1_recv_sem.at[0]).wait_send()
    remote(psend, precv.at[0], p_send_sem, p_recv_sem.at[0]).wait_send()
    pltpu.make_async_copy(ybuf, out.at[0, 0, pl.ds(0, rows), :], y_send_sem).wait()

    @pl.when(leads)
    def _():
        for copy in kv_copies(zero, zero):
            copy.wait_send()

    @pl.when(jnp.logical_not(even))
    def _():
        for i in range(2 * PARTS):
            w_copy(i).wait_send()

    @pl.when(last)
    def _():
        for i in range(RELAYED):
            hop_c(i).wait_send()


def run_stage(x_loc, params, n_stages):
    (ln1_gain, ln1_bias, w_q, b_q, w_kv, b_kv, w_o, b_o, ln2_gain, ln2_bias, w_up, b_up, w_down, b_down) = params
    n_micro, _, seq_loc, hidden = x_loc.shape
    ffn_loc = w_up.shape[2]
    rows = seq_loc // 2
    n_blocks = 4 * n_micro
    nq = hidden // CW
    nu = ffn_loc // CW
    heads_half = hidden // 2 // HEAD
    cfg = (n_stages, n_blocks, rows, hidden, ffn_loc)
    vmem = pl.BlockSpec(memory_space=pltpu.VMEM)
    anym = pl.BlockSpec(memory_space=pl.ANY)
    args = (
        x_loc, ln1_gain, ln1_bias, w_q, b_q.reshape(heads_half, 1, HEAD), w_kv, b_kv, w_o, b_o.reshape(nq, 1, CW),
        ln2_gain, ln2_bias, w_up, b_up.reshape(nu, 1, CW), w_down, b_down.reshape(nq, 1, CW),
    )
    in_specs = [anym, vmem, vmem, anym, vmem, anym, vmem, anym, vmem, vmem, vmem, anym, vmem, anym, vmem]
    half = hidden // 2
    out_shape = (
        jax.ShapeDtypeStruct(x_loc.shape, BF16),
        jax.ShapeDtypeStruct((hidden, half), BF16),
        jax.ShapeDtypeStruct((half, hidden), BF16),
        jax.ShapeDtypeStruct((hidden, half), BF16),
        jax.ShapeDtypeStruct((hidden, half), BF16),
        jax.ShapeDtypeStruct((half, hidden), BF16),
        jax.ShapeDtypeStruct((half, hidden), BF16),
    )
    dma = pltpu.SemaphoreType.DMA
    scratch = [
        pltpu.VMEM((SLOTS, hidden, CW), BF16),
        pltpu.VMEM((KEPT, hidden, CW), BF16),
        pltpu.VMEM((2, rows, hidden), BF16),
        pltpu.VMEM((rows, hidden), BF16),
        pltpu.VMEM((2 * heads_half, rows, HEAD), BF16),
        pltpu.VMEM((rows, hidden), BF16),
        pltpu.VMEM((rows, hidden), BF16),
        pltpu.VMEM((2, rows, hidden), BF16),
        pltpu.VMEM((rows, ffn_loc), BF16),
        pltpu.VMEM((rows, hidden), F32),
        pltpu.VMEM((rows, hidden), BF16),
        pltpu.VMEM((2, rows, hidden), BF16),
        pltpu.VMEM((rows, hidden), BF16),
        pltpu.VMEM((2, HEAD, 4 * rows), BF16),
        pltpu.VMEM((2, 4 * rows, 2 * HEAD), BF16),
        pltpu.VMEM((2 * heads_half, 1, HEAD), F32),
        dma((SLOTS,)),
        dma((KEPT,)),
        dma,
        dma((2,)),
        dma((2,)),
        dma((2 * PARTS,)),
        dma((2 * PARTS,)),
        dma((RELAYED,)),
        dma((RELAYED,)),
        dma((RELAYED,)),
        dma((RELAYED,)),
        dma((2,)),
        dma((4,)),
        dma((4,)),
        dma,
        dma((2,)),
        dma,
        dma((2,)),
        dma,
        pltpu.SemaphoreType.REGULAR,
        pltpu.SemaphoreType.REGULAR,
        pltpu.SemaphoreType.REGULAR,
    ]
    return pl.pallas_call(
        functools.partial(stage_kernel, cfg),
        out_shape=out_shape,
        in_specs=in_specs,
        out_specs=(anym,) * 7,
        scratch_shapes=scratch,
        compiler_params=pltpu.CompilerParams(collective_id=0, has_side_effects=True, vmem_limit_bytes=63 * 2 ** 20),
        name='stage_loop',
    )(*args)[0]


def solution(mesh):
    pp_size = mesh.shape['pp']

    def stage_program(x_loc, *params):
        result = run_stage(x_loc, params, pp_size)
        is_last = lax.axis_index('pp') == pp_size - 1
        return jnp.where(is_last, result, jnp.zeros_like(result))[None]

    return jax.shard_map(stage_program, mesh=mesh, in_specs=(P(None, 'dp', 'tp', None),) + PARAM_SPECS, out_specs=P('pp', None, 'dp', 'tp', None), check_vma=False)
```

```python
import functools

import jax
import jax.numpy as jnp
from jax import lax
from jax.experimental import pallas as pl
from jax.experimental.pallas import tpu as pltpu
from jax.sharding import PartitionSpec as P

F32 = jnp.float32
BF16 = jnp.bfloat16
MESH = pl.DeviceIdType.MESH

PARAM_SPECS = (P('pp', None), P('pp', None), P('pp', None, 'tp'), P('pp', 'tp'), P('pp', None, None), P('pp', None), P('pp', 'tp', None), P('pp', None), P('pp', None), P('pp', None), P('pp', None, 'tp'), P('pp', 'tp'), P('pp', 'tp', None), P('pp', None))

CW = 256
HEAD = 128
SLOTS = 16
AHEAD = 4
PARTS = 4
RELAYED = 5


def scoped(name, fn, *args):
    with jax.named_scope(name):
        return fn(*args)


def stage_kernel(cfg, x_in, g1, s1, wq, bq, wkv, bkv, wo, bo, g2, s2, wup, bup, wdn, bdn,
                 out, wq_peer, wo_peer, qa, qb, oa, ob,
                 ring, xbuf, hbuf, qbuf, cbuf, x1own, x1recv, ubuf, zbuf, psend, precv, ybuf, kt, vones, bq_all,
                 ring_sem, xload_sem, xslot_sem, bq_sem, w_send_sem, w_recv_sem, ra_recv_sem, rb_send_sem, rb_recv_sem, rc_send_sem,
                 kv_send_sem, k_recv_sem, v_recv_sem,
                 x1_send_sem, x1_recv_sem, p_send_sem, p_recv_sem, y_send_sem, go_sem, clear_sem, credit_sem):
    (n_stages, n_blocks, rows, hidden, ffn_loc) = cfg
    half = hidden // 2
    nq = hidden // CW
    nu = ffn_loc // CW
    heads_half = half // HEAD
    n_heads = 2 * heads_half
    stage = lax.axis_index('pp')
    rank = lax.axis_index('tp')
    peer = {'tp': 1 - rank}
    nxt = {'pp': jnp.minimum(stage + 1, n_stages - 1)}
    prv = {'pp': jnp.maximum(stage - 1, 0)}
    across = {'pp': 4 - stage}
    first = stage == 0
    second = stage == 1
    third = stage == 2
    last = stage == n_stages - 1
    even = lax.rem(stage, 2) == 0

    leads = lax.rem(rank + stage, 2) == 0
    lag = 1 - leads.astype(jnp.int32)
    n_steps = n_blocks + 1

    def own_block(k):
        return k - lag

    def peer_block(k):
        return k - 1 + lag

    def valid(b):
        return (b >= 0) & (b < n_blocks)

    KVQ, O, UP, DOWN, UP2, DOWN2 = 0, 1, 2, 3, 4, 5
    counts = (1 + nq, nq, nu, 2 * nq, nu, 2 * nq)
    own_count = sum(counts[:4])
    peer_count = sum(counts[4:])

    def base(k, phase):
        start = k * (own_count + peer_count) - jnp.where(k > 0, jnp.where(leads, peer_count, own_count), 0)
        if phase < UP2:
            return start + sum(counts[:phase])
        return start + jnp.where(valid(own_block(k)), own_count, 0) + sum(counts[UP2:phase])

    def slot_at(g):
        return lax.rem(g, SLOTS)

    def start_chunk(u, phase, idx):
        slot = slot_at(base(u, phase) + idx)
        dst = ring.at[slot]
        sem = ring_sem.at[slot]

        def cols(c, width):
            return pl.ds(pl.multiple_of(c * width, width), width)

        if phase == KVQ:
            @pl.when(idx == 0)
            def _():
                pltpu.make_async_copy(wkv.at[0], dst, sem).start()

            for b in range(2):
                block = (idx - 1) * 2 + b
                piece = dst.at[:, pl.ds(b * HEAD, HEAD)]

                @pl.when((idx > 0) & (block < heads_half))
                def _():
                    pltpu.make_async_copy(wq.at[0, :, cols(block, HEAD)], piece, sem).start()

                @pl.when((idx > 0) & (block >= heads_half))
                def _():
                    pltpu.make_async_copy(wq_peer.at[:, cols(block - heads_half, HEAD)], piece, sem).start()
        elif phase == O:
            pltpu.make_async_copy(wo.at[0, :, cols(idx, CW)], dst.at[pl.ds(0, half), :], sem).start()
            pltpu.make_async_copy(wo_peer.at[:, cols(idx, CW)], dst.at[pl.ds(half, half), :], sem).start()
        elif phase in (UP, UP2):
            pltpu.make_async_copy(wup.at[0, :, cols(idx, CW)], dst, sem).start()
        else:
            part = lax.rem(idx, 2)
            pltpu.make_async_copy(
                wdn.at[0, pl.ds(pl.multiple_of(part * hidden, hidden), hidden), cols(idx // 2, CW)], dst, sem).start()

    def start_at(u, part, pos, phases):
        firsts = KVQ if part == 0 else UP2
        for i, phase in enumerate(phases):
            low = sum(counts[firsts:phase])
            inside = (pos >= low) & (pos < low + counts[phase])

            @pl.when(inside)
            def _():
                start_chunk(u, phase, pos - low)

    def prefetch(u, phase, idx):
        part = 0 if phase < UP2 else 1
        length = (own_count, peer_count)[part]
        low = sum(counts[KVQ if part == 0 else UP2:phase])
        pos = idx + low + SLOTS
        last_phase = DOWN if part == 0 else DOWN2
        reach = [p for p in range(phase, last_phase + 1)]
        if phase == KVQ:
            @pl.when(own_block(u) != 0)
            def _():
                start_at(u, part, pos, reach[:3])
        else:
            start_at(u, part, pos, reach[:3])
        if phase == last_phase:
            past = pos >= length
            peer_next = valid(peer_block(u)) if part == 0 else (u + 1 < n_steps) & jnp.logical_not(valid(own_block(u + 1)))
            own_next = (jnp.logical_not(valid(peer_block(u))) if part == 0 else True) & (u + 1 < n_steps) & valid(own_block(u + 1))

            @pl.when(past & peer_next)
            def _():
                start_at(u if part == 0 else u + 1, 1, pos - length, (UP2, DOWN2))

            @pl.when(past & own_next)
            def _():
                start_at(u + 1, 0, pos - length, (KVQ,))

                @pl.when(own_block(u + 1) != 0)
                def _():
                    start_at(u + 1, 0, pos - length, (O, UP))

    def wait_chunk(g):
        slot = slot_at(g)
        pltpu.make_async_copy(wkv.at[0], ring.at[slot], ring_sem.at[slot]).wait()

    def layer_norm(src, dst, gain, shift):
        block = min(128, rows)
        pieces = [pl.ds(k * CW, CW) for k in range(hidden // CW)]

        def body(i, carry):
            at = pl.multiple_of(i * block, block)
            r = pl.ds(at, block)
            total = src[r, pieces[0]].astype(F32)
            for p in pieces[1:]:
                total = total + src[r, p].astype(F32)
            mean = jnp.sum(total, axis=-1, keepdims=True) * (1.0 / hidden)
            square = None
            for p in pieces:
                cen = src[r, p].astype(F32) - mean
                square = cen * cen if square is None else square + cen * cen
            inv = lax.rsqrt(jnp.sum(square, axis=-1, keepdims=True) * (1.0 / hidden) + 1e-5)
            for p in pieces:
                cen = src[r, p].astype(F32) - mean
                dst[r, p] = (cen * inv * gain[:, p] + shift[:, p]).astype(BF16)
            return carry

        lax.fori_loop(0, rows // block, body, 0)

    def place(b):
        return b // 4, lax.rem(b // 2, 2), pl.ds(pl.multiple_of(lax.rem(b, 2) * rows, rows), rows)

    def load_x(b):
        @pl.when(first & (b < n_blocks))
        def _():
            mb, seq, r = place(b)
            pltpu.make_async_copy(x_in.at[mb, seq, r, :], xbuf.at[lax.rem(b, 2)], xload_sem).start()

    def remote(src, dst, send_sem, recv_sem, to=peer):
        return pltpu.make_async_remote_copy(src, dst, send_sem, recv_sem, device_id=to, device_id_type=MESH)

    def signal(sem, to):
        pl.semaphore_signal(sem, inc=1, device_id=to, device_id_type=MESH)

    def bq_copy():
        return remote(bq, bq_all.at[pl.ds(heads_half, heads_half)], bq_sem.at[0], bq_sem.at[1])

    def piece(i, kind):
        ref = {'here': (wq.at[0], wo.at[0]), 'there': (wq_peer, wo_peer), 'a': (qa, oa), 'b': (qb, ob)}[kind][i // PARTS]
        n = (hidden, half)[i // PARTS] // PARTS
        return ref.at[pl.ds((i % PARTS) * n, n), :]

    def w_copy(i):
        return remote(piece(i, 'here'), piece(i, 'there'), w_send_sem.at[i], w_recv_sem.at[i])

    def hop_a(i):
        return remote(piece(i, 'here'), piece(i, 'a'), w_send_sem.at[i], ra_recv_sem.at[i], across)

    def hop_b(i):
        return remote(piece(i, 'a'), piece(i, 'b'), rb_send_sem.at[i], rb_recv_sem.at[i])

    def hop_c(i):
        return remote(piece(i, 'b'), piece(i, 'there'), rc_send_sem.at[i], w_recv_sem.at[i], across)

    barrier = pltpu.get_barrier_semaphore()
    signal(barrier, peer)

    @pl.when(stage > 0)
    def _():
        signal(barrier, prv)

    @pl.when(jnp.logical_not(last))
    def _():
        signal(barrier, nxt)

    @pl.when(jnp.logical_not(even))
    def _():
        signal(barrier, across)

    pl.semaphore_wait(barrier, 1 + (stage > 0).astype(jnp.int32) + (stage < n_stages - 1).astype(jnp.int32) + 1 - even.astype(jnp.int32))

    bq_copy().start()

    @pl.when(second)
    def _():
        for i in range(RELAYED):
            hop_a(i).start()
        scoped('go_wait', pl.semaphore_wait, go_sem, 1)
        for i in range(RELAYED, 2 * PARTS):
            w_copy(i).start()

    @pl.when(last)
    def _():
        for i in range(RELAYED + 1):
            if i < RELAYED:
                hop_a(i).wait_recv()
                hop_b(i).start()
            if i > 0:
                hop_b(i - 1).wait_recv()
                hop_c(i - 1).start()
        for i in range(RELAYED):
            hop_b(i).wait_send()
        signal(clear_sem, prv)
        scoped('go_wait', pl.semaphore_wait, go_sem, 1)

    @pl.when(third)
    def _():
        scoped('go_wait', pl.semaphore_wait, clear_sem, 1)

    @pl.when(jnp.logical_not(second))
    def _():
        for i in range(2 * PARTS):
            w_copy(i).start()

    bq_all[pl.ds(0, heads_half)] = bq[...]
    vones[:, :, HEAD:] = jnp.ones((2, 4 * rows, HEAD), BF16)

    zero = jnp.int32(0)
    own_chunks = 1 + heads_half // 2

    @pl.when(leads)
    def _():
        for i in range(min(SLOTS, own_chunks)):
            start_chunk(zero, KVQ, jnp.int32(i))

    @pl.when(jnp.logical_not(leads))
    def _():
        for i in range(SLOTS):
            start_chunk(zero, UP2, jnp.int32(i))

    load_x(zero)
    bq_copy().wait_recv()
    with jax.named_scope('wq_wait'):
        for i in range(PARTS):
            w_copy(i).wait_recv()

    @pl.when(leads)
    def _():
        for i in range(min(SLOTS, own_chunks), min(SLOTS, counts[KVQ])):
            start_chunk(zero, KVQ, jnp.int32(i))

    bq_copy().wait_send()

    @pl.when(even)
    def _():
        for i in range(PARTS):
            w_copy(i).wait_send()

        @pl.when(rank > 0)
        def _():
            for i in range(PARTS, 2 * PARTS):
                w_copy(i).wait_send()

        signal(go_sem, nxt)

    for i in range(AHEAD):
        wait_chunk(zero + i)

    def attention(j, seq):
        factor = HEAD ** -0.5 * 1.4426950408889634

        def two_heads(jj, i):
            kts, vs = kt.at[seq], vones.at[seq]
            q = qbuf[pl.ds(2 * i, 2)].reshape(2 * rows, HEAD)
            sd = jnp.dot(q, kts[:, jj * rows:(jj + 1) * rows], preferred_element_type=F32)
            row = jnp.bitwise_and(lax.broadcasted_iota(jnp.int32, (2 * rows, rows), 0), rows - 1)
            col = lax.broadcasted_iota(jnp.int32, (2 * rows, rows), 1)
            sd = jnp.where(col <= row, sd, -1e30)
            top = jnp.max(sd, axis=-1, keepdims=True)
            if jj:
                so = jnp.dot(q, kts[:, :jj * rows], preferred_element_type=F32)
                top = jnp.maximum(top, jnp.max(so, axis=-1, keepdims=True))
            pd = jnp.exp2((sd - top) * factor).astype(BF16)
            acc = jnp.dot(pd, vs[jj * rows:(jj + 1) * rows, :], preferred_element_type=F32)
            if jj:
                po = jnp.exp2((so - top) * factor).astype(BF16)
                acc = acc + jnp.dot(po, vs[:jj * rows, :], preferred_element_type=F32)
            c = (acc[:, :HEAD] / acc[:, HEAD:]).astype(BF16)
            at = pl.multiple_of(i * 2 * HEAD, 2 * HEAD)
            cbuf[:, pl.ds(at, HEAD)] = c[:rows]
            cbuf[:, pl.ds(at + HEAD, HEAD)] = c[rows:]

        for jj in range(4):
            @pl.when(j == jj)
            def _():
                def body(i, carry):
                    two_heads(jj, i)
                    return carry

                lax.fori_loop(0, n_heads // 2, body, 0)

    def x1_copy(slot, start, width):
        cols = pl.ds(start, width)
        return remote(x1own.at[:, cols], x1recv.at[slot, :, cols], x1_send_sem, x1_recv_sem.at[slot])

    def p_copy(slot, c, n):
        cols = pl.ds(pl.multiple_of(c * CW, CW), n * CW)
        return remote(psend.at[:, cols], precv.at[slot, :, cols], p_send_sem, p_recv_sem.at[slot])

    def kv_copies(seq, part):
        at = pl.ds(pl.multiple_of(part * rows, rows), rows)
        sem = 2 * seq + part
        return (remote(kt.at[seq, :, at], kt.at[seq, :, at], kv_send_sem.at[0], k_recv_sem.at[sem]),
                remote(vones.at[seq, at, pl.ds(0, HEAD)], vones.at[seq, at, pl.ds(0, HEAD)], kv_send_sem.at[1], v_recv_sem.at[sem]))

    def attend(u):
        b = own_block(u)
        seq = lax.rem(b // 2, 2)
        part = lax.rem(b, 2)
        j = part + 2 * lag
        slot2 = lax.rem(u, 2)
        xslot = lax.rem(b, 2)
        at_kvq = base(u, KVQ)
        at_o = base(u, O)

        @pl.when(first)
        def _():
            pltpu.make_async_copy(x_in.at[0, 0, pl.ds(0, rows), :], xbuf.at[xslot], xload_sem).wait()

        @pl.when(jnp.logical_not(first))
        def _():
            scoped('x_wait', remote(ybuf, xbuf.at[xslot], y_send_sem, xslot_sem.at[xslot], nxt).wait_recv)

        scoped('ln1', layer_norm, xbuf.at[xslot], hbuf, g1, s1)

        @pl.when(leads & (b > 0))
        def _():
            for copy in kv_copies(seq, part):
                copy.wait_send()

        def q_heads(c, slot):
            a = jnp.dot(hbuf[...], ring[slot], preferred_element_type=F32)
            qbuf[2 * c] = (a[:, :HEAD] + bq_all[2 * c]).astype(BF16)
            qbuf[2 * c + 1] = (a[:, HEAD:] + bq_all[2 * c + 1]).astype(BF16)

        wait_chunk(at_kvq + 4)
        wait_chunk(at_kvq + 5)
        kv = jnp.dot(hbuf[...], ring[slot_at(at_kvq)], preferred_element_type=F32) + bkv[...]
        at = pl.ds(pl.multiple_of(j * rows, rows), rows)
        kt[seq, :, at] = kv[:, :HEAD].astype(BF16).astype(F32).T.astype(BF16)
        vones[seq, at, :HEAD] = kv[:, HEAD:].astype(BF16)
        q_heads(0, slot_at(at_kvq + 1))

        @pl.when(leads)
        def _():
            for copy in kv_copies(seq, part):
                copy.start()

        prefetch(u, KVQ, zero)
        prefetch(u, KVQ, zero + 1)

        def q_body(i, carry):
            g = at_kvq + 2 * i

            @pl.when((b > 0) | (2 * i + 5 < counts[KVQ]))
            def _():
                wait_chunk(g + 4)
                wait_chunk(g + 5)

            q_heads(2 * i - 1, slot_at(g))
            q_heads(2 * i, slot_at(g + 1))
            prefetch(u, KVQ, 2 * i)
            prefetch(u, KVQ, 2 * i + 1)
            return carry

        scoped('q', lax.fori_loop, 1, (nq + 1) // 2, q_body, 0)

        @pl.when(jnp.logical_not(leads) & (part == 0))
        def _():
            with jax.named_scope('kv_wait'):
                for p in range(2):
                    for copy in kv_copies(seq, jnp.int32(p)):
                        copy.wait_recv()

        scoped('attn', attention, j, seq)


        @pl.when((u > 0) & valid(peer_block(u - 1)))
        def _():
            finish(u - 1)

        @pl.when(b == 0)
        def _():
            with jax.named_scope('wo_wait'):
                for i in range(PARTS, 2 * PARTS):
                    w_copy(i).wait_recv()
            for i in range(SLOTS):
                start_at(u, 0, zero + counts[KVQ] + i, (O, UP))
            for i in range(AHEAD):
                wait_chunk(at_o + i)

        @pl.when(b > 0)
        def _():
            remote(x1own, x1recv.at[slot2], x1_send_sem, x1_recv_sem.at[slot2]).wait_send()

        def o_cols(c, slot):
            cols = pl.ds(pl.multiple_of(c * CW, CW), CW)
            a = jnp.dot(cbuf[...], ring[slot], preferred_element_type=F32)
            x1own[:, cols] = (xbuf[xslot, :, cols].astype(F32) + a + bo[c]).astype(BF16)

        def o_body(i, carry):
            g = at_o + 2 * i
            wait_chunk(g + 4)
            wait_chunk(g + 5)
            o_cols(2 * i, slot_at(g))
            o_cols(2 * i + 1, slot_at(g + 1))

            @pl.when(i > 0)
            def _():
                x1_copy(slot2, pl.multiple_of((i - 1) * 2 * CW, CW), 2 * CW).start()

            prefetch(u, O, 2 * i)
            prefetch(u, O, 2 * i + 1)
            return carry

        scoped('o', lax.fori_loop, 0, nq // 2, o_body, 0)
        wait_chunk(at_o + nq + 3)
        o_cols(nq - 1, slot_at(at_o + nq - 1))
        prefetch(u, O, jnp.int32(nq - 1))
        tail = (nq // 2 - 1) * 2 * CW
        x1_copy(slot2, tail, hidden - tail).start()

        @pl.when((stage > 0) & (b + 2 < n_blocks))
        def _():
            signal(credit_sem, prv)


    def down(u, phase):
        slot2 = lax.rem(u, 2)
        at_d = base(u, phase)
        own = phase == DOWN

        if own:
            @pl.when(own_block(u) > 0)
            def _():
                remote(psend, precv.at[slot2], p_send_sem, p_recv_sem.at[slot2]).wait_send()

        def column(c, g):
            cols = pl.ds(pl.multiple_of(c * CW, CW), CW)
            a = (jnp.dot(ubuf[:, :hidden], ring[slot_at(g)], preferred_element_type=F32)
                 + jnp.dot(ubuf[:, hidden:], ring[slot_at(g + 1)], preferred_element_type=F32))
            if own:
                psend[:, cols] = a.astype(BF16)
            else:
                zbuf[:, cols] = x1recv[slot2, :, cols].astype(F32) + a + bdn[c]

        more = u + 1 < n_steps
        full = nq // 2

        def body(i, carry):
            g = at_d + 4 * i
            wait_chunk(g + 4)
            wait_chunk(g + 5)

            @pl.when(more | (i < full - 1))
            def _():
                wait_chunk(g + 6)
                wait_chunk(g + 7)

            column(2 * i, g)
            column(2 * i + 1, g + 2)
            if own:
                @pl.when(i > 0)
                def _():
                    p_copy(slot2, 2 * i - 2, 2).start()

            for k in range(4):
                prefetch(u, phase, 4 * i + k)
            return carry

        def rest():
            g = at_d + 4 * full

            @pl.when(more)
            def _():
                wait_chunk(g + 4)
                wait_chunk(g + 5)

            column(zero + 2 * full, g)
            for k in range(2):
                prefetch(u, phase, zero + 4 * full + k)

        assert nq % 2 == 1 and nu % 4 == 2
        with jax.named_scope('down' if own else 'down_peer'):
            lax.fori_loop(0, full, body, 0)
            rest()
        if own:
            p_copy(slot2, zero + 2 * full - 2, 3).start()

    def up(u, phase):
        at_u = base(u, phase)

        def cols_of(c, slot):
            a = jnp.dot(hbuf[...], ring[slot], preferred_element_type=F32) + bup[c]
            t = jnp.tanh(0.7978845608028654 * (a + 0.044715 * (a * a * a)))
            ubuf[:, pl.ds(pl.multiple_of(c * CW, CW), CW)] = (0.5 * a * (1.0 + t)).astype(BF16)

        def body(i, carry):
            g = at_u + 4 * i
            for k in range(4, 8):
                wait_chunk(g + k)
            for k in range(4):
                cols_of(4 * i + k, slot_at(g + k))
            for k in range(4):
                prefetch(u, phase, 4 * i + k)
            return carry

        def rest():
            for k in range(4, 4 + nu % 4):
                wait_chunk(at_u + full * 4 + k)
            for k in range(nu % 4):
                cols_of(zero + full * 4 + k, slot_at(at_u + full * 4 + k))
            for k in range(nu % 4):
                prefetch(u, phase, zero + full * 4 + k)

        full = nu // 4
        with jax.named_scope('up' if phase == UP else 'up_peer'):
            lax.fori_loop(0, full, body, 0)
            rest()

    def finish(u):
        v = peer_block(u)
        slot = lax.rem(u, 2)
        scoped('p_wait', remote(psend, precv.at[slot], p_send_sem, p_recv_sem.at[slot]).wait_recv)

        @pl.when(v > 0)
        def _():
            scoped('y_wait', pltpu.make_async_copy(ybuf, out.at[0, 0, pl.ds(0, rows), :], y_send_sem).wait)

        block = 32

        def body(i, carry):
            r = pl.ds(pl.multiple_of(i * block, block), block)
            ybuf[r, :] = (zbuf[r, :] + precv[slot, r, :].astype(F32)).astype(BF16)
            return carry

        lax.fori_loop(0, rows // block, body, 0)

        @pl.when(jnp.logical_not(last))
        def _():
            @pl.when(v >= 2)
            def _():
                pl.semaphore_wait(credit_sem, 1)

            to = lax.rem(v, 2)
            remote(ybuf, xbuf.at[to], y_send_sem, xslot_sem.at[to], nxt).start()

        @pl.when(last)
        def _():
            mb, seq, r = place(v)
            pltpu.make_async_copy(ybuf, out.at[mb, seq, r, :], y_send_sem).start()

    def step(u, carry):
        slot2 = lax.rem(u, 2)

        @pl.when(valid(own_block(u)))
        def _():
            attend(u)
            scoped('ln2', layer_norm, x1own, hbuf, g2, s2)
            up(u, UP)
            load_x(own_block(u) + 1)
            down(u, DOWN)

        @pl.when(leads & (u == n_steps - 1))
        def _():
            finish(u - 1)

        @pl.when(valid(peer_block(u)))
        def _():
            scoped('x1_wait', remote(x1own, x1recv.at[slot2], x1_send_sem, x1_recv_sem.at[slot2]).wait_recv)
            scoped('ln_peer', layer_norm, x1recv.at[slot2], hbuf, g2, s2)
            up(u, UP2)
            down(u, DOWN2)

        return carry

    lax.fori_loop(0, n_steps, step, 0)

    @pl.when(leads)
    def _():
        finish(zero + n_steps - 1)


    remote(x1own, x1recv.at[0], x1_send_sem, x1_recv_sem.at[0]).wait_send()
    remote(psend, precv.at[0], p_send_sem, p_recv_sem.at[0]).wait_send()
    pltpu.make_async_copy(ybuf, out.at[0, 0, pl.ds(0, rows), :], y_send_sem).wait()

    @pl.when(leads)
    def _():
        for copy in kv_copies(zero, zero):
            copy.wait_send()

    @pl.when(jnp.logical_not(even))
    def _():
        for i in range(2 * PARTS):
            w_copy(i).wait_send()

    @pl.when(even & (rank == 0))
    def _():
        for i in range(PARTS, 2 * PARTS):
            w_copy(i).wait_send()

    @pl.when(last)
    def _():
        for i in range(RELAYED):
            hop_c(i).wait_send()


def run_stage(x_loc, params, n_stages):
    (ln1_gain, ln1_bias, w_q, b_q, w_kv, b_kv, w_o, b_o, ln2_gain, ln2_bias, w_up, b_up, w_down, b_down) = params
    n_micro, _, seq_loc, hidden = x_loc.shape
    ffn_loc = w_up.shape[2]
    rows = seq_loc // 2
    n_blocks = 4 * n_micro
    nq = hidden // CW
    nu = ffn_loc // CW
    heads_half = hidden // 2 // HEAD
    cfg = (n_stages, n_blocks, rows, hidden, ffn_loc)
    vmem = pl.BlockSpec(memory_space=pltpu.VMEM)
    anym = pl.BlockSpec(memory_space=pl.ANY)
    args = (
        x_loc, ln1_gain, ln1_bias, w_q, b_q.reshape(heads_half, 1, HEAD), w_kv, b_kv, w_o, b_o.reshape(nq, 1, CW),
        ln2_gain, ln2_bias, w_up, b_up.reshape(nu, 1, CW), w_down, b_down.reshape(nq, 1, CW),
    )
    in_specs = [anym, vmem, vmem, anym, vmem, anym, vmem, anym, vmem, vmem, vmem, anym, vmem, anym, vmem]
    half = hidden // 2
    out_shape = (
        jax.ShapeDtypeStruct(x_loc.shape, BF16),
        jax.ShapeDtypeStruct((hidden, half), BF16),
        jax.ShapeDtypeStruct((half, hidden), BF16),
        jax.ShapeDtypeStruct((hidden, half), BF16),
        jax.ShapeDtypeStruct((hidden, half), BF16),
        jax.ShapeDtypeStruct((half, hidden), BF16),
        jax.ShapeDtypeStruct((half, hidden), BF16),
    )
    dma = pltpu.SemaphoreType.DMA
    scratch = [
        pltpu.VMEM((SLOTS, hidden, CW), BF16),
        pltpu.VMEM((2, rows, hidden), BF16),
        pltpu.VMEM((rows, hidden), BF16),
        pltpu.VMEM((2 * heads_half, rows, HEAD), BF16),
        pltpu.VMEM((rows, hidden), BF16),
        pltpu.VMEM((rows, hidden), BF16),
        pltpu.VMEM((2, rows, hidden), BF16),
        pltpu.VMEM((rows, ffn_loc), BF16),
        pltpu.VMEM((rows, hidden), F32),
        pltpu.VMEM((rows, hidden), BF16),
        pltpu.VMEM((2, rows, hidden), BF16),
        pltpu.VMEM((rows, hidden), BF16),
        pltpu.VMEM((2, HEAD, 4 * rows), BF16),
        pltpu.VMEM((2, 4 * rows, 2 * HEAD), BF16),
        pltpu.VMEM((2 * heads_half, 1, HEAD), F32),
        dma((SLOTS,)),
        dma,
        dma((2,)),
        dma((2,)),
        dma((2 * PARTS,)),
        dma((2 * PARTS,)),
        dma((RELAYED,)),
        dma((RELAYED,)),
        dma((RELAYED,)),
        dma((RELAYED,)),
        dma((2,)),
        dma((4,)),
        dma((4,)),
        dma,
        dma((2,)),
        dma,
        dma((2,)),
        dma,
        pltpu.SemaphoreType.REGULAR,
        pltpu.SemaphoreType.REGULAR,
        pltpu.SemaphoreType.REGULAR,
    ]
    return pl.pallas_call(
        functools.partial(stage_kernel, cfg),
        out_shape=out_shape,
        in_specs=in_specs,
        out_specs=(anym,) * 7,
        scratch_shapes=scratch,
        compiler_params=pltpu.CompilerParams(collective_id=0, has_side_effects=True, vmem_limit_bytes=60 * 2 ** 20),
        name='stage_loop',
    )(*args)[0]


def solution(mesh):
    pp_size = mesh.shape['pp']

    def stage_program(x_loc, *params):
        result = run_stage(x_loc, params, pp_size)
        is_last = lax.axis_index('pp') == pp_size - 1
        return jnp.where(is_last, result, jnp.zeros_like(result))[None]

    return jax.shard_map(stage_program, mesh=mesh, in_specs=(P(None, 'dp', 'tp', None),) + PARAM_SPECS, out_specs=P('pp', None, 'dp', 'tp', None), check_vma=False)
```

```python
import functools

import jax
import jax.numpy as jnp
from jax import lax
from jax.experimental import pallas as pl
from jax.experimental.pallas import tpu as pltpu
from jax.sharding import PartitionSpec as P

F32 = jnp.float32
BF16 = jnp.bfloat16
MESH = pl.DeviceIdType.MESH

PARAM_SPECS = (P('pp', None), P('pp', None), P('pp', None, 'tp'), P('pp', 'tp'), P('pp', None, None), P('pp', None), P('pp', 'tp', None), P('pp', None), P('pp', None), P('pp', None), P('pp', None, 'tp'), P('pp', 'tp'), P('pp', 'tp', None), P('pp', None))

CW = 256
HEAD = 128
SLOTS = 16
AHEAD = 4
PARTS = 4
RELAYED = 5


def scoped(name, fn, *args):
    with jax.named_scope(name):
        return fn(*args)


def stage_kernel(cfg, x_in, g1, s1, wq, bq, wkv, bkv, wo, bo, g2, s2, wup, bup, wdn, bdn,
                 out, wq_peer, wo_peer, qa, qb, oa, ob,
                 ring, xbuf, hbuf, qbuf, cbuf, x1own, x1recv, ubuf, zbuf, psend, precv, ybuf, kt, vones, bq_all,
                 ring_sem, xload_sem, xslot_sem, bq_sem, w_send_sem, w_recv_sem, ra_recv_sem, rb_send_sem, rb_recv_sem, rc_send_sem,
                 kv_send_sem, k_recv_sem, v_recv_sem,
                 x1_send_sem, x1_recv_sem, p_send_sem, p_recv_sem, y_send_sem, go_sem, clear_sem, credit_sem):
    (n_stages, n_blocks, rows, hidden, ffn_loc) = cfg
    half = hidden // 2
    nq = hidden // CW
    nu = ffn_loc // CW
    heads_half = half // HEAD
    n_heads = 2 * heads_half
    stage = lax.axis_index('pp')
    rank = lax.axis_index('tp')
    peer = {'tp': 1 - rank}
    nxt = {'pp': jnp.minimum(stage + 1, n_stages - 1)}
    prv = {'pp': jnp.maximum(stage - 1, 0)}
    across = {'pp': 4 - stage}
    first = stage == 0
    second = stage == 1
    third = stage == 2
    last = stage == n_stages - 1
    even = lax.rem(stage, 2) == 0

    leads = lax.rem(rank + stage, 2) == 0
    lag = 1 - leads.astype(jnp.int32)
    n_steps = n_blocks + 1

    def own_block(k):
        return k - lag

    def peer_block(k):
        return k - 1 + lag

    def valid(b):
        return (b >= 0) & (b < n_blocks)

    KVQ, O, UP, DOWN, UP2, DOWN2 = 0, 1, 2, 3, 4, 5
    counts = (1 + nq, nq, nu, 2 * nq, nu, 2 * nq)
    own_count = sum(counts[:4])
    peer_count = sum(counts[4:])

    def base(k, phase):
        start = k * (own_count + peer_count) - jnp.where(k > 0, jnp.where(leads, peer_count, own_count), 0)
        if phase < UP2:
            return start + sum(counts[:phase])
        return start + jnp.where(valid(own_block(k)), own_count, 0) + sum(counts[UP2:phase])

    def slot_at(g):
        return lax.rem(g, SLOTS)

    def start_chunk(u, phase, idx):
        slot = slot_at(base(u, phase) + idx)
        dst = ring.at[slot]
        sem = ring_sem.at[slot]

        def cols(c, width):
            return pl.ds(pl.multiple_of(c * width, width), width)

        if phase == KVQ:
            @pl.when(idx == 0)
            def _():
                pltpu.make_async_copy(wkv.at[0], dst, sem).start()

            for b in range(2):
                block = (idx - 1) * 2 + b
                piece = dst.at[:, pl.ds(b * HEAD, HEAD)]

                @pl.when((idx > 0) & (block < heads_half))
                def _():
                    pltpu.make_async_copy(wq.at[0, :, cols(block, HEAD)], piece, sem).start()

                @pl.when((idx > 0) & (block >= heads_half))
                def _():
                    pltpu.make_async_copy(wq_peer.at[:, cols(block - heads_half, HEAD)], piece, sem).start()
        elif phase == O:
            pltpu.make_async_copy(wo.at[0, :, cols(idx, CW)], dst.at[pl.ds(0, half), :], sem).start()
            pltpu.make_async_copy(wo_peer.at[:, cols(idx, CW)], dst.at[pl.ds(half, half), :], sem).start()
        elif phase in (UP, UP2):
            pltpu.make_async_copy(wup.at[0, :, cols(idx, CW)], dst, sem).start()
        else:
            part = lax.rem(idx, 2)
            pltpu.make_async_copy(
                wdn.at[0, pl.ds(pl.multiple_of(part * hidden, hidden), hidden), cols(idx // 2, CW)], dst, sem).start()

    def start_at(u, part, pos, phases):
        firsts = KVQ if part == 0 else UP2
        for i, phase in enumerate(phases):
            low = sum(counts[firsts:phase])
            inside = (pos >= low) & (pos < low + counts[phase])

            @pl.when(inside)
            def _():
                start_chunk(u, phase, pos - low)

    def prefetch(u, phase, idx):
        part = 0 if phase < UP2 else 1
        length = (own_count, peer_count)[part]
        low = sum(counts[KVQ if part == 0 else UP2:phase])
        pos = idx + low + SLOTS
        last_phase = DOWN if part == 0 else DOWN2
        reach = [p for p in range(phase, last_phase + 1)]
        if phase == KVQ:
            @pl.when(own_block(u) != 0)
            def _():
                start_at(u, part, pos, reach[:3])
        else:
            start_at(u, part, pos, reach[:3])
        if phase == last_phase:
            past = pos >= length
            peer_next = valid(peer_block(u)) if part == 0 else (u + 1 < n_steps) & jnp.logical_not(valid(own_block(u + 1)))
            own_next = (jnp.logical_not(valid(peer_block(u))) if part == 0 else True) & (u + 1 < n_steps) & valid(own_block(u + 1))

            @pl.when(past & peer_next)
            def _():
                start_at(u if part == 0 else u + 1, 1, pos - length, (UP2, DOWN2))

            @pl.when(past & own_next)
            def _():
                start_at(u + 1, 0, pos - length, (KVQ,))

                @pl.when(own_block(u + 1) != 0)
                def _():
                    start_at(u + 1, 0, pos - length, (O, UP))

    def wait_chunk(g):
        slot = slot_at(g)
        pltpu.make_async_copy(wkv.at[0], ring.at[slot], ring_sem.at[slot]).wait()

    def layer_norm(src, dst, gain, shift):
        block = min(128, rows)
        pieces = [pl.ds(k * CW, CW) for k in range(hidden // CW)]

        def body(i, carry):
            at = pl.multiple_of(i * block, block)
            r = pl.ds(at, block)
            total = src[r, pieces[0]].astype(F32)
            for p in pieces[1:]:
                total = total + src[r, p].astype(F32)
            mean = jnp.sum(total, axis=-1, keepdims=True) * (1.0 / hidden)
            square = None
            for p in pieces:
                cen = src[r, p].astype(F32) - mean
                square = cen * cen if square is None else square + cen * cen
            inv = lax.rsqrt(jnp.sum(square, axis=-1, keepdims=True) * (1.0 / hidden) + 1e-5)
            for p in pieces:
                cen = src[r, p].astype(F32) - mean
                dst[r, p] = (cen * inv * gain[:, p] + shift[:, p]).astype(BF16)
            return carry

        lax.fori_loop(0, rows // block, body, 0)

    def place(b):
        return b // 4, lax.rem(b // 2, 2), pl.ds(pl.multiple_of(lax.rem(b, 2) * rows, rows), rows)

    def load_x(b):
        @pl.when(first & (b < n_blocks))
        def _():
            mb, seq, r = place(b)
            pltpu.make_async_copy(x_in.at[mb, seq, r, :], xbuf.at[lax.rem(b, 2)], xload_sem).start()

    def remote(src, dst, send_sem, recv_sem, to=peer):
        return pltpu.make_async_remote_copy(src, dst, send_sem, recv_sem, device_id=to, device_id_type=MESH)

    def signal(sem, to):
        pl.semaphore_signal(sem, inc=1, device_id=to, device_id_type=MESH)

    def bq_copy():
        return remote(bq, bq_all.at[pl.ds(heads_half, heads_half)], bq_sem.at[0], bq_sem.at[1])

    def piece(i, kind):
        ref = {'here': (wq.at[0], wo.at[0]), 'there': (wq_peer, wo_peer), 'a': (qa, oa), 'b': (qb, ob)}[kind][i // PARTS]
        n = (hidden, half)[i // PARTS] // PARTS
        return ref.at[pl.ds((i % PARTS) * n, n), :]

    def w_copy(i):
        return remote(piece(i, 'here'), piece(i, 'there'), w_send_sem.at[i], w_recv_sem.at[i])

    def hop_a(i):
        return remote(piece(i, 'here'), piece(i, 'a'), w_send_sem.at[i], ra_recv_sem.at[i], across)

    def hop_b(i):
        return remote(piece(i, 'a'), piece(i, 'b'), rb_send_sem.at[i], rb_recv_sem.at[i])

    def hop_c(i):
        return remote(piece(i, 'b'), piece(i, 'there'), rc_send_sem.at[i], w_recv_sem.at[i], across)

    barrier = pltpu.get_barrier_semaphore()
    signal(barrier, peer)

    @pl.when(stage > 0)
    def _():
        signal(barrier, prv)

    @pl.when(jnp.logical_not(last))
    def _():
        signal(barrier, nxt)

    @pl.when(jnp.logical_not(even))
    def _():
        signal(barrier, across)

    pl.semaphore_wait(barrier, 1 + (stage > 0).astype(jnp.int32) + (stage < n_stages - 1).astype(jnp.int32) + 1 - even.astype(jnp.int32))

    bq_copy().start()

    @pl.when(second)
    def _():
        for i in range(RELAYED):
            hop_a(i).start()
        scoped('go_wait', pl.semaphore_wait, go_sem, 1)
        for i in range(RELAYED, 2 * PARTS):
            w_copy(i).start()

    @pl.when(last)
    def _():
        for i in range(RELAYED + 1):
            if i < RELAYED:
                hop_a(i).wait_recv()
                hop_b(i).start()
            if i > 0:
                hop_b(i - 1).wait_recv()
                hop_c(i - 1).start()
        for i in range(RELAYED):
            hop_b(i).wait_send()
        signal(clear_sem, prv)
        scoped('go_wait', pl.semaphore_wait, go_sem, 1)

    @pl.when(third)
    def _():
        scoped('go_wait', pl.semaphore_wait, clear_sem, 1)

    @pl.when(jnp.logical_not(second))
    def _():
        for i in range(2 * PARTS):
            w_copy(i).start()

    bq_all[pl.ds(0, heads_half)] = bq[...]
    vones[:, :, HEAD:] = jnp.ones((2, 4 * rows, HEAD), BF16)

    zero = jnp.int32(0)
    own_chunks = 1 + heads_half // 2

    @pl.when(leads)
    def _():
        for i in range(min(SLOTS, own_chunks)):
            start_chunk(zero, KVQ, jnp.int32(i))

    @pl.when(jnp.logical_not(leads))
    def _():
        for i in range(SLOTS):
            start_chunk(zero, UP2, jnp.int32(i))

    load_x(zero)
    bq_copy().wait_recv()
    with jax.named_scope('wq_wait'):
        for i in range(PARTS):
            w_copy(i).wait_recv()

    @pl.when(leads)
    def _():
        for i in range(min(SLOTS, own_chunks), min(SLOTS, counts[KVQ])):
            start_chunk(zero, KVQ, jnp.int32(i))

    bq_copy().wait_send()

    @pl.when(even)
    def _():
        for i in range(PARTS):
            w_copy(i).wait_send()

        @pl.when(rank > 0)
        def _():
            for i in range(PARTS, 2 * PARTS):
                w_copy(i).wait_send()

        signal(go_sem, nxt)

    for i in range(AHEAD):
        wait_chunk(zero + i)

    def attention(j, seq):
        factor = HEAD ** -0.5 * 1.4426950408889634

        def two_heads(jj, i):
            kts, vs = kt.at[seq], vones.at[seq]
            q = qbuf[pl.ds(2 * i, 2)].reshape(2 * rows, HEAD)
            sd = jnp.dot(q, kts[:, jj * rows:(jj + 1) * rows], preferred_element_type=F32)
            row = jnp.bitwise_and(lax.broadcasted_iota(jnp.int32, (2 * rows, rows), 0), rows - 1)
            col = lax.broadcasted_iota(jnp.int32, (2 * rows, rows), 1)
            sd = jnp.where(col <= row, sd, -1e30)
            top = jnp.max(sd, axis=-1, keepdims=True)
            if jj:
                so = jnp.dot(q, kts[:, :jj * rows], preferred_element_type=F32)
                top = jnp.maximum(top, jnp.max(so, axis=-1, keepdims=True))
            pd = jnp.exp2((sd - top) * factor).astype(BF16)
            acc = jnp.dot(pd, vs[jj * rows:(jj + 1) * rows, :], preferred_element_type=F32)
            if jj:
                po = jnp.exp2((so - top) * factor).astype(BF16)
                acc = acc + jnp.dot(po, vs[:jj * rows, :], preferred_element_type=F32)
            c = (acc[:, :HEAD] / acc[:, HEAD:]).astype(BF16)
            at = pl.multiple_of(i * 2 * HEAD, 2 * HEAD)
            cbuf[:, pl.ds(at, HEAD)] = c[:rows]
            cbuf[:, pl.ds(at + HEAD, HEAD)] = c[rows:]

        for jj in range(4):
            @pl.when(j == jj)
            def _():
                pairs = n_heads // 2
                n = 2 if jj >= 2 else 1

                def body(i, carry):
                    for k in range(n):
                        two_heads(jj, n * i + k)
                    return carry

                lax.fori_loop(0, pairs // n, body, 0)
                for i in range(pairs - pairs % n, pairs):
                    two_heads(jj, zero + i)

    def x1_copy(slot, start, width):
        cols = pl.ds(start, width)
        return remote(x1own.at[:, cols], x1recv.at[slot, :, cols], x1_send_sem, x1_recv_sem.at[slot])

    def p_copy(slot, c, n):
        cols = pl.ds(pl.multiple_of(c * CW, CW), n * CW)
        return remote(psend.at[:, cols], precv.at[slot, :, cols], p_send_sem, p_recv_sem.at[slot])

    def kv_copies(seq, part):
        at = pl.ds(pl.multiple_of(part * rows, rows), rows)
        sem = 2 * seq + part
        return (remote(kt.at[seq, :, at], kt.at[seq, :, at], kv_send_sem.at[0], k_recv_sem.at[sem]),
                remote(vones.at[seq, at, pl.ds(0, HEAD)], vones.at[seq, at, pl.ds(0, HEAD)], kv_send_sem.at[1], v_recv_sem.at[sem]))

    def attend(u):
        b = own_block(u)
        seq = lax.rem(b // 2, 2)
        part = lax.rem(b, 2)
        j = part + 2 * lag
        slot2 = lax.rem(u, 2)
        xslot = lax.rem(b, 2)
        at_kvq = base(u, KVQ)
        at_o = base(u, O)

        @pl.when(first)
        def _():
            pltpu.make_async_copy(x_in.at[0, 0, pl.ds(0, rows), :], xbuf.at[xslot], xload_sem).wait()

        @pl.when(jnp.logical_not(first))
        def _():
            scoped('x_wait', remote(ybuf, xbuf.at[xslot], y_send_sem, xslot_sem.at[xslot], nxt).wait_recv)

        scoped('ln1', layer_norm, xbuf.at[xslot], hbuf, g1, s1)

        @pl.when(leads & (b > 0))
        def _():
            for copy in kv_copies(seq, part):
                copy.wait_send()

        def q_heads(c, slot):
            a = jnp.dot(hbuf[...], ring[slot], preferred_element_type=F32)
            qbuf[2 * c] = (a[:, :HEAD] + bq_all[2 * c]).astype(BF16)
            qbuf[2 * c + 1] = (a[:, HEAD:] + bq_all[2 * c + 1]).astype(BF16)

        wait_chunk(at_kvq + 4)
        wait_chunk(at_kvq + 5)
        kv = jnp.dot(hbuf[...], ring[slot_at(at_kvq)], preferred_element_type=F32) + bkv[...]
        at = pl.ds(pl.multiple_of(j * rows, rows), rows)
        kt[seq, :, at] = kv[:, :HEAD].astype(BF16).astype(F32).T.astype(BF16)
        vones[seq, at, :HEAD] = kv[:, HEAD:].astype(BF16)
        q_heads(0, slot_at(at_kvq + 1))

        @pl.when(leads)
        def _():
            for copy in kv_copies(seq, part):
                copy.start()

        prefetch(u, KVQ, zero)
        prefetch(u, KVQ, zero + 1)

        quads = (nq - 1) // 4
        rest_q = (nq - 1) % 4
        inside = 4 * (quads - 1) + 7 < counts[KVQ]

        def q_body(i, carry):
            g = at_kvq + 4 * i + 2

            def waits():
                wait_chunk(g + 4)
                wait_chunk(g + 5)

            if inside:
                waits()
            else:
                pl.when((b > 0) | (4 * i + 7 < counts[KVQ]))(waits)
            for k in range(4):
                q_heads(4 * i + 1 + k, slot_at(g + k))
            for k in range(4):
                prefetch(u, KVQ, 4 * i + 2 + k)

            @pl.when((b > 0) | (4 * i + 9 < counts[KVQ]))
            def _():
                wait_chunk(g + 6)
                wait_chunk(g + 7)

            return carry

        with jax.named_scope('q'):
            lax.fori_loop(0, quads, q_body, 0)
            assert rest_q in (0, 2)
            g = at_kvq + 4 * quads + 2
            for k in range(rest_q):
                q_heads(zero + 4 * quads + 1 + k, slot_at(g + k))
            for k in range(rest_q):
                prefetch(u, KVQ, zero + 4 * quads + 2 + k)

            @pl.when(b > 0)
            def _():
                for k in range(rest_q):
                    wait_chunk(g + 4 + k)

        @pl.when(jnp.logical_not(leads) & (part == 0))
        def _():
            with jax.named_scope('kv_wait'):
                for p in range(2):
                    for copy in kv_copies(seq, jnp.int32(p)):
                        copy.wait_recv()

        scoped('attn', attention, j, seq)


        @pl.when((u > 0) & valid(peer_block(u - 1)))
        def _():
            finish(u - 1)

        @pl.when(b == 0)
        def _():
            with jax.named_scope('wo_wait'):
                for i in range(PARTS, 2 * PARTS):
                    w_copy(i).wait_recv()
            for i in range(SLOTS):
                start_at(u, 0, zero + counts[KVQ] + i, (O, UP))
            for i in range(AHEAD):
                wait_chunk(at_o + i)

        @pl.when(b > 0)
        def _():
            remote(x1own, x1recv.at[slot2], x1_send_sem, x1_recv_sem.at[slot2]).wait_send()

        def o_cols(c, slot):
            cols = pl.ds(pl.multiple_of(c * CW, CW), CW)
            a = jnp.dot(cbuf[...], ring[slot], preferred_element_type=F32)
            x1own[:, cols] = (xbuf[xslot, :, cols].astype(F32) + a + bo[c]).astype(BF16)

        def o_body(i, carry):
            g = at_o + 2 * i
            wait_chunk(g + 4)
            wait_chunk(g + 5)
            o_cols(2 * i, slot_at(g))
            o_cols(2 * i + 1, slot_at(g + 1))

            @pl.when(i > 0)
            def _():
                x1_copy(slot2, pl.multiple_of((i - 1) * 2 * CW, CW), 2 * CW).start()

            prefetch(u, O, 2 * i)
            prefetch(u, O, 2 * i + 1)
            return carry

        scoped('o', lax.fori_loop, 0, nq // 2, o_body, 0)
        wait_chunk(at_o + nq + 3)
        o_cols(nq - 1, slot_at(at_o + nq - 1))
        prefetch(u, O, jnp.int32(nq - 1))
        tail = (nq // 2 - 1) * 2 * CW
        x1_copy(slot2, tail, hidden - tail).start()

        @pl.when((stage > 0) & (b + 2 < n_blocks))
        def _():
            signal(credit_sem, prv)


    def down(u, phase):
        slot2 = lax.rem(u, 2)
        at_d = base(u, phase)
        own = phase == DOWN

        if own:
            @pl.when(own_block(u) > 0)
            def _():
                remote(psend, precv.at[slot2], p_send_sem, p_recv_sem.at[slot2]).wait_send()

        def column(c, g):
            cols = pl.ds(pl.multiple_of(c * CW, CW), CW)
            a = (jnp.dot(ubuf[:, :hidden], ring[slot_at(g)], preferred_element_type=F32)
                 + jnp.dot(ubuf[:, hidden:], ring[slot_at(g + 1)], preferred_element_type=F32))
            if own:
                psend[:, cols] = a.astype(BF16)
            else:
                zbuf[:, cols] = x1recv[slot2, :, cols].astype(F32) + a + bdn[c]

        more = u + 1 < n_steps
        full = nq // 2

        def body(i, carry):
            g = at_d + 4 * i
            wait_chunk(g + 4)
            wait_chunk(g + 5)
            column(2 * i, g)
            column(2 * i + 1, g + 2)
            if own:
                @pl.when(i > 0)
                def _():
                    p_copy(slot2, 2 * i - 2, 2).start()

            for k in range(4):
                prefetch(u, phase, 4 * i + k)

            @pl.when(more | (i < full - 1))
            def _():
                wait_chunk(g + 6)
                wait_chunk(g + 7)

            return carry

        def rest():
            g = at_d + 4 * full
            column(zero + 2 * full, g)
            for k in range(2):
                prefetch(u, phase, zero + 4 * full + k)

            @pl.when(more)
            def _():
                wait_chunk(g + 4)
                wait_chunk(g + 5)

        assert nq % 2 == 1 and nu % 4 == 2
        with jax.named_scope('down' if own else 'down_peer'):
            lax.fori_loop(0, full, body, 0)
            rest()
        if own:
            p_copy(slot2, zero + 2 * full - 2, 3).start()

    def up(u, phase):
        at_u = base(u, phase)

        def cols_of(c, slot):
            a = jnp.dot(hbuf[...], ring[slot], preferred_element_type=F32) + bup[c]
            t = jnp.tanh(0.7978845608028654 * (a + 0.044715 * (a * a * a)))
            ubuf[:, pl.ds(pl.multiple_of(c * CW, CW), CW)] = (0.5 * a * (1.0 + t)).astype(BF16)

        def body(i, carry):
            g = at_u + 4 * i
            for k in range(4, 8):
                wait_chunk(g + k)
            for k in range(4):
                cols_of(4 * i + k, slot_at(g + k))
            for k in range(4):
                prefetch(u, phase, 4 * i + k)
            return carry

        def rest():
            for k in range(4, 4 + nu % 4):
                wait_chunk(at_u + full * 4 + k)
            for k in range(nu % 4):
                cols_of(zero + full * 4 + k, slot_at(at_u + full * 4 + k))
            for k in range(nu % 4):
                prefetch(u, phase, zero + full * 4 + k)

        full = nu // 4
        with jax.named_scope('up' if phase == UP else 'up_peer'):
            lax.fori_loop(0, full, body, 0)
            rest()

    def finish(u):
        v = peer_block(u)
        slot = lax.rem(u, 2)
        scoped('p_wait', remote(psend, precv.at[slot], p_send_sem, p_recv_sem.at[slot]).wait_recv)

        @pl.when(v > 0)
        def _():
            scoped('y_wait', pltpu.make_async_copy(ybuf, out.at[0, 0, pl.ds(0, rows), :], y_send_sem).wait)

        block = 32

        def body(i, carry):
            r = pl.ds(pl.multiple_of(i * block, block), block)
            ybuf[r, :] = (zbuf[r, :] + precv[slot, r, :].astype(F32)).astype(BF16)
            return carry

        lax.fori_loop(0, rows // block, body, 0)

        @pl.when(jnp.logical_not(last))
        def _():
            @pl.when(v >= 2)
            def _():
                pl.semaphore_wait(credit_sem, 1)

            to = lax.rem(v, 2)
            remote(ybuf, xbuf.at[to], y_send_sem, xslot_sem.at[to], nxt).start()

        @pl.when(last)
        def _():
            mb, seq, r = place(v)
            pltpu.make_async_copy(ybuf, out.at[mb, seq, r, :], y_send_sem).start()

    def step(u, carry):
        slot2 = lax.rem(u, 2)

        @pl.when(valid(own_block(u)))
        def _():
            attend(u)
            scoped('ln2', layer_norm, x1own, hbuf, g2, s2)
            up(u, UP)
            load_x(own_block(u) + 1)
            down(u, DOWN)

        @pl.when(leads & (u == n_steps - 1))
        def _():
            finish(u - 1)

        @pl.when(valid(peer_block(u)))
        def _():
            scoped('x1_wait', remote(x1own, x1recv.at[slot2], x1_send_sem, x1_recv_sem.at[slot2]).wait_recv)
            scoped('ln_peer', layer_norm, x1recv.at[slot2], hbuf, g2, s2)
            up(u, UP2)
            down(u, DOWN2)

        return carry

    lax.fori_loop(0, n_steps, step, 0)

    @pl.when(leads)
    def _():
        finish(zero + n_steps - 1)


    remote(x1own, x1recv.at[0], x1_send_sem, x1_recv_sem.at[0]).wait_send()
    remote(psend, precv.at[0], p_send_sem, p_recv_sem.at[0]).wait_send()
    pltpu.make_async_copy(ybuf, out.at[0, 0, pl.ds(0, rows), :], y_send_sem).wait()

    @pl.when(leads)
    def _():
        for copy in kv_copies(zero, zero):
            copy.wait_send()

    @pl.when(jnp.logical_not(even))
    def _():
        for i in range(2 * PARTS):
            w_copy(i).wait_send()

    @pl.when(even & (rank == 0))
    def _():
        for i in range(PARTS, 2 * PARTS):
            w_copy(i).wait_send()

    @pl.when(last)
    def _():
        for i in range(RELAYED):
            hop_c(i).wait_send()


def run_stage(x_loc, params, n_stages):
    (ln1_gain, ln1_bias, w_q, b_q, w_kv, b_kv, w_o, b_o, ln2_gain, ln2_bias, w_up, b_up, w_down, b_down) = params
    n_micro, _, seq_loc, hidden = x_loc.shape
    ffn_loc = w_up.shape[2]
    rows = seq_loc // 2
    n_blocks = 4 * n_micro
    nq = hidden // CW
    nu = ffn_loc // CW
    heads_half = hidden // 2 // HEAD
    cfg = (n_stages, n_blocks, rows, hidden, ffn_loc)
    vmem = pl.BlockSpec(memory_space=pltpu.VMEM)
    anym = pl.BlockSpec(memory_space=pl.ANY)
    args = (
        x_loc, ln1_gain, ln1_bias, w_q, b_q.reshape(heads_half, 1, HEAD), w_kv, b_kv, w_o, b_o.reshape(nq, 1, CW),
        ln2_gain, ln2_bias, w_up, b_up.reshape(nu, 1, CW), w_down, b_down.reshape(nq, 1, CW),
    )
    in_specs = [anym, vmem, vmem, anym, vmem, anym, vmem, anym, vmem, vmem, vmem, anym, vmem, anym, vmem]
    half = hidden // 2
    out_shape = (
        jax.ShapeDtypeStruct(x_loc.shape, BF16),
        jax.ShapeDtypeStruct((hidden, half), BF16),
        jax.ShapeDtypeStruct((half, hidden), BF16),
        jax.ShapeDtypeStruct((hidden, half), BF16),
        jax.ShapeDtypeStruct((hidden, half), BF16),
        jax.ShapeDtypeStruct((half, hidden), BF16),
        jax.ShapeDtypeStruct((half, hidden), BF16),
    )
    dma = pltpu.SemaphoreType.DMA
    scratch = [
        pltpu.VMEM((SLOTS, hidden, CW), BF16),
        pltpu.VMEM((2, rows, hidden), BF16),
        pltpu.VMEM((rows, hidden), BF16),
        pltpu.VMEM((2 * heads_half, rows, HEAD), BF16),
        pltpu.VMEM((rows, hidden), BF16),
        pltpu.VMEM((rows, hidden), BF16),
        pltpu.VMEM((2, rows, hidden), BF16),
        pltpu.VMEM((rows, ffn_loc), BF16),
        pltpu.VMEM((rows, hidden), F32),
        pltpu.VMEM((rows, hidden), BF16),
        pltpu.VMEM((2, rows, hidden), BF16),
        pltpu.VMEM((rows, hidden), BF16),
        pltpu.VMEM((2, HEAD, 4 * rows), BF16),
        pltpu.VMEM((2, 4 * rows, 2 * HEAD), BF16),
        pltpu.VMEM((2 * heads_half, 1, HEAD), F32),
        dma((SLOTS,)),
        dma,
        dma((2,)),
        dma((2,)),
        dma((2 * PARTS,)),
        dma((2 * PARTS,)),
        dma((RELAYED,)),
        dma((RELAYED,)),
        dma((RELAYED,)),
        dma((RELAYED,)),
        dma((2,)),
        dma((4,)),
        dma((4,)),
        dma,
        dma((2,)),
        dma,
        dma((2,)),
        dma,
        pltpu.SemaphoreType.REGULAR,
        pltpu.SemaphoreType.REGULAR,
        pltpu.SemaphoreType.REGULAR,
    ]
    return pl.pallas_call(
        functools.partial(stage_kernel, cfg),
        out_shape=out_shape,
        in_specs=in_specs,
        out_specs=(anym,) * 7,
        scratch_shapes=scratch,
        compiler_params=pltpu.CompilerParams(collective_id=0, has_side_effects=True, vmem_limit_bytes=60 * 2 ** 20),
        name='stage_loop',
    )(*args)[0]


def solution(mesh):
    pp_size = mesh.shape['pp']

    def stage_program(x_loc, *params):
        result = run_stage(x_loc, params, pp_size)
        is_last = lax.axis_index('pp') == pp_size - 1
        return jnp.where(is_last, result, jnp.zeros_like(result))[None]

    return jax.shard_map(stage_program, mesh=mesh, in_specs=(P(None, 'dp', 'tp', None),) + PARAM_SPECS, out_specs=P('pp', None, 'dp', 'tp', None), check_vma=False)
```
